8 devices in a mesh: seqs: 2 (over z, y), states: 4 (over x, core).
Axes of the slice: x: 2, y: 2, z: 1, core: 2. Of those that a mesh axis runs over, the one named last changes fastest.
Arguments:
- trans_mat: bfloat16 [8192, 8192], P(None, 'states')
- emit_mat: bfloat16 [8192, 10000], P('states')
- init_prob: float32 [8192], P('states')
- tokens: int32 [64, 64], P('seqs'), parts along dimension 0
- lengths: int32 [64], P('seqs'), parts along dimension 0
Outputs:
- output 1: float32 [64], P('seqs'), parts along dimension 0
- output 2: float32 [64, 8192], P('seqs', 'states'), parts along dimension 0
- output 3: float32 [16384, 2048], P(('seqs', 'states')), parts along dimension 0
There are 2 independent parts. The reference program is written for one: setup_inputs(seed, part) draws one part's arguments, and reference() takes and returns one part's arrays. A program takes and returns all parts, laid end to end along the dimension named above; an argument that names none is the same for every part.
All inputs are finite; a program needn't handle non-finite values.
Results may differ from the reference program's by a relative error of at most 0.001.
Values are sent between devices in bfloat16 or wider.
A program may use at most 1 GiB of HBM per device.

```python
import jax
import jax.numpy as jnp
from jax import lax

K = 8192
V = 10000
B = 32
T = 64
GROUPS = 4
BLOCK_SIZE = K // GROUPS


def setup_inputs(seed: int = 0, part: int = 0) -> dict:
    key = jax.random.key(seed)
    key_trans, key_emit, key_init, key_part = jax.random.split(key, 4)
    part_key = jax.random.fold_in(key_part, part)
    key_tok, key_len = jax.random.split(part_key, 2)
    tile_rows = 512

    def trans_tile(tile_idx):
        logits = 2.0 * jax.random.normal(jax.random.fold_in(key_trans, tile_idx), (tile_rows, K), jnp.float32)
        return jax.nn.softmax(logits, axis=1).astype(jnp.bfloat16)

    def emit_tile(tile_idx):
        logits = 1.5 * jax.random.normal(jax.random.fold_in(key_emit, tile_idx), (tile_rows, V), jnp.float32)
        return jax.nn.softmax(logits, axis=1).astype(jnp.bfloat16)

    tile_ids = jnp.arange(K // tile_rows)
    trans_mat = lax.map(trans_tile, tile_ids).reshape(K, K)
    emit_mat = lax.map(emit_tile, tile_ids).reshape(K, V)
    init_prob = jax.nn.softmax(2.0 * jax.random.normal(key_init, (K,), jnp.float32))
    tokens = jax.random.randint(key_tok, (B, T), 0, V, jnp.int32)
    drawn_len = jax.random.randint(key_len, (B,), 1, T + 1, jnp.int32)
    lengths = jnp.where(jnp.arange(B) == 0, T, drawn_len).astype(jnp.int32)
    return {'trans_mat': trans_mat, 'emit_mat': emit_mat, 'init_prob': init_prob, 'tokens': tokens, 'lengths': lengths}


def reference(trans_mat, emit_mat, init_prob, tokens, lengths):
    def emit_at(step_idx):
        return jnp.take(emit_mat, tokens[:, step_idx], axis=1).T.astype(jnp.float32)

    first_mass = init_prob[None, :] * emit_at(0)
    first_norm = jnp.sum(first_mass, axis=1)
    alpha_first = first_mass / first_norm[:, None]

    def forward_step(alpha_cur, step_idx):
        pred_mass = jnp.dot(alpha_cur.astype(jnp.bfloat16), trans_mat, preferred_element_type=jnp.float32)
        new_mass = pred_mass * emit_at(step_idx)
        norm_sum = jnp.sum(new_mass, axis=1)
        live_mask = step_idx < lengths
        step_scale = jnp.where(live_mask, norm_sum, 1.0)
        alpha_next = jnp.where(live_mask[:, None], new_mass / norm_sum[:, None], alpha_cur)
        return alpha_next, (alpha_cur.astype(jnp.bfloat16), step_scale)

    later_steps = jnp.arange(1, T)
    alpha_last, (alpha_prev, scales) = lax.scan(forward_step, alpha_first, later_steps)
    loglik = jnp.log(first_norm) + jnp.sum(jnp.log(scales), axis=0)

    def backward_step(carry, inputs):
        beta_cur, pair_sum = carry
        step_idx, prev_bf, step_scale = inputs
        live_mask = step_idx < lengths
        weight = jnp.where(live_mask[:, None], emit_at(step_idx) * beta_cur / step_scale[:, None], 0.0).astype(jnp.bfloat16)
        pair_sum = pair_sum + jnp.einsum('bgi,bgj->gij', prev_bf.reshape(B, GROUPS, BLOCK_SIZE).astype(jnp.float32), weight.reshape(B, GROUPS, BLOCK_SIZE).astype(jnp.float32))
        beta_prev = lax.dot_general(weight, trans_mat, (((1,), (1,)), ((), ())), preferred_element_type=jnp.float32)
        beta_prev = beta_prev + jnp.where(live_mask, 0.0, 1.0)[:, None]
        return (beta_prev, pair_sum), None

    start = (jnp.ones((B, K), jnp.float32), jnp.zeros((GROUPS, BLOCK_SIZE, BLOCK_SIZE), jnp.float32))
    (_, pair_sum), _ = lax.scan(backward_step, start, (later_steps, alpha_prev, scales), reverse=True)
    diag_blocks = jnp.moveaxis(jnp.diagonal(trans_mat.reshape(GROUPS, BLOCK_SIZE, GROUPS, BLOCK_SIZE), axis1=0, axis2=2), 2, 0)
    counts = (diag_blocks.astype(jnp.float32) * pair_sum).reshape(K, BLOCK_SIZE)
    return loglik, alpha_last, counts
```

```python
import functools

import jax
import jax.numpy as jnp
from jax import lax
from jax.experimental import pallas as pl
from jax.experimental.pallas import tpu as pltpu
from jax.sharding import PartitionSpec as P

MESH = pl.DeviceIdType.MESH
CHUNKS = 4
LOADS = 8


def peers(me):
    return me + 1 - 2 * (me % 2), 3 - me, 3 - (me + 1 - 2 * (me % 2))


def entry_barrier(others):
    barrier = pltpu.get_barrier_semaphore()
    for other in others:
        pl.semaphore_signal(barrier, inc=1, device_id=other, device_id_type=MESH)
    pl.semaphore_wait(barrier, len(others))


def exchange_matmul(me, slot, xbuf, mat, acc, send_sem, recv_sem):
    partner, cross, far = peers(me)
    block = xbuf.shape[3]
    width = block // CHUNKS

    def part(owner, c):
        return xbuf.at[slot, owner, :, pl.ds(c * width, width)]

    def copy(owner, c, kind, device):
        ref = part(owner, c)
        return pltpu.make_async_remote_copy(
            src_ref=ref, dst_ref=ref, send_sem=send_sem.at[slot, kind, c], recv_sem=recv_sem.at[slot, kind, c],
            device_id={"states": device}, device_id_type=MESH)

    sends = []
    for c in range(CHUNKS):
        out = copy(me, c, 1, cross)
        out.start()
        sends.append(out)
        out = copy(me, c, 0, partner)
        out.start()
        sends.append(out)

    def dot(owner, lo, size):
        rows = pl.ds(pl.multiple_of(owner * block + lo, width), size)
        return jnp.dot(xbuf[slot, owner, :, pl.ds(lo, size)], mat[rows, :], preferred_element_type=jnp.float32)

    acc[...] = dot(me, 0, block)
    for c in range(CHUNKS):
        copy(partner, c, 0, partner).wait_recv()
    acc[...] += dot(partner, 0, block)

    def relay(c):
        copy(cross, c, 1, cross).wait_recv()
        out = copy(cross, c, 2, partner)
        out.start()
        sends.append(out)

    for c in range(CHUNKS):
        relay(c)
        acc[...] += dot(cross, c * width, width)
        if c:
            copy(far, c - 1, 2, partner).wait_recv()
            acc[...] += dot(far, (c - 1) * width, width)
    copy(far, CHUNKS - 1, 2, partner).wait_recv()
    acc[...] += dot(far, (CHUNKS - 1) * width, width)
    return sends


def packed(col):
    group = lax.broadcasted_iota(jnp.int32, (8, 128), 1) // 32
    out = jnp.broadcast_to(col[24:32], (8, 128))
    for k in range(3):
        out = jnp.where(group == k, jnp.broadcast_to(col[8 * k:8 * k + 8], (8, 128)), out)
    return out


def unpacked(tile):
    return jnp.concatenate([tile[:, 32 * k:32 * k + 1] for k in range(4)], axis=0)


def forward_kernel(emit_ref, init_ref, len_col, len_pack, a_hbm, hist_ref, scale_ref, log_ref, post_ref,
                   mat, xbuf, acc, cbuf, load_sem, send_sem, recv_sem, csend_sem, crecv_sem):
    me = lax.axis_index("states")
    partner, cross, far = peers(me)
    rows = mat.shape[0] // LOADS
    loads = [pltpu.make_async_copy(a_hbm.at[pl.ds(k * rows, rows)], mat.at[pl.ds(k * rows, rows)], load_sem.at[k]) for k in range(LOADS)]
    for load in loads:
        load.start()
    entry_barrier([{"states": partner}, {"states": cross}, {"states": far}])

    def norm_total(mass):
        cbuf[me] = packed(jnp.sum(mass, axis=1, keepdims=True))

        def copy(owner, kind, device):
            return pltpu.make_async_remote_copy(
                src_ref=cbuf.at[owner], dst_ref=cbuf.at[owner], send_sem=csend_sem.at[kind], recv_sem=crecv_sem.at[kind],
                device_id={"states": device}, device_id_type=MESH)

        others = (far, cross, partner)
        for kind, other in enumerate(others):
            copy(me, kind, other).start()
        for kind, other in enumerate(others):
            copy(other, kind, other).wait_recv()
        for kind, other in enumerate(others):
            copy(me, kind, other).wait_send()
        return cbuf[0] + cbuf[1] + cbuf[2] + cbuf[3]

    mass = init_ref[...] * emit_ref[0].astype(jnp.float32)
    total = norm_total(mass)
    scale_ref[0] = total
    log_ref[...] = jnp.log(total)
    alpha = mass * unpacked(1.0 / total)
    post_ref[...] = alpha
    xbuf[0, me] = alpha.astype(jnp.bfloat16)
    hist_ref[0] = alpha.astype(jnp.bfloat16)
    for load in loads:
        load.wait()

    def step(t, carry):
        slot = (t - 1) % 2
        sends = exchange_matmul(me, slot, xbuf, mat, acc, send_sem, recv_sem)
        mass = acc[...] * emit_ref[t].astype(jnp.float32)
        acc[...] = mass
        total = norm_total(mass)
        live = t < len_pack[...]
        scale = jnp.where(live, total, 1.0)
        scale_ref[t] = scale
        log_ref[...] += jnp.log(scale)
        alpha = jnp.where(t < len_col[...], acc[...] * unpacked(1.0 / total), post_ref[...])
        post_ref[...] = alpha
        xbuf[t % 2, me] = alpha.astype(jnp.bfloat16)
        hist_ref[t] = alpha.astype(jnp.bfloat16)
        for send in sends:
            send.wait_send()
        return carry

    lax.fori_loop(1, emit_ref.shape[0], step, 0)


def forward(emit_seq, init_loc, lengths_loc, trans_loc):
    steps, seqs, block = emit_seq.shape
    full = trans_loc.shape[0]
    col = jnp.broadcast_to(lengths_loc[:, None], (seqs, block))[:, :1]
    pack = jnp.broadcast_to(lengths_loc.reshape(4, 8).T[:, :, None], (8, 4, 32)).reshape(8, 128)
    vmem = pl.BlockSpec(memory_space=pltpu.VMEM)
    hist, scales, log_sum, last = pl.pallas_call(
        forward_kernel,
        out_shape=[
            jax.ShapeDtypeStruct((steps, seqs, block), jnp.bfloat16),
            jax.ShapeDtypeStruct((steps, 8, 128), jnp.float32),
            jax.ShapeDtypeStruct((8, 128), jnp.float32),
            jax.ShapeDtypeStruct((seqs, block), jnp.float32),
        ],
        in_specs=[vmem] * 4 + [pl.BlockSpec(memory_space=pltpu.HBM)],
        out_specs=[vmem] * 4,
        scratch_shapes=[
            pltpu.VMEM((full, block), jnp.bfloat16),
            pltpu.VMEM((2, 4, seqs, block), jnp.bfloat16),
            pltpu.VMEM((seqs, block), jnp.float32),
            pltpu.VMEM((4, 8, 128), jnp.float32),
            pltpu.SemaphoreType.DMA((LOADS,)),
            pltpu.SemaphoreType.DMA((2, 3, CHUNKS)),
            pltpu.SemaphoreType.DMA((2, 3, CHUNKS)),
            pltpu.SemaphoreType.DMA((3,)),
            pltpu.SemaphoreType.DMA((3,)),
        ],
        compiler_params=pltpu.CompilerParams(collective_id=0, has_side_effects=True, vmem_limit_bytes=60 * 1024 * 1024),
        name="forward",
    )(emit_seq, init_loc[None, :], col, pack, trans_loc)
    unpack = lambda x: jnp.swapaxes(x[..., ::32], -1, -2).reshape(x.shape[:-2] + (seqs,))
    return hist, unpack(scales), unpack(log_sum), last


def solution(mesh):
    def step_weight(live_mask, emit_now, beta_cur, step_scale):
        scaled = emit_now.astype(jnp.float32) * beta_cur / step_scale[:, None]
        return jnp.where(live_mask[:, None], scaled, 0.0).astype(jnp.bfloat16)

    def local_run(trans_loc, emit_loc, init_loc, tokens_loc, lengths_loc):
        seq_count, step_count = tokens_loc.shape
        block_size = trans_loc.shape[1]
        group_idx = lax.axis_index('states')
        emit_seq = jnp.transpose(emit_loc.at[:, tokens_loc.T].get(mode="promise_in_bounds"), (1, 2, 0))
        live_steps = jnp.arange(1, step_count)[:, None] < lengths_loc[None, :]

        hist, all_scales, loglik, alpha_last = forward(emit_seq, init_loc, lengths_loc, trans_loc)
        alpha_prev, scales = hist[:-1], all_scales[1:]

        def backward_step(beta_cur, inputs):
            live_mask, emit_now, step_scale = inputs
            weight = step_weight(live_mask, emit_now, beta_cur, step_scale)
            partial_sum = lax.dot_general(weight, trans_loc, (((1,), (1,)), ((), ())), preferred_element_type=jnp.float32)
            beta_prev = lax.psum_scatter(partial_sum, 'states', scatter_dimension=1, tiled=True)
            return beta_prev + jnp.where(live_mask, 0.0, 1.0)[:, None], weight

        beta_one, late_weights = lax.scan(backward_step, jnp.ones((seq_count, block_size), jnp.float32), (live_steps[1:], emit_seq[2:], scales[1:]), reverse=True)
        first_weight = step_weight(live_steps[0], emit_seq[1], beta_one, scales[0])
        pair_sum = jnp.einsum('tbi,tbj->ij', alpha_prev[1:], late_weights, preferred_element_type=jnp.float32)
        pair_sum = pair_sum + lax.dot_general(alpha_prev[0], first_weight, (((0,), (0,)), ((), ())), preferred_element_type=jnp.float32)
        diag_block = lax.dynamic_slice_in_dim(trans_loc, group_idx * block_size, block_size, axis=0)
        counts = diag_block.astype(jnp.float32) * pair_sum
        return loglik, alpha_last, counts

    return jax.shard_map(local_run, mesh=mesh, in_specs=(P(None, 'states'), P('states', None), P('states'), P('seqs', None), P('seqs')), out_specs=(P('seqs'), P('seqs', 'states'), P(('seqs', 'states'), None)), check_vma=False)
```

```python
import functools

import jax
import jax.numpy as jnp
from jax import lax
from jax.experimental import pallas as pl
from jax.experimental.pallas import tpu as pltpu
from jax.sharding import PartitionSpec as P

MESH = pl.DeviceIdType.MESH
CHUNKS = 4
LOADS = 8
TILE = 256


def peers(me):
    return me + 1 - 2 * (me % 2), 3 - me, 3 - (me + 1 - 2 * (me % 2))


def entry_barrier(others):
    barrier = pltpu.get_barrier_semaphore()
    for other in others:
        pl.semaphore_signal(barrier, inc=1, device_id=other, device_id_type=MESH)
    pl.semaphore_wait(barrier, len(others))


def exchange_matmul(me, slot, xbuf, mat, acc, send_sem, recv_sem, meanwhile):
    partner, cross, far = peers(me)
    block = xbuf.shape[3]
    width = block // CHUNKS

    def part(owner, c):
        return xbuf.at[slot, owner, :, pl.ds(c * width, width)]

    def copy(owner, c, kind, device):
        ref = part(owner, c)
        return pltpu.make_async_remote_copy(
            src_ref=ref, dst_ref=ref, send_sem=send_sem.at[slot, kind, c], recv_sem=recv_sem.at[slot, kind, c],
            device_id={"states": device}, device_id_type=MESH)

    sends = []
    for c in range(CHUNKS):
        out = copy(me, c, 1, cross)
        out.start()
        sends.append(out)
        out = copy(me, c, 0, partner)
        out.start()
        sends.append(out)
    meanwhile()

    def dot(owner, lo, size):
        rows = pl.ds(pl.multiple_of(owner * block + lo, width), size)
        return jnp.dot(xbuf[slot, owner, :, pl.ds(lo, size)], mat[rows, :], preferred_element_type=jnp.float32)

    acc[...] = dot(me, 0, block)
    for c in range(CHUNKS):
        copy(partner, c, 0, partner).wait_recv()
    acc[...] += dot(partner, 0, block)

    def relay(c):
        copy(cross, c, 1, cross).wait_recv()
        out = copy(cross, c, 2, partner)
        out.start()
        sends.append(out)

    for c in range(CHUNKS):
        relay(c)
        acc[...] += dot(cross, c * width, width)
        if c:
            copy(far, c - 1, 2, partner).wait_recv()
            acc[...] += dot(far, (c - 1) * width, width)
    copy(far, CHUNKS - 1, 2, partner).wait_recv()
    acc[...] += dot(far, (CHUNKS - 1) * width, width)
    return sends


def packed(col):
    group = lax.broadcasted_iota(jnp.int32, (8, 128), 1) // 32
    out = jnp.broadcast_to(col[24:32], (8, 128))
    for k in range(3):
        out = jnp.where(group == k, jnp.broadcast_to(col[8 * k:8 * k + 8], (8, 128)), out)
    return out


def unpacked(tile):
    return jnp.concatenate([tile[:, 32 * k:32 * k + 1] for k in range(4)], axis=0)


def forward_kernel(emit_ref, init_ref, len_col, len_pack, a_hbm, hist_ref, scale_ref, log_ref, post_ref, rows_hbm,
                   mat, xbuf, acc, cbuf, load_sem, send_sem, recv_sem, csend_sem, crecv_sem,
                   over_send, over_recv, turn_send, turn_recv, near_send, near_recv):
    me, seq = lax.axis_index("states"), lax.axis_index("seqs")
    partner, cross, far = peers(me)
    steps, _, block = emit_ref.shape
    rows = mat.shape[0] // LOADS
    loads = [pltpu.make_async_copy(a_hbm.at[pl.ds(k * rows, rows)], mat.at[pl.ds(k * rows, rows)], load_sem.at[k]) for k in range(LOADS)]
    for load in loads:
        load.start()
    entry_barrier([{"states": partner}, {"states": cross}, {"states": far}, {"seqs": 1 - seq}])

    half = block // 2
    piece = half // steps

    def over(b, kind, owner, other):
        lo = seq * half + b * piece
        return pltpu.make_async_remote_copy(
            src_ref=a_hbm.at[pl.ds(other * block + lo, piece)], dst_ref=rows_hbm.at[owner, pl.ds(lo, piece)],
            send_sem=over_send.at[b % 3, kind], recv_sem=over_recv.at[b % 3, kind], device_id={"states": other}, device_id_type=MESH)

    def turn(b, kind, owner):
        ref = rows_hbm.at[owner, pl.ds(seq * half + b * piece, piece)]
        return pltpu.make_async_remote_copy(
            src_ref=ref, dst_ref=ref, send_sem=turn_send.at[b % 2, kind], recv_sem=turn_recv.at[kind],
            device_id={"seqs": 1 - seq}, device_id_type=MESH)

    def near(b):
        return pltpu.make_async_remote_copy(
            src_ref=a_hbm.at[pl.ds(partner * block + b * 2 * piece, 2 * piece)], dst_ref=rows_hbm.at[me, pl.ds(b * 2 * piece, 2 * piece)],
            send_sem=near_send.at[b % 2], recv_sem=near_recv, device_id={"states": partner}, device_id_type=MESH)

    others = ((0, cross), (1, far))

    def rows_start(b):
        for kind, other in others:
            over(b, kind, me, other).start()
        near(b).start()

    def rows_turn(b):
        near(b).wait_send()
        for kind, other in others:
            over(b, kind, me, other).wait_send()
            over(b, kind, other, other).wait_recv()
            turn(b, kind, other).start()

    def rows_end(b):
        for kind, other in others:
            turn(b, kind, other).wait_send()

    def norm_total(mass):
        cbuf[me] = packed(jnp.sum(mass, axis=1, keepdims=True))

        def copy(owner, kind, device):
            return pltpu.make_async_remote_copy(
                src_ref=cbuf.at[owner], dst_ref=cbuf.at[owner], send_sem=csend_sem.at[kind], recv_sem=crecv_sem.at[kind],
                device_id={"states": device}, device_id_type=MESH)

        return [(copy(me, kind, other), copy(other, kind, other)) for kind, other in enumerate((far, cross, partner))]

    def norm_end(pairs):
        for _, arrive in pairs:
            arrive.wait_recv()
        for leave, _ in pairs:
            leave.wait_send()
        return cbuf[0] + cbuf[1] + cbuf[2] + cbuf[3]

    mass = init_ref[...] * emit_ref[0].astype(jnp.float32)
    pairs = norm_total(mass)
    for leave, _ in pairs:
        leave.start()
    rows_start(0)
    total = norm_end(pairs)
    scale_ref[0] = total
    log_ref[...] = jnp.log(total)
    alpha = mass * unpacked(1.0 / total)
    post_ref[...] = alpha
    xbuf[0, me] = alpha.astype(jnp.bfloat16)
    hist_ref[1] = alpha.astype(jnp.bfloat16)
    for load in loads:
        load.wait()

    def step(t, carry):
        slot = (t - 1) % 2
        sends = exchange_matmul(me, slot, xbuf, mat, acc, send_sem, recv_sem, lambda: rows_start(t))
        mass = acc[...] * emit_ref[t].astype(jnp.float32)
        acc[...] = mass
        pairs = norm_total(mass)
        for leave, _ in pairs:
            leave.start()
        for send in sends:
            send.wait_send()
        rows_turn(t - 1)

        @pl.when(t > 1)
        def _():
            rows_end(t - 2)

        total = norm_end(pairs)
        live = t < len_pack[...]
        scale = jnp.where(live, total, 1.0)
        scale_ref[t] = scale
        log_ref[...] += jnp.log(scale)
        alpha = jnp.where(t < len_col[...], acc[...] * unpacked(1.0 / total), post_ref[...])
        post_ref[...] = alpha
        xbuf[t % 2, me] = alpha.astype(jnp.bfloat16)
        hist_ref[(t + 1) % steps] = alpha.astype(jnp.bfloat16)
        return carry

    lax.fori_loop(1, steps, step, 0)
    rows_turn(steps - 1)
    rows_end(steps - 2)
    rows_end(steps - 1)

    def landed(ref, sem):
        pltpu.make_async_copy(ref, ref, sem).wait()

    for kind, other in others:
        landed(rows_hbm.at[other, pl.ds((1 - seq) * half, half)], turn_recv.at[kind])
    landed(rows_hbm.at[partner], near_recv)


def forward(emit_seq, init_loc, col, pack, trans_loc):
    steps, seqs, block = emit_seq.shape
    full = trans_loc.shape[0]
    vmem, hbm = pl.BlockSpec(memory_space=pltpu.VMEM), pl.BlockSpec(memory_space=pltpu.HBM)
    dma = pltpu.SemaphoreType.DMA
    return pl.pallas_call(
        forward_kernel,
        out_shape=[
            jax.ShapeDtypeStruct((steps, seqs, block), jnp.bfloat16),
            jax.ShapeDtypeStruct((steps, 8, 128), jnp.float32),
            jax.ShapeDtypeStruct((8, 128), jnp.float32),
            jax.ShapeDtypeStruct((seqs, block), jnp.float32),
            jax.ShapeDtypeStruct((full // block, block, block), jnp.bfloat16),
        ],
        in_specs=[vmem] * 4 + [hbm],
        out_specs=[vmem] * 4 + [hbm],
        scratch_shapes=[
            pltpu.VMEM((full, block), jnp.bfloat16),
            pltpu.VMEM((2, 4, seqs, block), jnp.bfloat16),
            pltpu.VMEM((seqs, block), jnp.float32),
            pltpu.VMEM((4, 8, 128), jnp.float32),
            dma((LOADS,)), dma((2, 3, CHUNKS)), dma((2, 3, CHUNKS)), dma((3,)), dma((3,)),
            dma((3, 2)), dma((3, 2)), dma((2, 2)), dma((2,)), dma((2,)), dma,
        ],
        compiler_params=pltpu.CompilerParams(collective_id=0, has_side_effects=True, vmem_limit_bytes=60 * 1024 * 1024),
        name="forward",
    )(emit_seq, init_loc[None, :], col, pack, trans_loc)


def backward_kernel(emit_ref, scale_ref, len_col, a_hbm, rows_hbm, hist_ref, mat, xbuf, acc, coef, load_sem, send_sem, recv_sem):
    me = lax.axis_index("states")
    partner, cross, far = peers(me)
    steps, _, block = emit_ref.shape
    owners = (me, partner, cross, far)
    loads = []
    for k, owner in enumerate(owners):
        src = a_hbm.at[pl.ds(me * block, block)] if k == 0 else rows_hbm.at[owner]
        loads.append(pltpu.make_async_copy(src, mat.at[pl.ds(owner * block, block)], load_sem.at[k]))
        loads[-1].start()
    entry_barrier([{"states": partner}, {"states": cross}, {"states": far}])

    def weigh(t):
        inv = jnp.where(t < len_col[...], unpacked(1.0 / scale_ref[t]), 0.0)
        coef[...] = emit_ref[t].astype(jnp.float32) * inv

    def emit_weight(t, weight):
        xbuf[t % 2, me] = weight.astype(jnp.bfloat16)
        hist_ref[t] = weight.astype(jnp.bfloat16)

    weigh(steps - 1)
    emit_weight(steps - 1, coef[...])
    hist_ref[0] = jnp.zeros(hist_ref.shape[1:], hist_ref.dtype)

    side = block // TILE
    for owner, load in zip(owners, loads):
        load.wait()

        def flip_row(r, carry):
            def flip(c, inner):
                def tile(p, q):
                    return pl.ds(pl.multiple_of(owner * block + p * TILE, TILE), TILE), pl.ds(pl.multiple_of(q * TILE, TILE), TILE)

                upper, lower = mat[tile(r, c)], mat[tile(c, r)]
                mat[tile(r, c)] = lower.T
                mat[tile(c, r)] = upper.T
                return inner

            return lax.fori_loop(r, side, flip, carry)

        lax.fori_loop(0, side, flip_row, 0)

    def step(k, carry):
        t = steps - 1 - k
        sends = exchange_matmul(me, t % 2, xbuf, mat, acc, send_sem, recv_sem, lambda: weigh(t - 1))
        beta = acc[...] + jnp.where(t < len_col[...], 0.0, 1.0)
        emit_weight(t - 1, coef[...] * beta)
        for send in sends:
            send.wait_send()
        return carry

    lax.fori_loop(0, steps - 2, step, 0)


def backward(emit_seq, scales, col, trans_loc, rows_loc):
    steps, seqs, block = emit_seq.shape
    full = trans_loc.shape[0]
    vmem, hbm = pl.BlockSpec(memory_space=pltpu.VMEM), pl.BlockSpec(memory_space=pltpu.HBM)
    dma = pltpu.SemaphoreType.DMA
    return pl.pallas_call(
        backward_kernel,
        out_shape=jax.ShapeDtypeStruct((steps, seqs, block), jnp.bfloat16),
        in_specs=[vmem] * 3 + [hbm] * 2,
        out_specs=vmem,
        scratch_shapes=[
            pltpu.VMEM((full, block), jnp.bfloat16),
            pltpu.VMEM((2, 4, seqs, block), jnp.bfloat16),
            pltpu.VMEM((seqs, block), jnp.float32),
            pltpu.VMEM((seqs, block), jnp.float32),
            dma((4,)), dma((2, 3, CHUNKS)), dma((2, 3, CHUNKS)),
        ],
        compiler_params=pltpu.CompilerParams(collective_id=1, has_side_effects=True, vmem_limit_bytes=60 * 1024 * 1024),
        name="backward",
    )(emit_seq, scales, col, trans_loc, rows_loc)


def solution(mesh):
    def local_run(trans_loc, emit_loc, init_loc, tokens_loc, lengths_loc):
        seqs, steps = tokens_loc.shape
        block = trans_loc.shape[1]
        emit_seq = jnp.transpose(emit_loc.at[:, tokens_loc.T].get(mode="promise_in_bounds"), (1, 2, 0))
        col = lengths_loc[:, None]
        pack = jnp.broadcast_to(lengths_loc.reshape(4, 8).T[:, :, None], (8, 4, 32)).reshape(8, 128)
        alphas, scales, log_sum, last, rows_loc = forward(emit_seq, init_loc, col, pack, trans_loc)
        weights = backward(emit_seq, scales, col, trans_loc, rows_loc)
        pair_sum = lax.dot_general(alphas.reshape(steps * seqs, block), weights.reshape(steps * seqs, block), (((0,), (0,)), ((), ())), preferred_element_type=jnp.float32)
        diag_block = lax.dynamic_slice_in_dim(trans_loc, lax.axis_index('states') * block, block, axis=0)
        counts = diag_block.astype(jnp.float32) * pair_sum
        return log_sum[:, ::32].T.reshape(seqs), last, counts

    return jax.shard_map(local_run, mesh=mesh, in_specs=(P(None, 'states'), P('states', None), P('states'), P('seqs', None), P('seqs')), out_specs=(P('seqs'), P('seqs', 'states'), P(('seqs', 'states'), None)), check_vma=False)
```

```python
import jax
import jax.numpy as jnp
from jax import lax
from jax.experimental import pallas as pl
from jax.experimental.pallas import tpu as pltpu
from jax.sharding import PartitionSpec as P

MESH = pl.DeviceIdType.MESH
LOADS = 8
TILE = 256
SLOTS = 4
COPIES = 4


def entry_barrier(others):
    barrier = pltpu.get_barrier_semaphore()
    for other in others:
        pl.semaphore_signal(barrier, inc=1, device_id=other, device_id_type=MESH)
    pl.semaphore_wait(barrier, len(others))


def cols(c):
    return pl.ds(c * TILE, TILE)


class Exchange:
    def __init__(self, me, xbuf, mat, acc, send_sem, recv_sem):
        self.me, self.xbuf, self.mat, self.acc = me, xbuf, mat, acc
        self.send_sem, self.recv_sem = send_sem, recv_sem
        self.block = xbuf.shape[3]
        self.partner = me + 1 - 2 * (me % 2)
        self.cross = 3 - me
        self.far = (me + 2) % 4
        quarter = self.block // 4
        self.pieces = [(k * quarter, quarter) for k in range(3)] + [(3 * quarter, quarter // 2), (3 * quarter + quarter // 2, quarter // 2)]

    def copy(self, slot, owner, k, kind, device):
        lo, size = self.pieces[k]
        ref = self.xbuf.at[slot, owner, :, pl.ds(lo, size)]
        return pltpu.make_async_remote_copy(
            src_ref=ref, dst_ref=ref, send_sem=self.send_sem.at[slot, kind, k], recv_sem=self.recv_sem.at[slot, kind, k],
            device_id={"states": device}, device_id_type=MESH)

    def send(self, slot, k, more):
        @pl.when(more)
        def _():
            self.copy(slot, self.me, k, 1, self.cross).start()
            self.copy(slot, self.me, k, 0, self.partner).start()

    def wait_sends(self, slot):
        for k in range(len(self.pieces)):
            self.copy(slot, self.me, k, 1, self.cross).wait_send()
            self.copy(slot, self.me, k, 0, self.partner).wait_send()
            self.copy(slot, self.cross, k, 2, self.partner).wait_send()

    def product(self, slot, owner, lo, size, first=False, last=False):
        lhs = self.xbuf[slot, owner, :, pl.ds(lo, size)]
        seqs = lhs.shape[0]
        rows = pl.ds(pl.multiple_of(owner * self.block + lo, 128), size)
        if last:
            self.acc[:seqs] += jnp.dot(lhs, self.mat[rows, :], preferred_element_type=jnp.float32)
        else:
            prod = jnp.dot(jnp.concatenate([lhs] * COPIES, axis=0), self.mat[rows, :], preferred_element_type=jnp.float32)
            self.acc[...] = prod if first else self.acc[...] + prod

    def run(self, slot, meanwhile):
        count = len(self.pieces)
        meanwhile()
        self.product(slot, self.me, 0, self.block, first=True)
        for k in range(count):
            self.copy(slot, self.partner, k, 0, self.partner).wait_recv()
        self.product(slot, self.partner, 0, self.block)
        for k in range(count + 1):
            if k < count:
                self.copy(slot, self.cross, k, 1, self.cross).wait_recv()
                self.copy(slot, self.cross, k, 2, self.partner).start()
                self.product(slot, self.cross, *self.pieces[k])
            if k:
                self.copy(slot, self.far, k - 1, 2, self.partner).wait_recv()
                self.product(slot, self.far, *self.pieces[k - 1], last=k == count)


def packed(col):
    group = lax.broadcasted_iota(jnp.int32, (8, 128), 1) // 32
    out = jnp.broadcast_to(col[24:32], (8, 128))
    for k in range(3):
        out = jnp.where(group == k, jnp.broadcast_to(col[8 * k:8 * k + 8], (8, 128)), out)
    return out


def unpacked(tile):
    return jnp.concatenate([tile[:, 32 * k:32 * k + 1] for k in range(4)], axis=0)


def forward_kernel(emit_ref, init_ref, len_col, len_pack, a_hbm, hist_ref, scale_ref, log_ref, post_ref, rows_hbm,
                   mat, xbuf, acc, cbuf, load_sem, send_sem, recv_sem, csend_sem, crecv_sem,
                   over_send, over_recv, turn_send, turn_recv, near_send, near_recv):
    me, seq = lax.axis_index("states"), lax.axis_index("seqs")
    partner, cross, far = me + 1 - 2 * (me % 2), 3 - me, (me + 2) % 4
    steps, seqs, block = emit_ref.shape
    chunks = block // TILE
    rows = mat.shape[0] // LOADS
    loads = [pltpu.make_async_copy(a_hbm.at[pl.ds(k * rows, rows)], mat.at[pl.ds(k * rows, rows)], load_sem.at[k]) for k in range(LOADS)]
    for load in loads:
        load.start()
    entry_barrier([{"states": partner}, {"states": cross}, {"states": far}, {"seqs": 1 - seq}])

    half = block // 2
    piece = half // steps
    others = ((0, cross), (1, far))

    def over(b, kind, owner, other):
        lo = seq * half + b * piece
        return pltpu.make_async_remote_copy(
            src_ref=a_hbm.at[pl.ds(other * block + lo, piece)], dst_ref=rows_hbm.at[owner, pl.ds(lo, piece)],
            send_sem=over_send.at[b % 3, kind], recv_sem=over_recv.at[b % 3, kind], device_id={"states": other}, device_id_type=MESH)

    def turn(b, kind, owner):
        ref = rows_hbm.at[owner, pl.ds(seq * half + b * piece, piece)]
        return pltpu.make_async_remote_copy(
            src_ref=ref, dst_ref=ref, send_sem=turn_send.at[b % 2, kind], recv_sem=turn_recv.at[kind],
            device_id={"seqs": 1 - seq}, device_id_type=MESH)

    def near(b):
        return pltpu.make_async_remote_copy(
            src_ref=a_hbm.at[pl.ds(partner * block + b * 2 * piece, 2 * piece)], dst_ref=rows_hbm.at[me, pl.ds(b * 2 * piece, 2 * piece)],
            send_sem=near_send.at[b % 2], recv_sem=near_recv, device_id={"states": partner}, device_id_type=MESH)

    def rows_start(b):
        for kind, other in others:
            over(b, kind, me, other).start()
        near(b).start()

    def rows_turn(b):
        near(b).wait_send()
        for kind, other in others:
            over(b, kind, me, other).wait_send()
            over(b, kind, other, other).wait_recv()
            turn(b, kind, other).start()

    def rows_end(b):
        for kind, other in others:
            turn(b, kind, other).wait_send()

    def norm_copy(owner, kind, device):
        return pltpu.make_async_remote_copy(
            src_ref=cbuf.at[owner], dst_ref=cbuf.at[owner], send_sem=csend_sem.at[kind], recv_sem=crecv_sem.at[kind],
            device_id={"states": device}, device_id_type=MESH)

    everyone = tuple(enumerate((far, cross, partner)))

    def norm_start(sums):
        cbuf[me] = packed(jnp.sum(sums, axis=1, keepdims=True))
        for kind, other in everyone:
            norm_copy(me, kind, other).start()

    def norm_end():
        for kind, other in everyone:
            norm_copy(other, kind, other).wait_recv()
        for kind, other in everyone:
            norm_copy(me, kind, other).wait_send()
        return cbuf[0] + cbuf[1] + cbuf[2] + cbuf[3]

    def body():
        ex = Exchange(me, xbuf, mat, acc, send_sem, recv_sem)
        ends = {(lo + size) // TILE - 1: k for k, (lo, size) in enumerate(ex.pieces)}

        def finish_step(t, total):
            inv = jnp.broadcast_to(unpacked(1.0 / total), (seqs, TILE))
            live = t < jnp.broadcast_to(len_col[...], (seqs, TILE))
            for n in range(chunks):
                alpha = jnp.where(live, acc[:seqs, cols(n)] * inv, post_ref[:, cols(n)])
                post_ref[:, cols(n)] = alpha
                low = alpha.astype(jnp.bfloat16)
                xbuf[t % SLOTS, me, :, cols(n)] = low
                hist_ref[(t + 1) % steps, :, cols(n)] = low
                if n in ends:
                    ex.send(t % SLOTS, ends[n], t < steps - 1)

        def fold(n, mass, sums):
            acc[:seqs, cols(n)] = mass
            return sums + mass[:, :128] + mass[:, 128:]

        sums = jnp.zeros((seqs, 128), jnp.float32)
        for n in range(chunks):
            sums = fold(n, init_ref[:, cols(n)] * emit_ref[0, :, cols(n)].astype(jnp.float32), sums)
        norm_start(sums)
        rows_start(0)
        post_ref[...] = jnp.zeros_like(post_ref)
        total = norm_end()
        scale_ref[0] = total
        log_ref[...] = jnp.log(total)
        finish_step(0, total)
        for load in loads:
            load.wait()

        def step(t, carry):
            slot = (t - 1) % SLOTS

            ex.run(slot, lambda: rows_start(t))
            sums = jnp.zeros((seqs, 128), jnp.float32)
            for n in range(chunks):
                sums = fold(n, acc[:seqs, cols(n)] * emit_ref[t, :, cols(n)].astype(jnp.float32), sums)
            norm_start(sums)
            rows_turn(t - 1)

            @pl.when(t > 1)
            def _():
                rows_end(t - 2)
                ex.wait_sends((t - 2) % SLOTS)

            total = norm_end()
            finish_step(t, total)
            scale = jnp.where(t < len_pack[...], total, 1.0)
            scale_ref[t] = scale
            log_ref[...] += jnp.log(scale)
            return carry

        lax.fori_loop(1, steps, step, 0)
        ex.wait_sends((steps - 2) % SLOTS)

    body()
    rows_turn(steps - 1)
    rows_end(steps - 2)
    rows_end(steps - 1)

    def landed(ref, sem):
        pltpu.make_async_copy(ref, ref, sem).wait()

    for kind, other in others:
        landed(rows_hbm.at[other, pl.ds((1 - seq) * half, half)], turn_recv.at[kind])
    landed(rows_hbm.at[partner], near_recv)


def forward(emit_seq, init_loc, col, pack, trans_loc):
    steps, seqs, block = emit_seq.shape
    full = trans_loc.shape[0]
    vmem, hbm = pl.BlockSpec(memory_space=pltpu.VMEM), pl.BlockSpec(memory_space=pltpu.HBM)
    dma = pltpu.SemaphoreType.DMA
    return pl.pallas_call(
        forward_kernel,
        out_shape=[
            jax.ShapeDtypeStruct((steps, seqs, block), jnp.bfloat16),
            jax.ShapeDtypeStruct((steps, 8, 128), jnp.float32),
            jax.ShapeDtypeStruct((8, 128), jnp.float32),
            jax.ShapeDtypeStruct((seqs, block), jnp.float32),
            jax.ShapeDtypeStruct((full // block, block, block), jnp.bfloat16),
        ],
        in_specs=[vmem] * 4 + [hbm],
        out_specs=[vmem] * 4 + [hbm],
        scratch_shapes=[
            pltpu.VMEM((full, block), jnp.bfloat16),
            pltpu.VMEM((SLOTS, 4, seqs, block), jnp.bfloat16),
            pltpu.VMEM((COPIES * seqs, block), jnp.float32),
            pltpu.VMEM((4, 8, 128), jnp.float32),
            dma((LOADS,)), dma((SLOTS, 3, 5)), dma((SLOTS, 3, 5)), dma((3,)), dma((3,)),
            dma((3, 2)), dma((3, 2)), dma((2, 2)), dma((2,)), dma((2,)), dma,
        ],
        compiler_params=pltpu.CompilerParams(collective_id=0, has_side_effects=True, vmem_limit_bytes=60 * 1024 * 1024),
        name="forward",
    )(emit_seq, init_loc[None, :], col, pack, trans_loc)


def backward_kernel(emit_ref, scale_ref, len_col, a_hbm, rows_hbm, hist_ref, mat, xbuf, coef, acc, load_sem, send_sem, recv_sem):
    me = lax.axis_index("states")
    partner, cross, far = me + 1 - 2 * (me % 2), 3 - me, (me + 2) % 4
    steps, seqs, block = emit_ref.shape
    chunks = block // TILE
    owners = (me, partner, cross, far)
    loads = []
    for k, owner in enumerate(owners):
        src = a_hbm.at[pl.ds(me * block, block)] if k == 0 else rows_hbm.at[owner]
        loads.append(pltpu.make_async_copy(src, mat.at[pl.ds(owner * block, block)], load_sem.at[k]))
        loads[-1].start()
    entry_barrier([{"states": partner}, {"states": cross}, {"states": far}])

    def weigh(t):
        inv = jnp.where(t < len_col[...], unpacked(1.0 / scale_ref[t]), 0.0)
        coef[...] = emit_ref[t].astype(jnp.float32) * inv

    weigh(steps - 1)
    hist_ref[0] = jnp.zeros(hist_ref.shape[1:], hist_ref.dtype)

    def flips():
        side = block // TILE
        for owner, load in zip(owners, loads):
            load.wait()

            def flip_row(r, carry):
                def flip(c, inner):
                    def tile(p, q):
                        return pl.ds(pl.multiple_of(owner * block + p * TILE, TILE), TILE), pl.ds(pl.multiple_of(q * TILE, TILE), TILE)

                    upper, lower = mat[tile(r, c)], mat[tile(c, r)]
                    mat[tile(r, c)] = lower.T
                    mat[tile(c, r)] = upper.T
                    return inner

                return lax.fori_loop(r, side, flip, carry)

            lax.fori_loop(0, side, flip_row, 0)

    def body():
        ex = Exchange(me, xbuf, mat, acc, send_sem, recv_sem)
        ends = {(lo + size) // TILE - 1: k for k, (lo, size) in enumerate(ex.pieces)}

        def emit_weight(t, n, weight):
            low = weight.astype(jnp.bfloat16)
            xbuf[t % SLOTS, me, :, cols(n)] = low
            hist_ref[t, :, cols(n)] = low
            if n in ends:
                ex.send(t % SLOTS, ends[n], t > 1)

        for n in range(chunks):
            emit_weight(steps - 1, n, coef[:, cols(n)])
        flips()

        def step(k, carry):
            t = steps - 1 - k
            weigh(t - 1)

            ex.run(t % SLOTS, lambda: None)
            dead = jnp.where(t < jnp.broadcast_to(len_col[...], (seqs, TILE)), 0.0, 1.0)
            for n in range(chunks):
                emit_weight(t - 1, n, coef[:, cols(n)] * (acc[:seqs, cols(n)] + dead))

            @pl.when(k > 0)
            def _():
                ex.wait_sends((t + 1) % SLOTS)

            return carry

        lax.fori_loop(0, steps - 2, step, 0)
        ex.wait_sends(2 % SLOTS)

    body()


def backward(emit_seq, scales, col, trans_loc, rows_loc):
    steps, seqs, block = emit_seq.shape
    full = trans_loc.shape[0]
    vmem, hbm = pl.BlockSpec(memory_space=pltpu.VMEM), pl.BlockSpec(memory_space=pltpu.HBM)
    dma = pltpu.SemaphoreType.DMA
    return pl.pallas_call(
        backward_kernel,
        out_shape=jax.ShapeDtypeStruct((steps, seqs, block), jnp.bfloat16),
        in_specs=[vmem] * 3 + [hbm] * 2,
        out_specs=vmem,
        scratch_shapes=[
            pltpu.VMEM((full, block), jnp.bfloat16),
            pltpu.VMEM((SLOTS, 4, seqs, block), jnp.bfloat16),
            pltpu.VMEM((seqs, block), jnp.float32),
            pltpu.VMEM((COPIES * seqs, block), jnp.float32),
            dma((4,)), dma((SLOTS, 3, 5)), dma((SLOTS, 3, 5)),
        ],
        compiler_params=pltpu.CompilerParams(collective_id=1, has_side_effects=True, vmem_limit_bytes=60 * 1024 * 1024),
        name="backward",
    )(emit_seq, scales, col, trans_loc, rows_loc)


def solution(mesh):
    def local_run(trans_loc, emit_loc, init_loc, tokens_loc, lengths_loc):
        seqs, steps = tokens_loc.shape
        block = trans_loc.shape[1]
        emit_seq = jnp.transpose(emit_loc.at[:, tokens_loc.T].get(mode="promise_in_bounds"), (1, 2, 0))
        col = lengths_loc[:, None]
        pack = jnp.broadcast_to(lengths_loc.reshape(4, 8).T[:, :, None], (8, 4, 32)).reshape(8, 128)
        alphas, scales, log_sum, last, rows_loc = forward(emit_seq, init_loc, col, pack, trans_loc)
        weights = backward(emit_seq, scales, col, trans_loc, rows_loc)
        pair_sum = lax.dot_general(alphas.reshape(steps * seqs, block), weights.reshape(steps * seqs, block), (((0,), (0,)), ((), ())), preferred_element_type=jnp.float32)
        diag_block = lax.dynamic_slice_in_dim(trans_loc, lax.axis_index('states') * block, block, axis=0)
        counts = diag_block.astype(jnp.float32) * pair_sum
        return log_sum[:, ::32].T.reshape(seqs), last, counts

    return jax.shard_map(local_run, mesh=mesh, in_specs=(P(None, 'states'), P('states', None), P('states'), P('seqs', None), P('seqs')), out_specs=(P('seqs'), P('seqs', 'states'), P(('seqs', 'states'), None)), check_vma=False)
```

```python
import jax
import jax.numpy as jnp
from jax import lax
from jax.experimental import pallas as pl
from jax.experimental.pallas import tpu as pltpu
from jax.sharding import PartitionSpec as P

MESH = pl.DeviceIdType.MESH
LOADS = 8
TILE = 256
SLOTS = 4
FORWARD_COPIES = 1
BACKWARD_COPIES = 4
ORDER = (
    "WP0", "P0", "P1", "P2", "R0", "P3", "C0", "R1", "C1", "WF0", "F0", "R2", "C2", "WF1", "R3", "C3", "R4", "F1", "C4", "WF2", "F2",
    "WF3", "WF4", "F3", "F4")


def entry_barrier(others):
    barrier = pltpu.get_barrier_semaphore()
    for other in others:
        pl.semaphore_signal(barrier, inc=1, device_id=other, device_id_type=MESH)
    pl.semaphore_wait(barrier, len(others))


def cols(c):
    return pl.ds(c * TILE, TILE)


class Exchange:
    def __init__(self, me, copies, xbuf, mat, acc, send_sem, recv_sem):
        self.copies = copies
        self.me, self.xbuf, self.mat, self.acc = me, xbuf, mat, acc
        self.send_sem, self.recv_sem = send_sem, recv_sem
        self.block = xbuf.shape[3]
        self.partner = me + 1 - 2 * (me % 2)
        self.cross = 3 - me
        self.far = (me + 2) % 4
        quarter = self.block // 4
        self.pieces = [(k * quarter, quarter) for k in range(3)] + [(3 * quarter, quarter // 2), (3 * quarter + quarter // 2, quarter // 2)]

    def copy(self, slot, owner, k, kind, device):
        lo, size = self.pieces[k]
        ref = self.xbuf.at[slot, owner, :, pl.ds(lo, size)]
        return pltpu.make_async_remote_copy(
            src_ref=ref, dst_ref=ref, send_sem=self.send_sem.at[slot, kind, k], recv_sem=self.recv_sem.at[slot, kind, k],
            device_id={"states": device}, device_id_type=MESH)

    def send(self, slot, k, more):
        @pl.when(more)
        def _():
            self.copy(slot, self.me, k, 1, self.cross).start()
            self.copy(slot, self.me, k, 0, self.partner).start()

    def wait_sends(self, slot):
        for k in range(len(self.pieces)):
            self.copy(slot, self.me, k, 1, self.cross).wait_send()
            self.copy(slot, self.me, k, 0, self.partner).wait_send()
            self.copy(slot, self.cross, k, 2, self.partner).wait_send()

    def product(self, slot, owner, lo, size, first=False, copies=1):
        lhs = self.xbuf[slot, owner, :, pl.ds(lo, size)]
        rows = pl.ds(pl.multiple_of(owner * self.block + lo, 128), size)
        prod = jnp.dot(jnp.concatenate([lhs] * copies, axis=0), self.mat[rows, :], preferred_element_type=jnp.float32)
        out = self.acc.at[:copies * lhs.shape[0]]
        out[...] = prod if first else out[...] + prod

    def run(self, slot, meanwhile):
        meanwhile()
        self.product(slot, self.me, 0, self.block, True, self.copies)
        for token in ORDER:
            what, k = token[:-1], int(token[-1])
            if what == "WP":
                for j in range(len(self.pieces)):
                    self.copy(slot, self.partner, j, 0, self.partner).wait_recv()
            elif what == "P":
                self.product(slot, self.partner, k * (self.block // 4), self.block // 4, copies=self.copies)
            elif what == "R":
                self.copy(slot, self.cross, k, 1, self.cross).wait_recv()
                self.copy(slot, self.cross, k, 2, self.partner).start()
            elif what == "WF":
                self.copy(slot, self.far, k, 2, self.partner).wait_recv()
            else:
                lo, size = self.pieces[k]
                self.product(slot, self.cross if what == "C" else self.far, lo, size)


def packed(col):
    group = lax.broadcasted_iota(jnp.int32, (8, 128), 1) // 32
    out = jnp.broadcast_to(col[24:32], (8, 128))
    for k in range(3):
        out = jnp.where(group == k, jnp.broadcast_to(col[8 * k:8 * k + 8], (8, 128)), out)
    return out


def unpacked(tile):
    return jnp.concatenate([tile[:, 32 * k:32 * k + 1] for k in range(4)], axis=0)


def forward_kernel(emit_ref, init_ref, len_col, len_pack, a_hbm, hist_ref, scale_ref, log_ref, post_ref, rows_hbm,
                   mat, xbuf, acc, cbuf, load_sem, send_sem, recv_sem, csend_sem, crecv_sem,
                   over_send, over_recv, turn_send, turn_recv, near_send, near_recv):
    me, seq = lax.axis_index("states"), lax.axis_index("seqs")
    partner, cross, far = me + 1 - 2 * (me % 2), 3 - me, (me + 2) % 4
    steps, seqs, block = emit_ref.shape
    chunks = block // TILE
    rows = mat.shape[0] // LOADS
    loads = [pltpu.make_async_copy(a_hbm.at[pl.ds(k * rows, rows)], mat.at[pl.ds(k * rows, rows)], load_sem.at[k]) for k in range(LOADS)]
    for load in loads:
        load.start()
    entry_barrier([{"states": partner}, {"states": cross}, {"states": far}, {"seqs": 1 - seq}])

    half = block // 2
    piece = half // steps
    others = ((0, cross), (1, far))

    def over(b, kind, owner, other):
        lo = seq * half + b * piece
        return pltpu.make_async_remote_copy(
            src_ref=a_hbm.at[pl.ds(other * block + lo, piece)], dst_ref=rows_hbm.at[owner, pl.ds(lo, piece)],
            send_sem=over_send.at[b % 3, kind], recv_sem=over_recv.at[b % 3, kind], device_id={"states": other}, device_id_type=MESH)

    def turn(b, kind, owner):
        ref = rows_hbm.at[owner, pl.ds(seq * half + b * piece, piece)]
        return pltpu.make_async_remote_copy(
            src_ref=ref, dst_ref=ref, send_sem=turn_send.at[b % 2, kind], recv_sem=turn_recv.at[kind],
            device_id={"seqs": 1 - seq}, device_id_type=MESH)

    def near(b):
        return pltpu.make_async_remote_copy(
            src_ref=a_hbm.at[pl.ds(partner * block + b * 2 * piece, 2 * piece)], dst_ref=rows_hbm.at[me, pl.ds(b * 2 * piece, 2 * piece)],
            send_sem=near_send.at[b % 2], recv_sem=near_recv, device_id={"states": partner}, device_id_type=MESH)

    def rows_start(b):
        for kind, other in others:
            over(b, kind, me, other).start()
        near(b).start()

    def rows_turn(b):
        near(b).wait_send()
        for kind, other in others:
            over(b, kind, me, other).wait_send()
            over(b, kind, other, other).wait_recv()
            turn(b, kind, other).start()

    def rows_end(b):
        for kind, other in others:
            turn(b, kind, other).wait_send()

    def norm_copy(owner, kind, device):
        return pltpu.make_async_remote_copy(
            src_ref=cbuf.at[owner], dst_ref=cbuf.at[owner], send_sem=csend_sem.at[kind], recv_sem=crecv_sem.at[kind],
            device_id={"states": device}, device_id_type=MESH)

    everyone = tuple(enumerate((far, cross, partner)))

    def norm_start(sums):
        cbuf[me] = packed(jnp.sum(sums, axis=1, keepdims=True))
        for kind, other in everyone:
            norm_copy(me, kind, other).start()

    def norm_end():
        for kind, other in everyone:
            norm_copy(other, kind, other).wait_recv()
        for kind, other in everyone:
            norm_copy(me, kind, other).wait_send()
        return cbuf[0] + cbuf[1] + cbuf[2] + cbuf[3]

    def body():
        ex = Exchange(me, FORWARD_COPIES, xbuf, mat, acc, send_sem, recv_sem)
        ends = {(lo + size) // TILE - 1: k for k, (lo, size) in enumerate(ex.pieces)}

        def finish_step(t, total):
            inv = jnp.broadcast_to(unpacked(1.0 / total), (seqs, TILE))
            live = t < jnp.broadcast_to(len_col[...], (seqs, TILE))
            for n in range(chunks):
                alpha = jnp.where(live, acc[:seqs, cols(n)] * inv, post_ref[:, cols(n)])
                post_ref[:, cols(n)] = alpha
                low = alpha.astype(jnp.bfloat16)
                xbuf[t % SLOTS, me, :, cols(n)] = low
                hist_ref[(t + 1) % steps, :, cols(n)] = low
                if n in ends:
                    ex.send(t % SLOTS, ends[n], t < steps - 1)

        def fold(n, mass, sums):
            acc[:seqs, cols(n)] = mass
            return sums + mass[:, :128] + mass[:, 128:]

        sums = jnp.zeros((seqs, 128), jnp.float32)
        for n in range(chunks):
            sums = fold(n, init_ref[:, cols(n)] * emit_ref[0, :, cols(n)].astype(jnp.float32), sums)
        norm_start(sums)
        rows_start(0)
        post_ref[...] = jnp.zeros_like(post_ref)
        total = norm_end()
        scale_ref[0] = total
        log_ref[...] = jnp.log(total)
        finish_step(0, total)
        for load in loads:
            load.wait()

        def step(t, carry):
            slot = (t - 1) % SLOTS

            ex.run(slot, lambda: rows_start(t))
            sums = jnp.zeros((seqs, 128), jnp.float32)
            for n in range(chunks):
                sums = fold(n, acc[:seqs, cols(n)] * emit_ref[t, :, cols(n)].astype(jnp.float32), sums)
            norm_start(sums)
            rows_turn(t - 1)

            @pl.when(t > 1)
            def _():
                rows_end(t - 2)
                ex.wait_sends((t - 2) % SLOTS)

            total = norm_end()
            finish_step(t, total)
            scale = jnp.where(t < len_pack[...], total, 1.0)
            scale_ref[t] = scale
            log_ref[...] += jnp.log(scale)
            return carry

        lax.fori_loop(1, steps, step, 0)
        ex.wait_sends((steps - 2) % SLOTS)

    body()
    rows_turn(steps - 1)
    rows_end(steps - 2)
    rows_end(steps - 1)

    def landed(ref, sem):
        pltpu.make_async_copy(ref, ref, sem).wait()

    for kind, other in others:
        landed(rows_hbm.at[other, pl.ds((1 - seq) * half, half)], turn_recv.at[kind])
    landed(rows_hbm.at[partner], near_recv)


def forward(emit_seq, init_loc, col, pack, trans_loc):
    steps, seqs, block = emit_seq.shape
    full = trans_loc.shape[0]
    vmem, hbm = pl.BlockSpec(memory_space=pltpu.VMEM), pl.BlockSpec(memory_space=pltpu.HBM)
    dma = pltpu.SemaphoreType.DMA
    return pl.pallas_call(
        forward_kernel,
        out_shape=[
            jax.ShapeDtypeStruct((steps, seqs, block), jnp.bfloat16),
            jax.ShapeDtypeStruct((steps, 8, 128), jnp.float32),
            jax.ShapeDtypeStruct((8, 128), jnp.float32),
            jax.ShapeDtypeStruct((seqs, block), jnp.float32),
            jax.ShapeDtypeStruct((full // block, block, block), jnp.bfloat16),
        ],
        in_specs=[vmem] * 4 + [hbm],
        out_specs=[vmem] * 4 + [hbm],
        scratch_shapes=[
            pltpu.VMEM((full, block), jnp.bfloat16),
            pltpu.VMEM((SLOTS, 4, seqs, block), jnp.bfloat16),
            pltpu.VMEM((FORWARD_COPIES * seqs, block), jnp.float32),
            pltpu.VMEM((4, 8, 128), jnp.float32),
            dma((LOADS,)), dma((SLOTS, 3, 5)), dma((SLOTS, 3, 5)), dma((3,)), dma((3,)),
            dma((3, 2)), dma((3, 2)), dma((2, 2)), dma((2,)), dma((2,)), dma,
        ],
        compiler_params=pltpu.CompilerParams(collective_id=0, has_side_effects=True, vmem_limit_bytes=60 * 1024 * 1024),
        name="forward",
    )(emit_seq, init_loc[None, :], col, pack, trans_loc)


def backward_kernel(emit_ref, scale_ref, len_col, a_hbm, rows_hbm, hist_ref, mat, xbuf, coef, acc, load_sem, send_sem, recv_sem):
    me = lax.axis_index("states")
    partner, cross, far = me + 1 - 2 * (me % 2), 3 - me, (me + 2) % 4
    steps, seqs, block = emit_ref.shape
    chunks = block // TILE
    owners = (me, partner, cross, far)
    loads = []
    for k, owner in enumerate(owners):
        src = a_hbm.at[pl.ds(me * block, block)] if k == 0 else rows_hbm.at[owner]
        loads.append(pltpu.make_async_copy(src, mat.at[pl.ds(owner * block, block)], load_sem.at[k]))
        loads[-1].start()
    entry_barrier([{"states": partner}, {"states": cross}, {"states": far}])

    def weigh(t):
        inv = jnp.where(t < len_col[...], unpacked(1.0 / scale_ref[t]), 0.0)
        coef[...] = emit_ref[t].astype(jnp.float32) * inv

    weigh(steps - 1)
    hist_ref[0] = jnp.zeros(hist_ref.shape[1:], hist_ref.dtype)

    def flips():
        side = block // TILE
        for owner, load in zip(owners, loads):
            load.wait()

            def flip_row(r, carry):
                def flip(c, inner):
                    def tile(p, q):
                        return pl.ds(pl.multiple_of(owner * block + p * TILE, TILE), TILE), pl.ds(pl.multiple_of(q * TILE, TILE), TILE)

                    upper, lower = mat[tile(r, c)], mat[tile(c, r)]
                    mat[tile(r, c)] = lower.T
                    mat[tile(c, r)] = upper.T
                    return inner

                return lax.fori_loop(r, side, flip, carry)

            lax.fori_loop(0, side, flip_row, 0)

    def body():
        ex = Exchange(me, BACKWARD_COPIES, xbuf, mat, acc, send_sem, recv_sem)
        ends = {(lo + size) // TILE - 1: k for k, (lo, size) in enumerate(ex.pieces)}

        def emit_weight(t, n, weight):
            low = weight.astype(jnp.bfloat16)
            xbuf[t % SLOTS, me, :, cols(n)] = low
            hist_ref[t, :, cols(n)] = low
            if n in ends:
                ex.send(t % SLOTS, ends[n], t > 1)

        for n in range(chunks):
            emit_weight(steps - 1, n, coef[:, cols(n)])
        flips()

        def step(k, carry):
            t = steps - 1 - k
            weigh(t - 1)

            ex.run(t % SLOTS, lambda: None)
            dead = jnp.where(t < jnp.broadcast_to(len_col[...], (seqs, TILE)), 0.0, 1.0)
            for n in range(chunks):
                emit_weight(t - 1, n, coef[:, cols(n)] * (acc[:seqs, cols(n)] + dead))

            @pl.when(k > 0)
            def _():
                ex.wait_sends((t + 1) % SLOTS)

            return carry

        lax.fori_loop(0, steps - 2, step, 0)
        ex.wait_sends(2 % SLOTS)

    body()


def backward(emit_seq, scales, col, trans_loc, rows_loc):
    steps, seqs, block = emit_seq.shape
    full = trans_loc.shape[0]
    vmem, hbm = pl.BlockSpec(memory_space=pltpu.VMEM), pl.BlockSpec(memory_space=pltpu.HBM)
    dma = pltpu.SemaphoreType.DMA
    return pl.pallas_call(
        backward_kernel,
        out_shape=jax.ShapeDtypeStruct((steps, seqs, block), jnp.bfloat16),
        in_specs=[vmem] * 3 + [hbm] * 2,
        out_specs=vmem,
        scratch_shapes=[
            pltpu.VMEM((full, block), jnp.bfloat16),
            pltpu.VMEM((SLOTS, 4, seqs, block), jnp.bfloat16),
            pltpu.VMEM((seqs, block), jnp.float32),
            pltpu.VMEM((BACKWARD_COPIES * seqs, block), jnp.float32),
            dma((4,)), dma((SLOTS, 3, 5)), dma((SLOTS, 3, 5)),
        ],
        compiler_params=pltpu.CompilerParams(collective_id=1, has_side_effects=True, vmem_limit_bytes=60 * 1024 * 1024),
        name="backward",
    )(emit_seq, scales, col, trans_loc, rows_loc)


AHEAD = 6
ROWS = 8


def gather_kernel(tok_smem, tok_ref, emit_hbm, out_ref, buf, sem):
    t = pl.program_id(0)
    seqs, steps = tok_ref.shape

    def copies(step):
        slot = step % AHEAD
        return [pltpu.make_async_copy(
            emit_hbm.at[pl.ds(pl.multiple_of(tok_smem[b, step] // ROWS * ROWS, ROWS), ROWS)],
            buf.at[slot, pl.ds(b * ROWS, ROWS)], sem.at[slot, b]) for b in range(seqs)]

    @pl.when(t == 0)
    def _():
        for step in range(min(AHEAD - 1, steps)):
            for c in copies(step):
                c.start()

    @pl.when(t + AHEAD - 1 < steps)
    def _():
        for c in copies(t + AHEAD - 1):
            c.start()

    for c in copies(t):
        c.wait()
    lane = lax.broadcasted_iota(jnp.int32, tok_ref.shape, 1)
    token = jnp.sum(jnp.where(lane == t, tok_ref[...], 0).astype(jnp.float32), axis=1, keepdims=True).astype(jnp.int32)
    wide = (seqs, seqs * ROWS)
    pick = lax.broadcasted_iota(jnp.int32, wide, 0) * ROWS + jnp.broadcast_to(token % ROWS, wide)
    chosen = jnp.where(lax.broadcasted_iota(jnp.int32, wide, 1) == pick, 1.0, 0.0).astype(jnp.bfloat16)
    out_ref[0] = jnp.dot(chosen, buf[t % AHEAD], preferred_element_type=jnp.float32).astype(jnp.bfloat16)


def gather(emit_loc, tokens_loc):
    seqs, steps = tokens_loc.shape
    block = emit_loc.shape[0]
    return pl.pallas_call(
        gather_kernel,
        grid=(steps,),
        out_shape=jax.ShapeDtypeStruct((steps, seqs, block), jnp.bfloat16),
        in_specs=[pl.BlockSpec(memory_space=pltpu.SMEM), pl.BlockSpec(memory_space=pltpu.VMEM), pl.BlockSpec(memory_space=pltpu.HBM)],
        out_specs=pl.BlockSpec((1, seqs, block), lambda t: (t, 0, 0)),
        scratch_shapes=[pltpu.VMEM((AHEAD, seqs * ROWS, block), jnp.bfloat16), pltpu.SemaphoreType.DMA((AHEAD, seqs))],
        compiler_params=pltpu.CompilerParams(dimension_semantics=("arbitrary",), vmem_limit_bytes=32 * 1024 * 1024),
        name="gather",
    )(tokens_loc, tokens_loc, emit_loc.T)


def solution(mesh):
    def local_run(trans_loc, emit_loc, init_loc, tokens_loc, lengths_loc):
        seqs, steps = tokens_loc.shape
        block = trans_loc.shape[1]
        emit_seq = gather(emit_loc, tokens_loc)
        col = lengths_loc[:, None]
        pack = jnp.broadcast_to(lengths_loc.reshape(4, 8).T[:, :, None], (8, 4, 32)).reshape(8, 128)
        alphas, scales, log_sum, last, rows_loc = forward(emit_seq, init_loc, col, pack, trans_loc)
        weights = backward(emit_seq, scales, col, trans_loc, rows_loc)
        pair_sum = lax.dot_general(alphas.reshape(steps * seqs, block), weights.reshape(steps * seqs, block), (((0,), (0,)), ((), ())), preferred_element_type=jnp.float32)
        diag_block = lax.dynamic_slice_in_dim(trans_loc, lax.axis_index('states') * block, block, axis=0)
        counts = diag_block.astype(jnp.float32) * pair_sum
        return log_sum[:, ::32].T.reshape(seqs), last, counts

    return jax.shard_map(local_run, mesh=mesh, in_specs=(P(None, 'states'), P('states', None), P('states'), P('seqs', None), P('seqs')), out_specs=(P('seqs'), P('seqs', 'states'), P(('seqs', 'states'), None)), check_vma=False)
```

```python
import jax
import jax.numpy as jnp
from jax import lax
from jax.experimental import pallas as pl
from jax.experimental.pallas import tpu as pltpu
from jax.sharding import PartitionSpec as P

MESH = pl.DeviceIdType.MESH
LOADS = 8
TILE = 256
SLOTS = 4
FORWARD_COPIES = 1
BACKWARD_COPIES = 4
ORDER = (
    "WP0", "P0", "P1", "P2", "R0", "P3", "C0", "R1", "C1", "WF0", "F0", "R2", "C2", "WF1", "R3", "C3", "R4", "F1", "C4", "WF2", "F2",
    "WF3", "WF4", "F3", "F4")


def entry_barrier(others):
    barrier = pltpu.get_barrier_semaphore()
    for other in others:
        pl.semaphore_signal(barrier, inc=1, device_id=other, device_id_type=MESH)
    pl.semaphore_wait(barrier, len(others))


def cols(c):
    return pl.ds(c * TILE, TILE)


class Exchange:
    def __init__(self, me, copies, xbuf, mat, acc, send_sem, recv_sem):
        self.copies = copies
        self.me, self.xbuf, self.mat, self.acc = me, xbuf, mat, acc
        self.send_sem, self.recv_sem = send_sem, recv_sem
        self.block = xbuf.shape[3]
        self.partner = me + 1 - 2 * (me % 2)
        self.cross = 3 - me
        self.far = (me + 2) % 4
        quarter = self.block // 4
        self.pieces = [(k * quarter, quarter) for k in range(3)] + [(3 * quarter, quarter // 2), (3 * quarter + quarter // 2, quarter // 2)]

    def copy(self, slot, owner, k, kind, device):
        lo, size = self.pieces[k]
        ref = self.xbuf.at[slot, owner, :, pl.ds(lo, size)]
        return pltpu.make_async_remote_copy(
            src_ref=ref, dst_ref=ref, send_sem=self.send_sem.at[slot, kind, k], recv_sem=self.recv_sem.at[slot, kind, k],
            device_id={"states": device}, device_id_type=MESH)

    def send(self, slot, k, more):
        @pl.when(more)
        def _():
            self.copy(slot, self.me, k, 1, self.cross).start()
            self.copy(slot, self.me, k, 0, self.partner).start()

    def wait_sends(self, slot):
        for k in range(len(self.pieces)):
            self.copy(slot, self.me, k, 1, self.cross).wait_send()
            self.copy(slot, self.me, k, 0, self.partner).wait_send()
            self.copy(slot, self.cross, k, 2, self.partner).wait_send()

    def product(self, slot, owner, lo, size, first=False, copies=1):
        lhs = self.xbuf[slot, owner, :, pl.ds(lo, size)]
        rows = pl.ds(pl.multiple_of(owner * self.block + lo, 128), size)
        prod = jnp.dot(jnp.concatenate([lhs] * copies, axis=0), self.mat[rows, :], preferred_element_type=jnp.float32)
        out = self.acc.at[:copies * lhs.shape[0]]
        out[...] = prod if first else out[...] + prod

    def run(self, slot, meanwhile):
        meanwhile()
        self.product(slot, self.me, 0, self.block, True, self.copies)
        for token in ORDER:
            what, k = token[:-1], int(token[-1])
            if what == "WP":
                for j in range(len(self.pieces)):
                    self.copy(slot, self.partner, j, 0, self.partner).wait_recv()
            elif what == "P":
                self.product(slot, self.partner, k * (self.block // 4), self.block // 4, copies=self.copies)
            elif what == "R":
                self.copy(slot, self.cross, k, 1, self.cross).wait_recv()
                self.copy(slot, self.cross, k, 2, self.partner).start()
            elif what == "WF":
                self.copy(slot, self.far, k, 2, self.partner).wait_recv()
            else:
                lo, size = self.pieces[k]
                self.product(slot, self.cross if what == "C" else self.far, lo, size)


def packed(col):
    group = lax.broadcasted_iota(jnp.int32, (8, 128), 1) // 32
    out = jnp.broadcast_to(col[24:32], (8, 128))
    for k in range(3):
        out = jnp.where(group == k, jnp.broadcast_to(col[8 * k:8 * k + 8], (8, 128)), out)
    return out


def unpacked(tile):
    return jnp.concatenate([tile[:, 32 * k:32 * k + 1] for k in range(4)], axis=0)


def forward_kernel(emit_ref, init_ref, len_col, len_pack, a_hbm, hist_ref, scale_ref, log_ref, post_ref, rows_hbm,
                   mat, xbuf, acc, cbuf, load_sem, send_sem, recv_sem, csend_sem, crecv_sem,
                   over_send, over_recv, turn_send, turn_recv, near_send, near_recv):
    me, seq = lax.axis_index("states"), lax.axis_index("seqs")
    partner, cross, far = me + 1 - 2 * (me % 2), 3 - me, (me + 2) % 4
    steps, seqs, block = emit_ref.shape
    chunks = block // TILE
    rows = mat.shape[0] // LOADS
    loads = [pltpu.make_async_copy(a_hbm.at[pl.ds(k * rows, rows)], mat.at[pl.ds(k * rows, rows)], load_sem.at[k]) for k in range(LOADS)]
    for load in loads:
        load.start()
    entry_barrier([{"states": partner}, {"states": cross}, {"states": far}, {"seqs": 1 - seq}])

    half = block // 2
    piece = half // steps
    others = ((0, cross), (1, far))

    def over(b, kind, owner, other):
        lo = seq * half + b * piece
        return pltpu.make_async_remote_copy(
            src_ref=a_hbm.at[pl.ds(other * block + lo, piece)], dst_ref=rows_hbm.at[owner, pl.ds(lo, piece)],
            send_sem=over_send.at[b % 3, kind], recv_sem=over_recv.at[b % 3, kind], device_id={"states": other}, device_id_type=MESH)

    def turn(b, kind, owner):
        ref = rows_hbm.at[owner, pl.ds(seq * half + b * piece, piece)]
        return pltpu.make_async_remote_copy(
            src_ref=ref, dst_ref=ref, send_sem=turn_send.at[b % 2, kind], recv_sem=turn_recv.at[kind],
            device_id={"seqs": 1 - seq}, device_id_type=MESH)

    def near(b):
        return pltpu.make_async_remote_copy(
            src_ref=a_hbm.at[pl.ds(partner * block + b * 2 * piece, 2 * piece)], dst_ref=rows_hbm.at[me, pl.ds(b * 2 * piece, 2 * piece)],
            send_sem=near_send.at[b % 2], recv_sem=near_recv, device_id={"states": partner}, device_id_type=MESH)

    def rows_start(b):
        for kind, other in others:
            over(b, kind, me, other).start()
        near(b).start()

    def rows_turn(b):
        near(b).wait_send()
        for kind, other in others:
            over(b, kind, me, other).wait_send()
            over(b, kind, other, other).wait_recv()
            turn(b, kind, other).start()

    def rows_end(b):
        for kind, other in others:
            turn(b, kind, other).wait_send()

    def norm_copy(owner, kind, device):
        return pltpu.make_async_remote_copy(
            src_ref=cbuf.at[owner], dst_ref=cbuf.at[owner], send_sem=csend_sem.at[kind], recv_sem=crecv_sem.at[kind],
            device_id={"states": device}, device_id_type=MESH)

    everyone = tuple(enumerate((far, cross, partner)))

    def norm_start(sums):
        cbuf[me] = packed(jnp.sum(sums, axis=1, keepdims=True))
        for kind, other in everyone:
            norm_copy(me, kind, other).start()

    def norm_end():
        for kind, other in everyone:
            norm_copy(other, kind, other).wait_recv()
        for kind, other in everyone:
            norm_copy(me, kind, other).wait_send()
        return cbuf[0] + cbuf[1] + cbuf[2] + cbuf[3]

    def body():
        ex = Exchange(me, FORWARD_COPIES, xbuf, mat, acc, send_sem, recv_sem)
        ends = {(lo + size) // TILE - 1: k for k, (lo, size) in enumerate(ex.pieces)}

        def finish_step(t, total):
            inv = jnp.broadcast_to(unpacked(1.0 / total), (seqs, TILE))
            live = t < jnp.broadcast_to(len_col[...], (seqs, TILE))
            for n in range(chunks):
                alpha = jnp.where(live, acc[:seqs, cols(n)] * inv, post_ref[:, cols(n)])
                post_ref[:, cols(n)] = alpha
                low = alpha.astype(jnp.bfloat16)
                xbuf[t % SLOTS, me, :, cols(n)] = low
                hist_ref[(t + 1) % steps, :, cols(n)] = low
                if n in ends:
                    ex.send(t % SLOTS, ends[n], t < steps - 1)

        def fold(n, mass, sums):
            acc[:seqs, cols(n)] = mass
            return sums + mass[:, :128] + mass[:, 128:]

        sums = jnp.zeros((seqs, 128), jnp.float32)
        for n in range(chunks):
            sums = fold(n, init_ref[:, cols(n)] * emit_ref[0, :, cols(n)].astype(jnp.float32), sums)
        norm_start(sums)
        rows_start(0)
        post_ref[...] = jnp.zeros_like(post_ref)
        total = norm_end()
        scale_ref[0] = total
        log_ref[...] = jnp.log(total)
        finish_step(0, total)
        for load in loads:
            load.wait()

        def step(t, carry):
            slot = (t - 1) % SLOTS

            ex.run(slot, lambda: rows_start(t))
            sums = jnp.zeros((seqs, 128), jnp.float32)
            for n in range(chunks):
                sums = fold(n, acc[:seqs, cols(n)] * emit_ref[t, :, cols(n)].astype(jnp.float32), sums)
            norm_start(sums)
            rows_turn(t - 1)

            @pl.when(t > 1)
            def _():
                rows_end(t - 2)
                ex.wait_sends((t - 2) % SLOTS)

            total = norm_end()
            finish_step(t, total)
            scale = jnp.where(t < len_pack[...], total, 1.0)
            scale_ref[t] = scale
            log_ref[...] += jnp.log(scale)
            return carry

        lax.fori_loop(1, steps, step, 0)
        ex.wait_sends((steps - 2) % SLOTS)

    body()
    rows_turn(steps - 1)
    rows_end(steps - 2)
    rows_end(steps - 1)

    def landed(ref, sem):
        pltpu.make_async_copy(ref, ref, sem).wait()

    for kind, other in others:
        landed(rows_hbm.at[other, pl.ds((1 - seq) * half, half)], turn_recv.at[kind])
    landed(rows_hbm.at[partner], near_recv)


def forward(emit_seq, init_loc, col, pack, trans_loc):
    steps, seqs, block = emit_seq.shape
    full = trans_loc.shape[0]
    vmem, hbm = pl.BlockSpec(memory_space=pltpu.VMEM), pl.BlockSpec(memory_space=pltpu.HBM)
    dma = pltpu.SemaphoreType.DMA
    return pl.pallas_call(
        forward_kernel,
        out_shape=[
            jax.ShapeDtypeStruct((steps, seqs, block), jnp.bfloat16),
            jax.ShapeDtypeStruct((steps, 8, 128), jnp.float32),
            jax.ShapeDtypeStruct((8, 128), jnp.float32),
            jax.ShapeDtypeStruct((seqs, block), jnp.float32),
            jax.ShapeDtypeStruct((full // block, block, block), jnp.bfloat16),
        ],
        in_specs=[vmem] * 4 + [hbm],
        out_specs=[vmem] * 4 + [hbm],
        scratch_shapes=[
            pltpu.VMEM((full, block), jnp.bfloat16),
            pltpu.VMEM((SLOTS, 4, seqs, block), jnp.bfloat16),
            pltpu.VMEM((FORWARD_COPIES * seqs, block), jnp.float32),
            pltpu.VMEM((4, 8, 128), jnp.float32),
            dma((LOADS,)), dma((SLOTS, 3, 5)), dma((SLOTS, 3, 5)), dma((3,)), dma((3,)),
            dma((3, 2)), dma((3, 2)), dma((2, 2)), dma((2,)), dma((2,)), dma,
        ],
        compiler_params=pltpu.CompilerParams(collective_id=0, has_side_effects=True, vmem_limit_bytes=60 * 1024 * 1024),
        name="forward",
    )(emit_seq, init_loc[None, :], col, pack, trans_loc)


def backward_kernel(emit_ref, scale_ref, len_col, a_hbm, rows_hbm, hist_ref, mat, xbuf, coef, acc, load_sem, send_sem, recv_sem):
    me = lax.axis_index("states")
    partner, cross, far = me + 1 - 2 * (me % 2), 3 - me, (me + 2) % 4
    steps, seqs, block = emit_ref.shape
    chunks = block // TILE
    owners = (me, partner, cross, far)
    loads = []
    for k, owner in enumerate(owners):
        src = a_hbm.at[pl.ds(me * block, block)] if k == 0 else rows_hbm.at[owner]
        loads.append(pltpu.make_async_copy(src, mat.at[pl.ds(owner * block, block)], load_sem.at[k]))
        loads[-1].start()
    entry_barrier([{"states": partner}, {"states": cross}, {"states": far}])

    def weigh(t):
        inv = jnp.where(t < len_col[...], unpacked(1.0 / scale_ref[t]), 0.0)
        coef[...] = emit_ref[t].astype(jnp.float32) * inv

    weigh(steps - 1)
    hist_ref[0] = jnp.zeros(hist_ref.shape[1:], hist_ref.dtype)

    def flips():
        side = block // TILE
        for owner, load in zip(owners, loads):
            load.wait()

            def flip_row(r, carry):
                def flip(c, inner):
                    def tile(p, q):
                        return pl.ds(pl.multiple_of(owner * block + p * TILE, TILE), TILE), pl.ds(pl.multiple_of(q * TILE, TILE), TILE)

                    upper, lower = mat[tile(r, c)], mat[tile(c, r)]
                    mat[tile(r, c)] = lower.T
                    mat[tile(c, r)] = upper.T
                    return inner

                return lax.fori_loop(r, side, flip, carry)

            lax.fori_loop(0, side, flip_row, 0)

    def body():
        ex = Exchange(me, BACKWARD_COPIES, xbuf, mat, acc, send_sem, recv_sem)
        ends = {(lo + size) // TILE - 1: k for k, (lo, size) in enumerate(ex.pieces)}

        def emit_weight(t, n, weight):
            low = weight.astype(jnp.bfloat16)
            xbuf[t % SLOTS, me, :, cols(n)] = low
            hist_ref[t, :, cols(n)] = low
            if n in ends:
                ex.send(t % SLOTS, ends[n], t > 1)

        for n in range(chunks):
            emit_weight(steps - 1, n, coef[:, cols(n)])
        flips()

        def step(k, carry):
            t = steps - 1 - k
            weigh(t - 1)

            ex.run(t % SLOTS, lambda: None)
            dead = jnp.where(t < jnp.broadcast_to(len_col[...], (seqs, TILE)), 0.0, 1.0)
            for n in range(chunks):
                emit_weight(t - 1, n, coef[:, cols(n)] * (acc[:seqs, cols(n)] + dead))

            @pl.when(k > 0)
            def _():
                ex.wait_sends((t + 1) % SLOTS)

            return carry

        lax.fori_loop(0, steps - 2, step, 0)
        ex.wait_sends(2 % SLOTS)

    body()


def backward(emit_seq, scales, col, trans_loc, rows_loc):
    steps, seqs, block = emit_seq.shape
    full = trans_loc.shape[0]
    vmem, hbm = pl.BlockSpec(memory_space=pltpu.VMEM), pl.BlockSpec(memory_space=pltpu.HBM)
    dma = pltpu.SemaphoreType.DMA
    return pl.pallas_call(
        backward_kernel,
        out_shape=jax.ShapeDtypeStruct((steps, seqs, block), jnp.bfloat16),
        in_specs=[vmem] * 3 + [hbm] * 2,
        out_specs=vmem,
        scratch_shapes=[
            pltpu.VMEM((full, block), jnp.bfloat16),
            pltpu.VMEM((SLOTS, 4, seqs, block), jnp.bfloat16),
            pltpu.VMEM((seqs, block), jnp.float32),
            pltpu.VMEM((BACKWARD_COPIES * seqs, block), jnp.float32),
            dma((4,)), dma((SLOTS, 3, 5)), dma((SLOTS, 3, 5)),
        ],
        compiler_params=pltpu.CompilerParams(collective_id=1, has_side_effects=True, vmem_limit_bytes=60 * 1024 * 1024),
        name="backward",
    )(emit_seq, scales, col, trans_loc, rows_loc)


AHEAD = 6
ROWS = 8


def gather_kernel(tok_smem, tok_ref, emit_hbm, out_ref, buf, sem):
    t = pl.program_id(0)
    seqs, steps = tok_ref.shape

    def copies(step):
        slot = step % AHEAD
        return [pltpu.make_async_copy(
            emit_hbm.at[pl.ds(pl.multiple_of(tok_smem[b, step] // ROWS * ROWS, ROWS), ROWS)],
            buf.at[slot, pl.ds(b * ROWS, ROWS)], sem.at[slot]) for b in range(seqs)]

    @pl.when(t == 0)
    def _():
        for step in range(min(AHEAD - 1, steps)):
            for c in copies(step):
                c.start()

    @pl.when(t + AHEAD - 1 < steps)
    def _():
        for c in copies(t + AHEAD - 1):
            c.start()

    landed = buf.at[t % AHEAD]
    pltpu.make_async_copy(landed, landed, sem.at[t % AHEAD]).wait()
    lane = lax.broadcasted_iota(jnp.int32, tok_ref.shape, 1)
    token = jnp.sum(jnp.where(lane == t, tok_ref[...], 0).astype(jnp.float32), axis=1, keepdims=True).astype(jnp.int32)
    wide = (seqs, seqs * ROWS)
    pick = lax.broadcasted_iota(jnp.int32, wide, 0) * ROWS + jnp.broadcast_to(token % ROWS, wide)
    chosen = jnp.where(lax.broadcasted_iota(jnp.int32, wide, 1) == pick, 1.0, 0.0).astype(jnp.bfloat16)
    out_ref[0] = jnp.dot(chosen, buf[t % AHEAD], preferred_element_type=jnp.float32).astype(jnp.bfloat16)


def gather(emit_loc, tokens_loc):
    seqs, steps = tokens_loc.shape
    block = emit_loc.shape[0]
    return pl.pallas_call(
        gather_kernel,
        grid=(steps,),
        out_shape=jax.ShapeDtypeStruct((steps, seqs, block), jnp.bfloat16),
        in_specs=[pl.BlockSpec(memory_space=pltpu.SMEM), pl.BlockSpec(memory_space=pltpu.VMEM), pl.BlockSpec(memory_space=pltpu.HBM)],
        out_specs=pl.BlockSpec((1, seqs, block), lambda t: (t, 0, 0)),
        scratch_shapes=[pltpu.VMEM((AHEAD, seqs * ROWS, block), jnp.bfloat16), pltpu.SemaphoreType.DMA((AHEAD,))],
        compiler_params=pltpu.CompilerParams(dimension_semantics=("arbitrary",), vmem_limit_bytes=32 * 1024 * 1024),
        name="gather",
    )(tokens_loc, tokens_loc, emit_loc.T)


def solution(mesh):
    def local_run(trans_loc, emit_loc, init_loc, tokens_loc, lengths_loc):
        seqs, steps = tokens_loc.shape
        block = trans_loc.shape[1]
        emit_seq = gather(emit_loc, tokens_loc)
        col = lengths_loc[:, None]
        pack = jnp.broadcast_to(lengths_loc.reshape(4, 8).T[:, :, None], (8, 4, 32)).reshape(8, 128)
        alphas, scales, log_sum, last, rows_loc = forward(emit_seq, init_loc, col, pack, trans_loc)
        weights = backward(emit_seq, scales, col, trans_loc, rows_loc)
        pair_sum = lax.dot_general(alphas.reshape(steps * seqs, block), weights.reshape(steps * seqs, block), (((0,), (0,)), ((), ())), preferred_element_type=jnp.float32)
        diag_block = lax.dynamic_slice_in_dim(trans_loc, lax.axis_index('states') * block, block, axis=0)
        counts = diag_block.astype(jnp.float32) * pair_sum
        return log_sum[:, ::32].T.reshape(seqs), last, counts

    return jax.shard_map(local_run, mesh=mesh, in_specs=(P(None, 'states'), P('states', None), P('states'), P('seqs', None), P('seqs')), out_specs=(P('seqs'), P('seqs', 'states'), P(('seqs', 'states'), None)), check_vma=False)
```

```python
import jax
import jax.numpy as jnp
from jax import lax
from jax.experimental import pallas as pl
from jax.experimental.pallas import tpu as pltpu
from jax.sharding import PartitionSpec as P

MESH = pl.DeviceIdType.MESH
TILE = 256
SLOTS = 4
FORWARD_COPIES = 4
BACKWARD_COPIES = 4
ORDER = (
    "WP0", "P0", "P1", "P2", "R0", "P3", "C0", "R1", "C1", "WF0", "F0", "R2", "C2", "WF1", "R3", "C3", "R4", "F1", "C4", "WF2", "F2",
    "WF3", "WF4", "F3", "F4")


def entry_barrier(others):
    barrier = pltpu.get_barrier_semaphore()
    for other in others:
        pl.semaphore_signal(barrier, inc=1, device_id=other, device_id_type=MESH)
    pl.semaphore_wait(barrier, len(others))


def cols(c):
    return pl.ds(c * TILE, TILE)


class Exchange:
    def __init__(self, me, copies, xbuf, mat, acc, send_sem, recv_sem, hist, hist_sem):
        self.hist, self.hist_sem = hist, hist_sem
        self.copies = copies
        self.me, self.xbuf, self.mat, self.acc = me, xbuf, mat, acc
        self.send_sem, self.recv_sem = send_sem, recv_sem
        self.block = xbuf.shape[3]
        self.partner = me + 1 - 2 * (me % 2)
        self.cross = 3 - me
        self.far = (me + 2) % 4
        quarter = self.block // 4
        self.pieces = [(k * quarter, quarter) for k in range(3)] + [(3 * quarter, quarter // 2), (3 * quarter + quarter // 2, quarter // 2)]

    def copy(self, slot, owner, k, kind, device):
        lo, size = self.pieces[k]
        ref = self.xbuf.at[slot, owner, :, pl.ds(lo, size)]
        return pltpu.make_async_remote_copy(
            src_ref=ref, dst_ref=ref, send_sem=self.send_sem.at[slot, kind, k], recv_sem=self.recv_sem.at[slot, kind, k],
            device_id={"states": device}, device_id_type=MESH)

    def send(self, slot, k, more):
        @pl.when(more)
        def _():
            self.copy(slot, self.me, k, 1, self.cross).start()
            self.copy(slot, self.me, k, 0, self.partner).start()

    def keep(self, slot, t):
        return pltpu.make_async_copy(self.xbuf.at[slot, self.me], self.hist.at[t], self.hist_sem.at[slot])

    def wait_sends(self, slot):
        self.keep(slot, 0).wait()
        for k in range(len(self.pieces)):
            self.copy(slot, self.me, k, 1, self.cross).wait_send()
            self.copy(slot, self.me, k, 0, self.partner).wait_send()
            self.copy(slot, self.cross, k, 2, self.partner).wait_send()

    def product(self, slot, owner, lo, size, first=False, copies=1):
        lhs = self.xbuf[slot, owner, :, pl.ds(lo, size)]
        rows = pl.ds(pl.multiple_of(owner * self.block + lo, 128), size)
        prod = jnp.dot(jnp.concatenate([lhs] * copies, axis=0), self.mat[rows, :], preferred_element_type=jnp.float32)
        out = self.acc.at[:copies * lhs.shape[0]]
        out[...] = prod if first else out[...] + prod

    def run(self, slot, meanwhile, ready=lambda k: None):
        meanwhile()
        ready(0)
        self.product(slot, self.me, 0, self.block, True, self.copies)
        for i, token in enumerate(ORDER):
            what, k = token[:-1], int(token[-1])
            if token in ("WP0", "R0", "WF0"):
                ready(("WP0", "R0", "WF0").index(token) + 1)
            if what == "WP":
                for j in range(len(self.pieces)):
                    self.copy(slot, self.partner, j, 0, self.partner).wait_recv()
            elif what == "P":
                self.product(slot, self.partner, k * (self.block // 4), self.block // 4, copies=self.copies)
            elif what == "R":
                self.copy(slot, self.cross, k, 1, self.cross).wait_recv()
                self.copy(slot, self.cross, k, 2, self.partner).start()
            elif what == "WF":
                self.copy(slot, self.far, k, 2, self.partner).wait_recv()
            else:
                lo, size = self.pieces[k]
                long = size == self.block // 4 and i < len(ORDER) - 2
                self.product(slot, self.cross if what == "C" else self.far, lo, size, copies=self.copies if long else 1)


def packed(col):
    group = lax.broadcasted_iota(jnp.int32, (8, 128), 1) // 32
    out = jnp.broadcast_to(col[24:32], (8, 128))
    for k in range(3):
        out = jnp.where(group == k, jnp.broadcast_to(col[8 * k:8 * k + 8], (8, 128)), out)
    return out


def unpacked(tile):
    return jnp.concatenate([tile[:, 32 * k:32 * k + 1] for k in range(4)], axis=0)


def forward_kernel(init_ref, len_col, len_pack, emit_hbm, a_hbm, hist_ref, scale_ref, log_ref, post_ref, rows_hbm,
                   mat, xbuf, acc, cbuf, emit, emit_sem, hist_sem, load_sem, send_sem, recv_sem, csend_sem, crecv_sem,
                   over_send, over_recv, turn_send, turn_recv, near_send, near_recv):
    me, seq = lax.axis_index("states"), lax.axis_index("seqs")
    partner, cross, far = me + 1 - 2 * (me % 2), 3 - me, (me + 2) % 4
    steps, seqs, block = emit_hbm.shape
    chunks = block // TILE

    def fetch(t):
        return pltpu.make_async_copy(emit_hbm.at[t], emit.at[t % 2], emit_sem.at[t % 2])

    fetch(0).start()
    loads = []
    for k, owner in enumerate((me, partner, cross, far)):
        rows = pl.ds(owner * block, block)
        loads.append(pltpu.make_async_copy(a_hbm.at[rows], mat.at[rows], load_sem.at[k]))
        loads[-1].start()
    entry_barrier([{"states": partner}, {"states": cross}, {"states": far}, {"seqs": 1 - seq}])

    half = block // 2
    piece = half // steps
    others = ((0, cross), (1, far))

    def over(b, kind, owner, other):
        lo = seq * half + b * piece
        return pltpu.make_async_remote_copy(
            src_ref=a_hbm.at[pl.ds(other * block + lo, piece)], dst_ref=rows_hbm.at[owner, pl.ds(lo, piece)],
            send_sem=over_send.at[b % 3, kind], recv_sem=over_recv.at[b % 3, kind], device_id={"states": other}, device_id_type=MESH)

    def turn(b, kind, owner):
        ref = rows_hbm.at[owner, pl.ds(seq * half + b * piece, piece)]
        return pltpu.make_async_remote_copy(
            src_ref=ref, dst_ref=ref, send_sem=turn_send.at[b % 2, kind], recv_sem=turn_recv.at[kind],
            device_id={"seqs": 1 - seq}, device_id_type=MESH)

    def near(b):
        return pltpu.make_async_remote_copy(
            src_ref=a_hbm.at[pl.ds(partner * block + b * 2 * piece, 2 * piece)], dst_ref=rows_hbm.at[me, pl.ds(b * 2 * piece, 2 * piece)],
            send_sem=near_send.at[b % 2], recv_sem=near_recv, device_id={"states": partner}, device_id_type=MESH)

    def rows_start(b):
        for kind, other in others:
            over(b, kind, me, other).start()
        near(b).start()

    def rows_turn(b):
        near(b).wait_send()
        for kind, other in others:
            over(b, kind, me, other).wait_send()
            over(b, kind, other, other).wait_recv()
            turn(b, kind, other).start()

    def rows_end(b):
        for kind, other in others:
            turn(b, kind, other).wait_send()

    def norm_copy(owner, kind, device):
        return pltpu.make_async_remote_copy(
            src_ref=cbuf.at[owner], dst_ref=cbuf.at[owner], send_sem=csend_sem.at[kind], recv_sem=crecv_sem.at[kind],
            device_id={"states": device}, device_id_type=MESH)

    everyone = tuple(enumerate((far, cross, partner)))

    def norm_start(sums):
        cbuf[me] = packed(jnp.sum(sums, axis=1, keepdims=True))
        for kind, other in everyone:
            norm_copy(me, kind, other).start()

    def norm_end():
        for kind, other in everyone:
            norm_copy(other, kind, other).wait_recv()
        for kind, other in everyone:
            norm_copy(me, kind, other).wait_send()
        return cbuf[0] + cbuf[1] + cbuf[2] + cbuf[3]

    def body():
        ex = Exchange(me, FORWARD_COPIES, xbuf, mat, acc, send_sem, recv_sem, hist_ref, hist_sem)
        ends = {(lo + size) // TILE - 1: k for k, (lo, size) in enumerate(ex.pieces)}

        def finish_step(t, total):
            inv = jnp.broadcast_to(unpacked(1.0 / total), (seqs, TILE))
            live = t < jnp.broadcast_to(len_col[...], (seqs, TILE))
            for n in range(chunks):
                alpha = jnp.where(live, acc[:seqs, cols(n)] * inv, post_ref[:, cols(n)])
                post_ref[:, cols(n)] = alpha
                low = alpha.astype(jnp.bfloat16)
                xbuf[t % SLOTS, me, :, cols(n)] = low
                if n in ends:
                    ex.send(t % SLOTS, ends[n], t < steps - 1)
            ex.keep(t % SLOTS, (t + 1) % steps).start()

        def fold(n, mass, sums):
            acc[:seqs, cols(n)] = mass
            return sums + mass[:, :128] + mass[:, 128:]

        fetch(0).wait()
        sums = jnp.zeros((seqs, 128), jnp.float32)
        for n in range(chunks):
            sums = fold(n, init_ref[:, cols(n)] * emit[0, :, cols(n)].astype(jnp.float32), sums)
        fetch(1).start()
        norm_start(sums)
        rows_start(0)
        post_ref[...] = jnp.zeros_like(post_ref)
        total = norm_end()
        scale_ref[0] = total
        log_ref[...] = jnp.log(total)
        finish_step(0, total)

        def step(t, carry):
            slot = (t - 1) % SLOTS

            def begin():
                rows_start(t)
                fetch(t).wait()
                pl.when(t + 1 < steps)(lambda: fetch(t + 1).start())

            ex.run(slot, begin, lambda k: pl.when(t == 1)(lambda: loads[k].wait()))
            sums = jnp.zeros((seqs, 128), jnp.float32)
            for n in range(chunks):
                sums = fold(n, acc[:seqs, cols(n)] * emit[t % 2, :, cols(n)].astype(jnp.float32), sums)
            norm_start(sums)
            rows_turn(t - 1)

            @pl.when(t > 1)
            def _():
                rows_end(t - 2)
                ex.wait_sends((t - 2) % SLOTS)

            total = norm_end()
            finish_step(t, total)
            scale = jnp.where(t < len_pack[...], total, 1.0)
            scale_ref[t] = scale
            log_ref[...] += jnp.log(scale)
            return carry

        lax.fori_loop(1, steps, step, 0)
        ex.wait_sends((steps - 2) % SLOTS)
        ex.keep((steps - 1) % SLOTS, 0).wait()

    body()
    rows_turn(steps - 1)
    rows_end(steps - 2)
    rows_end(steps - 1)

    def landed(ref, sem):
        pltpu.make_async_copy(ref, ref, sem).wait()

    for kind, other in others:
        landed(rows_hbm.at[other, pl.ds((1 - seq) * half, half)], turn_recv.at[kind])
    landed(rows_hbm.at[partner], near_recv)


def forward(emit_seq, init_loc, col, pack, trans_loc):
    steps, seqs, block = emit_seq.shape
    full = trans_loc.shape[0]
    vmem, hbm = pl.BlockSpec(memory_space=pltpu.VMEM), pl.BlockSpec(memory_space=pltpu.HBM)
    dma = pltpu.SemaphoreType.DMA
    return pl.pallas_call(
        forward_kernel,
        out_shape=[
            jax.ShapeDtypeStruct((steps, seqs, block), jnp.bfloat16),
            jax.ShapeDtypeStruct((steps, 8, 128), jnp.float32),
            jax.ShapeDtypeStruct((8, 128), jnp.float32),
            jax.ShapeDtypeStruct((seqs, block), jnp.float32),
            jax.ShapeDtypeStruct((full // block, block, block), jnp.bfloat16),
        ],
        in_specs=[vmem] * 3 + [hbm] * 2,
        out_specs=[hbm] + [vmem] * 3 + [hbm],
        scratch_shapes=[
            pltpu.VMEM((full, block), jnp.bfloat16),
            pltpu.VMEM((SLOTS, 4, seqs, block), jnp.bfloat16),
            pltpu.VMEM((FORWARD_COPIES * seqs, block), jnp.float32),
            pltpu.VMEM((4, 8, 128), jnp.float32),
            pltpu.VMEM((2, seqs, block), jnp.bfloat16),
            dma((2,)), dma((SLOTS,)), dma((4,)), dma((SLOTS, 3, 5)), dma((SLOTS, 3, 5)), dma((3,)), dma((3,)),
            dma((3, 2)), dma((3, 2)), dma((2, 2)), dma((2,)), dma((2,)), dma,
        ],
        compiler_params=pltpu.CompilerParams(collective_id=0, has_side_effects=True, vmem_limit_bytes=60 * 1024 * 1024),
        name="forward",
    )(init_loc[None, :], col, pack, emit_seq, trans_loc)


def backward_kernel(scale_ref, len_col, emit_hbm, a_hbm, rows_hbm, hist_ref,
                    mat, xbuf, coef, acc, emit, emit_sem, hist_sem, load_sem, send_sem, recv_sem):
    me = lax.axis_index("states")
    partner, cross, far = me + 1 - 2 * (me % 2), 3 - me, (me + 2) % 4
    steps, seqs, block = emit_hbm.shape
    chunks = block // TILE
    owners = (me, partner, cross, far)

    def fetch(t):
        return pltpu.make_async_copy(emit_hbm.at[t], emit.at[t % 2], emit_sem.at[t % 2])

    fetch(steps - 1).start()
    fetch(steps - 2).start()
    loads = []
    for k, owner in enumerate(owners):
        src = a_hbm.at[pl.ds(me * block, block)] if k == 0 else rows_hbm.at[owner]
        loads.append(pltpu.make_async_copy(src, mat.at[pl.ds(owner * block, block)], load_sem.at[k]))
        loads[-1].start()
    entry_barrier([{"states": partner}, {"states": cross}, {"states": far}])

    def weigh(t):
        inv = jnp.where(t < len_col[...], unpacked(1.0 / scale_ref[t]), 0.0)
        fetch(t).wait()
        coef[...] = emit[t % 2].astype(jnp.float32) * inv
        pl.when(t > 2)(lambda: fetch(t - 2).start())

    weigh(steps - 1)
    xbuf[0, me] = jnp.zeros(xbuf.shape[2:], xbuf.dtype)

    def flips():
        side = block // TILE
        for owner, load in zip(owners, loads):
            load.wait()

            def flip_row(r, carry):
                def flip(c, inner):
                    def tile(p, q):
                        return pl.ds(pl.multiple_of(owner * block + p * TILE, TILE), TILE), pl.ds(pl.multiple_of(q * TILE, TILE), TILE)

                    upper, lower = mat[tile(r, c)], mat[tile(c, r)]
                    mat[tile(r, c)] = lower.T
                    mat[tile(c, r)] = upper.T
                    return inner

                return lax.fori_loop(r, side, flip, carry)

            lax.fori_loop(0, side, flip_row, 0)

    def body():
        ex = Exchange(me, BACKWARD_COPIES, xbuf, mat, acc, send_sem, recv_sem, hist_ref, hist_sem)
        ends = {(lo + size) // TILE - 1: k for k, (lo, size) in enumerate(ex.pieces)}

        def emit_weight(t, n, weight):
            low = weight.astype(jnp.bfloat16)
            xbuf[t % SLOTS, me, :, cols(n)] = low
            if n in ends:
                ex.send(t % SLOTS, ends[n], t > 1)

        for n in range(chunks):
            emit_weight(steps - 1, n, coef[:, cols(n)])
        ex.keep((steps - 1) % SLOTS, steps - 1).start()
        ex.keep(0, 0).start()
        flips()
        ex.keep(0, 0).wait()

        def step(k, carry):
            t = steps - 1 - k
            weigh(t - 1)

            ex.run(t % SLOTS, lambda: None)
            dead = jnp.where(t < jnp.broadcast_to(len_col[...], (seqs, TILE)), 0.0, 1.0)
            for n in range(chunks):
                emit_weight(t - 1, n, coef[:, cols(n)] * (acc[:seqs, cols(n)] + dead))
            ex.keep((t - 1) % SLOTS, t - 1).start()

            @pl.when(k > 0)
            def _():
                ex.wait_sends((t + 1) % SLOTS)

            return carry

        lax.fori_loop(0, steps - 2, step, 0)
        ex.wait_sends(2 % SLOTS)
        ex.keep(1 % SLOTS, 1).wait()

    body()


def backward(emit_seq, scales, col, trans_loc, rows_loc):
    steps, seqs, block = emit_seq.shape
    full = trans_loc.shape[0]
    vmem, hbm = pl.BlockSpec(memory_space=pltpu.VMEM), pl.BlockSpec(memory_space=pltpu.HBM)
    dma = pltpu.SemaphoreType.DMA
    return pl.pallas_call(
        backward_kernel,
        out_shape=jax.ShapeDtypeStruct((steps, seqs, block), jnp.bfloat16),
        in_specs=[vmem] * 2 + [hbm] * 3,
        out_specs=hbm,
        scratch_shapes=[
            pltpu.VMEM((full, block), jnp.bfloat16),
            pltpu.VMEM((SLOTS, 4, seqs, block), jnp.bfloat16),
            pltpu.VMEM((seqs, block), jnp.float32),
            pltpu.VMEM((BACKWARD_COPIES * seqs, block), jnp.float32),
            pltpu.VMEM((2, seqs, block), jnp.bfloat16),
            dma((2,)), dma((SLOTS,)), dma((4,)), dma((SLOTS, 3, 5)), dma((SLOTS, 3, 5)),
        ],
        compiler_params=pltpu.CompilerParams(collective_id=1, has_side_effects=True, vmem_limit_bytes=60 * 1024 * 1024),
        name="backward",
    )(scales, col, emit_seq, trans_loc, rows_loc)


GROUP = 4
ROWS = 8


def gather_kernel(tok_smem, tok_ref, emit_hbm, out_ref, buf, sem):
    g = pl.program_id(0)
    seqs, steps = tok_ref.shape

    def fetch(group):
        for s in range(GROUP):
            for b in range(seqs):
                lo = pl.multiple_of(tok_smem[b, group * GROUP + s] // ROWS * ROWS, ROWS)
                pltpu.make_async_copy(emit_hbm.at[pl.ds(lo, ROWS)], buf.at[group % 2, s, pl.ds(b * ROWS, ROWS)], sem.at[group % 2]).start()

    pl.when(g == 0)(lambda: fetch(0))
    pl.when(g + 1 < steps // GROUP)(lambda: fetch(g + 1))
    landed = buf.at[g % 2]
    pltpu.make_async_copy(landed, landed, sem.at[g % 2]).wait()
    lane = lax.broadcasted_iota(jnp.int32, tok_ref.shape, 1)
    wide = (seqs, seqs * ROWS)
    row, column = (lax.broadcasted_iota(jnp.int32, wide, d) for d in range(2))
    for s in range(GROUP):
        token = jnp.sum(jnp.where(lane == g * GROUP + s, tok_ref[...], 0).astype(jnp.float32), axis=1, keepdims=True).astype(jnp.int32)
        chosen = jnp.where(column == row * ROWS + jnp.broadcast_to(token % ROWS, wide), 1.0, 0.0).astype(jnp.bfloat16)
        out_ref[s] = jnp.dot(chosen, buf[g % 2, s], preferred_element_type=jnp.float32).astype(jnp.bfloat16)


def gather(emit_loc, tokens_loc):
    seqs, steps = tokens_loc.shape
    block = emit_loc.shape[0]
    return pl.pallas_call(
        gather_kernel,
        grid=(steps // GROUP,),
        out_shape=jax.ShapeDtypeStruct((steps, seqs, block), jnp.bfloat16),
        in_specs=[pl.BlockSpec(memory_space=pltpu.SMEM), pl.BlockSpec(memory_space=pltpu.VMEM), pl.BlockSpec(memory_space=pltpu.HBM)],
        out_specs=pl.BlockSpec((GROUP, seqs, block), lambda g: (g, 0, 0)),
        scratch_shapes=[pltpu.VMEM((2, GROUP, seqs * ROWS, block), jnp.bfloat16), pltpu.SemaphoreType.DMA((2,))],
        compiler_params=pltpu.CompilerParams(dimension_semantics=("arbitrary",), vmem_limit_bytes=32 * 1024 * 1024),
        name="gather",
    )(tokens_loc, tokens_loc, emit_loc.T)


def solution(mesh):
    def local_run(trans_loc, emit_loc, init_loc, tokens_loc, lengths_loc):
        seqs, steps = tokens_loc.shape
        block = trans_loc.shape[1]
        emit_seq = gather(emit_loc, tokens_loc)
        col = lengths_loc[:, None]
        pack = jnp.broadcast_to(lengths_loc.reshape(4, 8).T[:, :, None], (8, 4, 32)).reshape(8, 128)
        alphas, scales, log_sum, last, rows_loc = forward(emit_seq, init_loc, col, pack, trans_loc)
        weights = backward(emit_seq, scales, col, trans_loc, rows_loc)
        pair_sum = lax.dot_general(alphas.reshape(steps * seqs, block), weights.reshape(steps * seqs, block), (((0,), (0,)), ((), ())), preferred_element_type=jnp.float32)
        diag_block = lax.dynamic_slice_in_dim(trans_loc, lax.axis_index('states') * block, block, axis=0)
        counts = diag_block.astype(jnp.float32) * pair_sum
        return log_sum[:, ::32].T.reshape(seqs), last, counts

    return jax.shard_map(local_run, mesh=mesh, in_specs=(P(None, 'states'), P('states', None), P('states'), P('seqs', None), P('seqs')), out_specs=(P('seqs'), P('seqs', 'states'), P(('seqs', 'states'), None)), check_vma=False)
```

```python
import jax
import jax.numpy as jnp
from jax import lax
from jax.experimental import pallas as pl
from jax.experimental.pallas import tpu as pltpu
from jax.sharding import PartitionSpec as P

MESH = pl.DeviceIdType.MESH
TILE = 256
SLOTS = 4
FORWARD_COPIES = 4
BACKWARD_COPIES = 4
FORWARD_ORDER = (
    "E0", "WP0", "P0", "P1", "P2", "R1", "P3", "G0", "C0", "F0", "R2", "C1", "R3", "WF1", "F1", "R4", "C2", "C3", "C4", "WF2", "F2",
    "WF3", "F3", "WF4", "F4")
BACKWARD_ORDER = (
    "WP0", "P0", "P1", "P2", "R0", "P3", "C0", "R1", "C1", "WF0", "F0", "R2", "C2", "WF1", "R3", "C3", "R4", "F1", "C4", "WF2", "F2",
    "WF3", "WF4", "F3", "F4")


def entry_barrier(others):
    barrier = pltpu.get_barrier_semaphore()
    for other in others:
        pl.semaphore_signal(barrier, inc=1, device_id=other, device_id_type=MESH)
    pl.semaphore_wait(barrier, len(others))


def cols(c):
    return pl.ds(c * TILE, TILE)


class Exchange:
    def __init__(self, me, copies, order, xbuf, mat, acc, send_sem, recv_sem, hist, hist_sem):
        self.hist, self.hist_sem = hist, hist_sem
        self.copies, self.order = copies, order
        self.first = int("R0" not in order)
        self.me, self.xbuf, self.mat, self.acc = me, xbuf, mat, acc
        self.send_sem, self.recv_sem = send_sem, recv_sem
        self.block = xbuf.shape[3]
        self.partner = me + 1 - 2 * (me % 2)
        self.cross = 3 - me
        self.far = (me + 2) % 4
        quarter = self.block // 4
        self.pieces = [(k * quarter, quarter) for k in range(3)] + [(3 * quarter, quarter // 2), (3 * quarter + quarter // 2, quarter // 2)]

    def copy(self, slot, owner, k, kind, device):
        lo, size = self.pieces[k]
        ref = self.xbuf.at[slot, owner, :, pl.ds(lo, size)]
        return pltpu.make_async_remote_copy(
            src_ref=ref, dst_ref=ref, send_sem=self.send_sem.at[slot, kind, k], recv_sem=self.recv_sem.at[slot, kind, k],
            device_id={"states": device}, device_id_type=MESH)

    def send(self, slot, k, more):
        @pl.when(more)
        def _():
            if k >= self.first:
                self.copy(slot, self.me, k, 1, self.cross).start()
            self.copy(slot, self.me, k, 0, self.partner).start()

    def keep(self, slot, t):
        return pltpu.make_async_copy(self.xbuf.at[slot, self.me], self.hist.at[t], self.hist_sem.at[slot])

    def wait_sends(self, slot):
        self.keep(slot, 0).wait()
        for k in range(len(self.pieces)):
            self.copy(slot, self.me, k, 0, self.partner).wait_send()
            if k >= self.first:
                self.copy(slot, self.me, k, 1, self.cross).wait_send()
                self.copy(slot, self.cross, k, 2, self.partner).wait_send()

    def product(self, slot, owner, lo, size, first=False, copies=1):
        lhs = self.xbuf[slot, owner, :, pl.ds(lo, size)]
        rows = pl.ds(pl.multiple_of(owner * self.block + lo, 128), size)
        prod = jnp.dot(jnp.concatenate([lhs] * copies, axis=0), self.mat[rows, :], preferred_element_type=jnp.float32)
        out = self.acc.at[:copies * lhs.shape[0]]
        out[...] = prod if first else out[...] + prod

    def run(self, slot, meanwhile, ready=lambda k: None, early=None):
        meanwhile()
        ready(0)
        self.product(slot, self.me, 0, self.block, True, self.copies)
        for i, token in enumerate(self.order):
            what, k = token[:-1], int(token[-1])
            for part in {"WP0": (1,), "R0": (2,), "WF0": (3,), "G0": (2, 3)}.get(token, ()):
                ready(part)
            if what in "EG":
                early("EG".index(what))
            elif what == "WP":
                for j in range(len(self.pieces)):
                    self.copy(slot, self.partner, j, 0, self.partner).wait_recv()
            elif what == "P":
                self.product(slot, self.partner, k * (self.block // 4), self.block // 4, copies=self.copies)
            elif what == "R":
                self.copy(slot, self.cross, k, 1, self.cross).wait_recv()
                self.copy(slot, self.cross, k, 2, self.partner).start()
            elif what == "WF":
                self.copy(slot, self.far, k, 2, self.partner).wait_recv()
            else:
                lo, size = self.pieces[k]
                long = size == self.block // 4 and i < len(self.order) - 2
                self.product(slot, self.cross if what == "C" else self.far, lo, size, copies=self.copies if long else 1)


def packed(col):
    group = lax.broadcasted_iota(jnp.int32, (8, 128), 1) // 32
    out = jnp.broadcast_to(col[24:32], (8, 128))
    for k in range(3):
        out = jnp.where(group == k, jnp.broadcast_to(col[8 * k:8 * k + 8], (8, 128)), out)
    return out


def unpacked(tile):
    return jnp.concatenate([tile[:, 32 * k:32 * k + 1] for k in range(4)], axis=0)


def forward_kernel(init_ref, len_col, len_pack, emit_hbm, a_hbm, hist_ref, scale_ref, log_ref, post_ref, rows_hbm,
                   mat, xbuf, acc, cbuf, emit, raw, raw_in, inv_ref, raw_send, raw_recv, emit_sem, hist_sem, load_sem, send_sem, recv_sem, csend_sem, crecv_sem,
                   over_send, over_recv, turn_send, turn_recv, near_send, near_recv):
    me, seq = lax.axis_index("states"), lax.axis_index("seqs")
    partner, cross, far = me + 1 - 2 * (me % 2), 3 - me, (me + 2) % 4
    steps, seqs, block = emit_hbm.shape
    chunks = block // TILE

    def fetch(t):
        return pltpu.make_async_copy(emit_hbm.at[t], emit.at[t % 2], emit_sem.at[t % 2])

    fetch(0).start()
    loads = []
    for k, owner in enumerate((me, partner, cross, far)):
        rows = pl.ds(owner * block, block)
        loads.append(pltpu.make_async_copy(a_hbm.at[rows], mat.at[rows], load_sem.at[k]))
        loads[-1].start()
    entry_barrier([{"states": partner}, {"states": cross}, {"states": far}, {"seqs": 1 - seq}])

    half = block // 2
    piece = half // steps
    others = ((0, cross), (1, far))

    def over(b, kind, owner, other):
        lo = seq * half + b * piece
        return pltpu.make_async_remote_copy(
            src_ref=a_hbm.at[pl.ds(other * block + lo, piece)], dst_ref=rows_hbm.at[owner, pl.ds(lo, piece)],
            send_sem=over_send.at[b % 3, kind], recv_sem=over_recv.at[b % 3, kind], device_id={"states": other}, device_id_type=MESH)

    def turn(b, kind, owner):
        ref = rows_hbm.at[owner, pl.ds(seq * half + b * piece, piece)]
        return pltpu.make_async_remote_copy(
            src_ref=ref, dst_ref=ref, send_sem=turn_send.at[b % 2, kind], recv_sem=turn_recv.at[kind],
            device_id={"seqs": 1 - seq}, device_id_type=MESH)

    def near(b):
        return pltpu.make_async_remote_copy(
            src_ref=a_hbm.at[pl.ds(partner * block + b * 2 * piece, 2 * piece)], dst_ref=rows_hbm.at[me, pl.ds(b * 2 * piece, 2 * piece)],
            send_sem=near_send.at[b % 2], recv_sem=near_recv, device_id={"states": partner}, device_id_type=MESH)

    def rows_start(b):
        for kind, other in others:
            over(b, kind, me, other).start()
        near(b).start()

    def rows_turn(b):
        near(b).wait_send()
        for kind, other in others:
            over(b, kind, me, other).wait_send()
            over(b, kind, other, other).wait_recv()
            turn(b, kind, other).start()

    def rows_end(b):
        for kind, other in others:
            turn(b, kind, other).wait_send()

    def norm_copy(owner, kind, device):
        return pltpu.make_async_remote_copy(
            src_ref=cbuf.at[owner], dst_ref=cbuf.at[owner], send_sem=csend_sem.at[kind], recv_sem=crecv_sem.at[kind],
            device_id={"states": device}, device_id_type=MESH)

    everyone = tuple(enumerate((far, cross, partner)))

    def norm_start(sums):
        cbuf[me] = packed(jnp.sum(sums, axis=1, keepdims=True))
        for kind, other in everyone:
            norm_copy(me, kind, other).start()

    def norm_end():
        for kind, other in everyone:
            norm_copy(other, kind, other).wait_recv()
        for kind, other in everyone:
            norm_copy(me, kind, other).wait_send()
        return cbuf[0] + cbuf[1] + cbuf[2] + cbuf[3]

    width = block // 4

    def raw_copy(t, hop):
        slot = t % 2
        return pltpu.make_async_remote_copy(
            src_ref=raw_in.at[slot, 0] if hop else raw.at[slot], dst_ref=raw_in.at[slot, hop],
            send_sem=raw_send.at[slot, hop], recv_sem=raw_recv.at[slot, hop],
            device_id={"states": partner if hop else cross}, device_id_type=MESH)

    def raw_finish(t, hop):
        raw_copy(t, hop).wait_recv()
        if hop == 0:
            raw_copy(t, 1).start()
        owner = far if hop else cross
        live = t < jnp.broadcast_to(len_col[...], (seqs, 128))
        for k in range(width // 128):
            part = pl.ds(k * 128, 128)
            before = xbuf[(t + SLOTS - 1) % SLOTS, owner, :, part].astype(jnp.float32)
            xbuf[t % SLOTS, owner, :, part] = jnp.where(live, raw_in[t % 2, hop, :, part] * inv_ref[...], before).astype(jnp.bfloat16)

    def raw_end(t):
        raw_copy(t, 0).wait_send()
        raw_copy(t, 1).wait_send()

    def body():
        ex = Exchange(me, FORWARD_COPIES, FORWARD_ORDER, xbuf, mat, acc, send_sem, recv_sem, hist_ref, hist_sem)
        ends = {(lo + size) // TILE - 1: k for k, (lo, size) in enumerate(ex.pieces)}

        def finish_step(t, total):
            inv = jnp.broadcast_to(unpacked(1.0 / total), (seqs, TILE))
            inv_ref[...] = inv[:, :128]
            live = t < jnp.broadcast_to(len_col[...], (seqs, TILE))
            for n in range(chunks):
                alpha = jnp.where(live, acc[:seqs, cols(n)] * inv, post_ref[:, cols(n)])
                post_ref[:, cols(n)] = alpha
                low = alpha.astype(jnp.bfloat16)
                xbuf[t % SLOTS, me, :, cols(n)] = low
                if n in ends:
                    ex.send(t % SLOTS, ends[n], t < steps - 1)
            ex.keep(t % SLOTS, (t + 1) % steps).start()

        def fold(t, n, mass, sums):
            acc[:seqs, cols(n)] = mass
            if (n + 1) * TILE <= width:
                raw[t % 2, :, cols(n)] = mass
            return sums + mass[:, :128] + mass[:, 128:]

        fetch(0).wait()
        sums = jnp.zeros((seqs, 128), jnp.float32)
        for n in range(chunks):
            sums = fold(0, n, init_ref[:, cols(n)] * emit[0, :, cols(n)].astype(jnp.float32), sums)
        fetch(1).start()
        norm_start(sums)
        raw_copy(0, 0).start()
        xbuf[SLOTS - 1] = jnp.zeros(xbuf.shape[1:], xbuf.dtype)
        rows_start(0)
        post_ref[...] = jnp.zeros_like(post_ref)
        total = norm_end()
        scale_ref[0] = total
        log_ref[...] = jnp.log(total)
        finish_step(0, total)

        def step(t, carry):
            slot = (t - 1) % SLOTS

            def begin():
                rows_start(t)
                fetch(t).wait()
                pl.when(t + 1 < steps)(lambda: fetch(t + 1).start())

            ex.run(slot, begin, lambda k: pl.when(t == 1)(lambda: loads[k].wait()), lambda hop: raw_finish(t - 1, hop))
            sums = jnp.zeros((seqs, 128), jnp.float32)
            for n in range(chunks):
                sums = fold(t, n, acc[:seqs, cols(n)] * emit[t % 2, :, cols(n)].astype(jnp.float32), sums)
            norm_start(sums)
            pl.when(t + 1 < steps)(lambda: raw_copy(t, 0).start())
            raw_end(t - 1)
            rows_turn(t - 1)

            @pl.when(t > 1)
            def _():
                rows_end(t - 2)
                ex.wait_sends((t - 2) % SLOTS)

            total = norm_end()
            finish_step(t, total)
            scale = jnp.where(t < len_pack[...], total, 1.0)
            scale_ref[t] = scale
            log_ref[...] += jnp.log(scale)
            return carry

        lax.fori_loop(1, steps, step, 0)
        ex.wait_sends((steps - 2) % SLOTS)
        ex.keep((steps - 1) % SLOTS, 0).wait()

    body()
    rows_turn(steps - 1)
    rows_end(steps - 2)
    rows_end(steps - 1)

    def landed(ref, sem):
        pltpu.make_async_copy(ref, ref, sem).wait()

    for kind, other in others:
        landed(rows_hbm.at[other, pl.ds((1 - seq) * half, half)], turn_recv.at[kind])
    landed(rows_hbm.at[partner], near_recv)


def forward(emit_seq, init_loc, col, pack, trans_loc):
    steps, seqs, block = emit_seq.shape
    full = trans_loc.shape[0]
    vmem, hbm = pl.BlockSpec(memory_space=pltpu.VMEM), pl.BlockSpec(memory_space=pltpu.HBM)
    dma = pltpu.SemaphoreType.DMA
    return pl.pallas_call(
        forward_kernel,
        out_shape=[
            jax.ShapeDtypeStruct((steps, seqs, block), jnp.bfloat16),
            jax.ShapeDtypeStruct((steps, 8, 128), jnp.float32),
            jax.ShapeDtypeStruct((8, 128), jnp.float32),
            jax.ShapeDtypeStruct((seqs, block), jnp.float32),
            jax.ShapeDtypeStruct((full // block, block, block), jnp.bfloat16),
        ],
        in_specs=[vmem] * 3 + [hbm] * 2,
        out_specs=[hbm] + [vmem] * 3 + [hbm],
        scratch_shapes=[
            pltpu.VMEM((full, block), jnp.bfloat16),
            pltpu.VMEM((SLOTS, 4, seqs, block), jnp.bfloat16),
            pltpu.VMEM((FORWARD_COPIES * seqs, block), jnp.float32),
            pltpu.VMEM((4, 8, 128), jnp.float32),
            pltpu.VMEM((2, seqs, block), jnp.bfloat16),
            pltpu.VMEM((2, seqs, block // 4), jnp.float32),
            pltpu.VMEM((2, 2, seqs, block // 4), jnp.float32),
            pltpu.VMEM((seqs, 128), jnp.float32),
            dma((2, 2)), dma((2, 2)),
            dma((2,)), dma((SLOTS,)), dma((4,)), dma((SLOTS, 3, 5)), dma((SLOTS, 3, 5)), dma((3,)), dma((3,)),
            dma((3, 2)), dma((3, 2)), dma((2, 2)), dma((2,)), dma((2,)), dma,
        ],
        compiler_params=pltpu.CompilerParams(collective_id=0, has_side_effects=True, vmem_limit_bytes=60 * 1024 * 1024),
        name="forward",
    )(init_loc[None, :], col, pack, emit_seq, trans_loc)


def backward_kernel(scale_ref, len_col, emit_hbm, a_hbm, rows_hbm, hist_ref,
                    mat, xbuf, coef, acc, emit, emit_sem, hist_sem, load_sem, send_sem, recv_sem):
    me = lax.axis_index("states")
    partner, cross, far = me + 1 - 2 * (me % 2), 3 - me, (me + 2) % 4
    steps, seqs, block = emit_hbm.shape
    chunks = block // TILE
    owners = (me, partner, cross, far)

    def fetch(t):
        return pltpu.make_async_copy(emit_hbm.at[t], emit.at[t % 2], emit_sem.at[t % 2])

    fetch(steps - 1).start()
    fetch(steps - 2).start()
    loads = []
    for k, owner in enumerate(owners):
        src = a_hbm.at[pl.ds(me * block, block)] if k == 0 else rows_hbm.at[owner]
        loads.append(pltpu.make_async_copy(src, mat.at[pl.ds(owner * block, block)], load_sem.at[k]))
        loads[-1].start()
    entry_barrier([{"states": partner}, {"states": cross}, {"states": far}])

    def weigh(t):
        inv = jnp.where(t < len_col[...], unpacked(1.0 / scale_ref[t]), 0.0)
        fetch(t).wait()
        coef[...] = emit[t % 2].astype(jnp.float32) * inv
        pl.when(t > 2)(lambda: fetch(t - 2).start())

    weigh(steps - 1)
    xbuf[0, me] = jnp.zeros(xbuf.shape[2:], xbuf.dtype)

    def flips():
        side = block // TILE
        for owner, load in zip(owners, loads):
            load.wait()

            def flip_row(r, carry):
                def flip(c, inner):
                    def tile(p, q):
                        return pl.ds(pl.multiple_of(owner * block + p * TILE, TILE), TILE), pl.ds(pl.multiple_of(q * TILE, TILE), TILE)

                    upper, lower = mat[tile(r, c)], mat[tile(c, r)]
                    mat[tile(r, c)] = lower.T
                    mat[tile(c, r)] = upper.T
                    return inner

                return lax.fori_loop(r, side, flip, carry)

            lax.fori_loop(0, side, flip_row, 0)

    def body():
        ex = Exchange(me, BACKWARD_COPIES, BACKWARD_ORDER, xbuf, mat, acc, send_sem, recv_sem, hist_ref, hist_sem)
        ends = {(lo + size) // TILE - 1: k for k, (lo, size) in enumerate(ex.pieces)}

        def emit_weight(t, n, weight):
            low = weight.astype(jnp.bfloat16)
            xbuf[t % SLOTS, me, :, cols(n)] = low
            if n in ends:
                ex.send(t % SLOTS, ends[n], t > 1)

        for n in range(chunks):
            emit_weight(steps - 1, n, coef[:, cols(n)])
        ex.keep((steps - 1) % SLOTS, steps - 1).start()
        ex.keep(0, 0).start()
        flips()
        ex.keep(0, 0).wait()

        def step(k, carry):
            t = steps - 1 - k
            weigh(t - 1)

            ex.run(t % SLOTS, lambda: None)
            dead = jnp.where(t < jnp.broadcast_to(len_col[...], (seqs, TILE)), 0.0, 1.0)
            for n in range(chunks):
                emit_weight(t - 1, n, coef[:, cols(n)] * (acc[:seqs, cols(n)] + dead))
            ex.keep((t - 1) % SLOTS, t - 1).start()

            @pl.when(k > 0)
            def _():
                ex.wait_sends((t + 1) % SLOTS)

            return carry

        lax.fori_loop(0, steps - 2, step, 0)
        ex.wait_sends(2 % SLOTS)
        ex.keep(1 % SLOTS, 1).wait()

    body()


def backward(emit_seq, scales, col, trans_loc, rows_loc):
    steps, seqs, block = emit_seq.shape
    full = trans_loc.shape[0]
    vmem, hbm = pl.BlockSpec(memory_space=pltpu.VMEM), pl.BlockSpec(memory_space=pltpu.HBM)
    dma = pltpu.SemaphoreType.DMA
    return pl.pallas_call(
        backward_kernel,
        out_shape=jax.ShapeDtypeStruct((steps, seqs, block), jnp.bfloat16),
        in_specs=[vmem] * 2 + [hbm] * 3,
        out_specs=hbm,
        scratch_shapes=[
            pltpu.VMEM((full, block), jnp.bfloat16),
            pltpu.VMEM((SLOTS, 4, seqs, block), jnp.bfloat16),
            pltpu.VMEM((seqs, block), jnp.float32),
            pltpu.VMEM((BACKWARD_COPIES * seqs, block), jnp.float32),
            pltpu.VMEM((2, seqs, block), jnp.bfloat16),
            dma((2,)), dma((SLOTS,)), dma((4,)), dma((SLOTS, 3, 5)), dma((SLOTS, 3, 5)),
        ],
        compiler_params=pltpu.CompilerParams(collective_id=1, has_side_effects=True, vmem_limit_bytes=60 * 1024 * 1024),
        name="backward",
    )(scales, col, emit_seq, trans_loc, rows_loc)


GROUP = 4
ROWS = 8


def gather_kernel(tok_smem, tok_ref, emit_hbm, out_ref, buf, sem):
    g = pl.program_id(0)
    seqs, steps = tok_ref.shape

    def fetch(group):
        for s in range(GROUP):
            for b in range(seqs):
                lo = pl.multiple_of(tok_smem[b, group * GROUP + s] // ROWS * ROWS, ROWS)
                pltpu.make_async_copy(emit_hbm.at[pl.ds(lo, ROWS)], buf.at[group % 2, s, pl.ds(b * ROWS, ROWS)], sem.at[group % 2]).start()

    pl.when(g == 0)(lambda: fetch(0))
    pl.when(g + 1 < steps // GROUP)(lambda: fetch(g + 1))
    landed = buf.at[g % 2]
    pltpu.make_async_copy(landed, landed, sem.at[g % 2]).wait()
    lane = lax.broadcasted_iota(jnp.int32, tok_ref.shape, 1)
    wide = (seqs, seqs * ROWS)
    row, column = (lax.broadcasted_iota(jnp.int32, wide, d) for d in range(2))
    for s in range(GROUP):
        token = jnp.sum(jnp.where(lane == g * GROUP + s, tok_ref[...], 0).astype(jnp.float32), axis=1, keepdims=True).astype(jnp.int32)
        chosen = jnp.where(column == row * ROWS + jnp.broadcast_to(token % ROWS, wide), 1.0, 0.0).astype(jnp.bfloat16)
        out_ref[s] = jnp.dot(chosen, buf[g % 2, s], preferred_element_type=jnp.float32).astype(jnp.bfloat16)


def gather(emit_loc, tokens_loc):
    seqs, steps = tokens_loc.shape
    block = emit_loc.shape[0]
    return pl.pallas_call(
        gather_kernel,
        grid=(steps // GROUP,),
        out_shape=jax.ShapeDtypeStruct((steps, seqs, block), jnp.bfloat16),
        in_specs=[pl.BlockSpec(memory_space=pltpu.SMEM), pl.BlockSpec(memory_space=pltpu.VMEM), pl.BlockSpec(memory_space=pltpu.HBM)],
        out_specs=pl.BlockSpec((GROUP, seqs, block), lambda g: (g, 0, 0)),
        scratch_shapes=[pltpu.VMEM((2, GROUP, seqs * ROWS, block), jnp.bfloat16), pltpu.SemaphoreType.DMA((2,))],
        compiler_params=pltpu.CompilerParams(dimension_semantics=("arbitrary",), vmem_limit_bytes=60 * 1024 * 1024),
        name="gather",
    )(tokens_loc, tokens_loc, emit_loc.T)


def solution(mesh):
    def local_run(trans_loc, emit_loc, init_loc, tokens_loc, lengths_loc):
        seqs, steps = tokens_loc.shape
        block = trans_loc.shape[1]
        emit_seq = gather(emit_loc, tokens_loc)
        col = lengths_loc[:, None]
        pack = jnp.broadcast_to(lengths_loc.reshape(4, 8).T[:, :, None], (8, 4, 32)).reshape(8, 128)
        alphas, scales, log_sum, last, rows_loc = forward(emit_seq, init_loc, col, pack, trans_loc)
        weights = backward(emit_seq, scales, col, trans_loc, rows_loc)
        pair_sum = lax.dot_general(alphas.reshape(steps * seqs, block), weights.reshape(steps * seqs, block), (((0,), (0,)), ((), ())), preferred_element_type=jnp.float32)
        diag_block = lax.dynamic_slice_in_dim(trans_loc, lax.axis_index('states') * block, block, axis=0)
        counts = diag_block.astype(jnp.float32) * pair_sum
        return log_sum[:, ::32].T.reshape(seqs), last, counts

    return jax.shard_map(local_run, mesh=mesh, in_specs=(P(None, 'states'), P('states', None), P('states'), P('seqs', None), P('seqs')), out_specs=(P('seqs'), P('seqs', 'states'), P(('seqs', 'states'), None)), check_vma=False)
```

```python
import jax
import jax.numpy as jnp
from jax import lax
from jax.experimental import pallas as pl
from jax.experimental.pallas import tpu as pltpu
from jax.sharding import PartitionSpec as P

MESH = pl.DeviceIdType.MESH
TILE = 256
SLOTS = 4
FORWARD_COPIES = 4
BACKWARD_COPIES = 4
FORWARD_PIECES = (3, 2, 2, 1)
FORWARD_ORDER = (
    "WP0", "E0", "P0", "P1", "P2", "P3", "R1", "G0", "C0", "F0", "R2", "WF1", "R3", "F1", "C3", "C2", "C1", "WF2", "WF3", "F2", "F3")
BACKWARD_PIECES = (2, 2, 2, 1, 1)
BACKWARD_ORDER = (
    "WP0", "P0", "P1", "P2", "R0", "P3", "C0", "R1", "C1", "WF0", "F0", "R2", "C2", "WF1", "R3", "C3", "R4", "F1", "C4", "WF2", "F2",
    "WF3", "WF4", "F3", "F4")


def entry_barrier(others):
    barrier = pltpu.get_barrier_semaphore()
    for other in others:
        pl.semaphore_signal(barrier, inc=1, device_id=other, device_id_type=MESH)
    pl.semaphore_wait(barrier, len(others))


def cols(c):
    return pl.ds(c * TILE, TILE)


class Exchange:
    def __init__(self, me, copies, order, eighths, xbuf, mat, acc, send_sem, recv_sem, hist, hist_sem):
        self.hist, self.hist_sem = hist, hist_sem
        self.copies, self.order = copies, order
        self.first = int("R0" not in order)
        self.me, self.xbuf, self.mat, self.acc = me, xbuf, mat, acc
        self.send_sem, self.recv_sem = send_sem, recv_sem
        self.block = xbuf.shape[3]
        self.partner = me + 1 - 2 * (me % 2)
        self.cross = 3 - me
        self.far = (me + 2) % 4
        unit = self.block // 8
        self.pieces = [(sum(eighths[:k]) * unit, e * unit) for k, e in enumerate(eighths)]

    def copy(self, slot, owner, k, kind, device):
        lo, size = self.pieces[k]
        ref = self.xbuf.at[slot, owner, :, pl.ds(lo, size)]
        return pltpu.make_async_remote_copy(
            src_ref=ref, dst_ref=ref, send_sem=self.send_sem.at[slot, kind, k], recv_sem=self.recv_sem.at[slot, kind, k],
            device_id={"states": device}, device_id_type=MESH)

    def send(self, slot, k, more):
        @pl.when(more)
        def _():
            if k >= self.first:
                self.copy(slot, self.me, k, 1, self.cross).start()
            self.copy(slot, self.me, k, 0, self.partner).start()

    def keep(self, slot, t):
        return pltpu.make_async_copy(self.xbuf.at[slot, self.me], self.hist.at[t], self.hist_sem.at[slot])

    def wait_sends(self, slot):
        self.keep(slot, 0).wait()
        for k in range(len(self.pieces)):
            self.copy(slot, self.me, k, 0, self.partner).wait_send()
            if k >= self.first:
                self.copy(slot, self.me, k, 1, self.cross).wait_send()
                self.copy(slot, self.cross, k, 2, self.partner).wait_send()

    def product(self, slot, owner, lo, size, first=False, copies=1):
        lhs = self.xbuf[slot, owner, :, pl.ds(lo, size)]
        rows = pl.ds(pl.multiple_of(owner * self.block + lo, 128), size)
        prod = jnp.dot(jnp.concatenate([lhs] * copies, axis=0), self.mat[rows, :], preferred_element_type=jnp.float32)
        out = self.acc.at[:copies * lhs.shape[0]]
        out[...] = prod if first else out[...] + prod

    def run(self, slot, meanwhile, ready=lambda k: None, early=None):
        meanwhile()
        ready(0)
        self.product(slot, self.me, 0, self.block, True, self.copies)
        for i, token in enumerate(self.order):
            what, k = token[:-1], int(token[-1])
            for part in {"WP0": (1,), "R0": (2,), "WF0": (3,), "G0": (2, 3)}.get(token, ()):
                ready(part)
            if what in "EG":
                early("EG".index(what))
            elif what == "WP":
                for j in range(len(self.pieces)):
                    self.copy(slot, self.partner, j, 0, self.partner).wait_recv()
            elif what == "P":
                self.product(slot, self.partner, k * (self.block // 4), self.block // 4, copies=self.copies)
            elif what == "R":
                self.copy(slot, self.cross, k, 1, self.cross).wait_recv()
                self.copy(slot, self.cross, k, 2, self.partner).start()
            elif what == "WF":
                self.copy(slot, self.far, k, 2, self.partner).wait_recv()
            else:
                lo, size = self.pieces[k]
                long = size >= self.block // 4 and i < len(self.order) - (1 if self.first else 2)
                self.product(slot, self.cross if what == "C" else self.far, lo, size, copies=self.copies if long else 1)


def packed(col):
    group = lax.broadcasted_iota(jnp.int32, (8, 128), 1) // 32
    out = jnp.broadcast_to(col[24:32], (8, 128))
    for k in range(3):
        out = jnp.where(group == k, jnp.broadcast_to(col[8 * k:8 * k + 8], (8, 128)), out)
    return out


def table(lens, where):
    out = jnp.zeros(where.shape, jnp.int32)
    for i in range(lens.shape[0]):
        out = jnp.where(where == i, lens[i], out)
    return out


def row_of(shape):
    return lax.broadcasted_iota(jnp.int32, shape, 0)


def unpacked(tile):
    return jnp.concatenate([tile[:, 32 * k:32 * k + 1] for k in range(4)], axis=0)


def forward_kernel(init_ref, lens, emit_hbm, a_hbm, hist_ref, scale_ref, log_ref, post_ref, rows_hbm,
                   mat, xbuf, acc, cbuf, emit, raw, raw_in, inv_ref, len_col, len_pack, log_acc, raw_send, raw_recv, emit_sem, hist_sem, load_sem, send_sem, recv_sem, csend_sem, crecv_sem,
                   over_send, over_recv, turn_send, turn_recv, near_send, near_recv):
    me, seq = lax.axis_index("states"), lax.axis_index("seqs")
    partner, cross, far = me + 1 - 2 * (me % 2), 3 - me, (me + 2) % 4
    steps, seqs, block = emit_hbm.shape
    chunks = block // TILE

    def fetch(t):
        return pltpu.make_async_copy(emit_hbm.at[t], emit.at[t % 2], emit_sem.at[t % 2])

    fetch(0).start()
    len_col[...] = table(lens, row_of((seqs, 128)))
    len_pack[...] = table(lens, lax.broadcasted_iota(jnp.int32, (8, 128), 1) // 32 * 8 + row_of((8, 128)))
    loads = []
    for k, owner in enumerate((me, partner, cross, far)):
        rows = pl.ds(owner * block, block)
        loads.append(pltpu.make_async_copy(a_hbm.at[rows], mat.at[rows], load_sem.at[k]))
        loads[-1].start()
    entry_barrier([{"states": partner}, {"states": cross}, {"states": far}, {"seqs": 1 - seq}])

    half = block // 2
    piece = half // steps
    others = ((0, cross), (1, far))

    def over(b, kind, owner, other):
        lo = seq * half + b * piece
        return pltpu.make_async_remote_copy(
            src_ref=a_hbm.at[pl.ds(other * block + lo, piece)], dst_ref=rows_hbm.at[owner, pl.ds(lo, piece)],
            send_sem=over_send.at[b % 3, kind], recv_sem=over_recv.at[b % 3, kind], device_id={"states": other}, device_id_type=MESH)

    def turn(b, kind, owner):
        ref = rows_hbm.at[owner, pl.ds(seq * half + b * piece, piece)]
        return pltpu.make_async_remote_copy(
            src_ref=ref, dst_ref=ref, send_sem=turn_send.at[b % 2, kind], recv_sem=turn_recv.at[kind],
            device_id={"seqs": 1 - seq}, device_id_type=MESH)

    def near(b):
        return pltpu.make_async_remote_copy(
            src_ref=a_hbm.at[pl.ds(partner * block + b * 2 * piece, 2 * piece)], dst_ref=rows_hbm.at[me, pl.ds(b * 2 * piece, 2 * piece)],
            send_sem=near_send.at[b % 2], recv_sem=near_recv, device_id={"states": partner}, device_id_type=MESH)

    def rows_start(b):
        for kind, other in others:
            over(b, kind, me, other).start()
        near(b).start()

    def rows_turn(b):
        near(b).wait_send()
        for kind, other in others:
            over(b, kind, me, other).wait_send()
            over(b, kind, other, other).wait_recv()
            turn(b, kind, other).start()

    def rows_end(b):
        for kind, other in others:
            turn(b, kind, other).wait_send()

    def norm_copy(owner, kind, device):
        return pltpu.make_async_remote_copy(
            src_ref=cbuf.at[owner], dst_ref=cbuf.at[owner], send_sem=csend_sem.at[kind], recv_sem=crecv_sem.at[kind],
            device_id={"states": device}, device_id_type=MESH)

    everyone = tuple(enumerate((far, cross, partner)))

    def norm_start(sums):
        cbuf[me] = packed(jnp.sum(sums, axis=1, keepdims=True))
        for kind, other in everyone:
            norm_copy(me, kind, other).start()

    def norm_end():
        for kind, other in everyone:
            norm_copy(other, kind, other).wait_recv()
        for kind, other in everyone:
            norm_copy(me, kind, other).wait_send()
        return cbuf[0] + cbuf[1] + cbuf[2] + cbuf[3]

    width = block // 8 * FORWARD_PIECES[0]

    def raw_copy(t, hop):
        slot = t % 2
        return pltpu.make_async_remote_copy(
            src_ref=raw_in.at[slot, 0] if hop else raw.at[slot], dst_ref=raw_in.at[slot, hop],
            send_sem=raw_send.at[slot, hop], recv_sem=raw_recv.at[slot, hop],
            device_id={"states": partner if hop else cross}, device_id_type=MESH)

    def raw_finish(t, hop):
        raw_copy(t, hop).wait_recv()
        if hop == 0:
            raw_copy(t, 1).start()
        owner = far if hop else cross
        live = t < len_col[...]
        for k in range(width // 128):
            part = pl.ds(k * 128, 128)
            before = xbuf[(t + SLOTS - 1) % SLOTS, owner, :, part].astype(jnp.float32)
            xbuf[t % SLOTS, owner, :, part] = jnp.where(live, raw_in[t % 2, hop, :, part] * inv_ref[...], before).astype(jnp.bfloat16)

    def raw_end(t):
        raw_copy(t, 0).wait_send()
        raw_copy(t, 1).wait_send()

    def body():
        ex = Exchange(me, FORWARD_COPIES, FORWARD_ORDER, FORWARD_PIECES, xbuf, mat, acc, send_sem, recv_sem, hist_ref, hist_sem)
        ends = {(lo + size) // TILE - 1: k for k, (lo, size) in enumerate(ex.pieces)}

        def finish_step(t, total):
            inv = jnp.broadcast_to(unpacked(1.0 / total), (seqs, TILE))
            inv_ref[...] = inv[:, :128]
            live = t < jnp.broadcast_to(len_col[:, :1], (seqs, TILE))
            for n in range(chunks):
                alpha = jnp.where(live, acc[:seqs, cols(n)] * inv, post_ref[:, cols(n)])
                post_ref[:, cols(n)] = alpha
                low = alpha.astype(jnp.bfloat16)
                xbuf[t % SLOTS, me, :, cols(n)] = low
                if n in ends:
                    ex.send(t % SLOTS, ends[n], t < steps - 1)
            ex.keep(t % SLOTS, (t + 1) % steps).start()

        def fold(t, n, mass, sums):
            acc[:seqs, cols(n)] = mass
            if (n + 1) * TILE <= width:
                raw[t % 2, :, cols(n)] = mass
            return sums + mass[:, :128] + mass[:, 128:]

        fetch(0).wait()
        sums = jnp.zeros((seqs, 128), jnp.float32)
        for n in range(chunks):
            sums = fold(0, n, init_ref[:, cols(n)] * emit[0, :, cols(n)].astype(jnp.float32), sums)
        fetch(1).start()
        norm_start(sums)
        raw_copy(0, 0).start()
        xbuf[SLOTS - 1] = jnp.zeros(xbuf.shape[1:], xbuf.dtype)
        rows_start(0)
        post_ref[...] = jnp.zeros_like(post_ref)
        total = norm_end()
        scale_ref[0] = total
        log_acc[...] = jnp.log(total)
        finish_step(0, total)

        def step(t, carry):
            slot = (t - 1) % SLOTS

            def begin():
                rows_start(t)
                fetch(t).wait()
                pl.when(t + 1 < steps)(lambda: fetch(t + 1).start())

            ex.run(slot, begin, lambda k: pl.when(t == 1)(lambda: loads[k].wait()), lambda hop: raw_finish(t - 1, hop))
            sums = jnp.zeros((seqs, 128), jnp.float32)
            for n in range(chunks):
                sums = fold(t, n, acc[:seqs, cols(n)] * emit[t % 2, :, cols(n)].astype(jnp.float32), sums)
            norm_start(sums)
            pl.when(t + 1 < steps)(lambda: raw_copy(t, 0).start())
            raw_end(t - 1)
            rows_turn(t - 1)

            @pl.when(t > 1)
            def _():
                rows_end(t - 2)
                ex.wait_sends((t - 2) % SLOTS)

            total = norm_end()
            finish_step(t, total)
            scale = jnp.where(t < len_pack[...], total, 1.0)
            scale_ref[t] = scale
            log_acc[...] += jnp.log(scale)
            return carry

        lax.fori_loop(1, steps, step, 0)
        ex.wait_sends((steps - 2) % SLOTS)
        ex.keep((steps - 1) % SLOTS, 0).wait()
        square = (seqs, 128)
        logs = jnp.broadcast_to(unpacked(log_acc[...]), square)
        log_ref[...] = jnp.sum(jnp.where(row_of(square) == lax.broadcasted_iota(jnp.int32, square, 1), logs, 0.0), axis=0, keepdims=True)

    body()
    rows_turn(steps - 1)
    rows_end(steps - 2)
    rows_end(steps - 1)

    def landed(ref, sem):
        pltpu.make_async_copy(ref, ref, sem).wait()

    for kind, other in others:
        landed(rows_hbm.at[other, pl.ds((1 - seq) * half, half)], turn_recv.at[kind])
    landed(rows_hbm.at[partner], near_recv)


def forward(emit_seq, init_loc, lengths_loc, trans_loc):
    steps, seqs, block = emit_seq.shape
    full = trans_loc.shape[0]
    vmem, hbm = pl.BlockSpec(memory_space=pltpu.VMEM), pl.BlockSpec(memory_space=pltpu.HBM)
    dma = pltpu.SemaphoreType.DMA
    return pl.pallas_call(
        forward_kernel,
        out_shape=[
            jax.ShapeDtypeStruct((steps, seqs, block), jnp.bfloat16),
            jax.ShapeDtypeStruct((steps, 8, 128), jnp.float32),
            jax.ShapeDtypeStruct((1, 128), jnp.float32),
            jax.ShapeDtypeStruct((seqs, block), jnp.float32),
            jax.ShapeDtypeStruct((full // block, block, block), jnp.bfloat16),
        ],
        in_specs=[vmem, pl.BlockSpec(memory_space=pltpu.SMEM)] + [hbm] * 2,
        out_specs=[hbm] + [vmem] * 3 + [hbm],
        scratch_shapes=[
            pltpu.VMEM((full, block), jnp.bfloat16),
            pltpu.VMEM((SLOTS, 4, seqs, block), jnp.bfloat16),
            pltpu.VMEM((FORWARD_COPIES * seqs, block), jnp.float32),
            pltpu.VMEM((4, 8, 128), jnp.float32),
            pltpu.VMEM((2, seqs, block), jnp.bfloat16),
            pltpu.VMEM((2, seqs, block // 8 * FORWARD_PIECES[0]), jnp.float32),
            pltpu.VMEM((2, 2, seqs, block // 8 * FORWARD_PIECES[0]), jnp.float32),
            pltpu.VMEM((seqs, 128), jnp.float32),
            pltpu.VMEM((seqs, 128), jnp.int32),
            pltpu.VMEM((8, 128), jnp.int32),
            pltpu.VMEM((8, 128), jnp.float32),
            dma((2, 2)), dma((2, 2)),
            dma((2,)), dma((SLOTS,)), dma((4,)), dma((SLOTS, 3, 5)), dma((SLOTS, 3, 5)), dma((3,)), dma((3,)),
            dma((3, 2)), dma((3, 2)), dma((2, 2)), dma((2,)), dma((2,)), dma,
        ],
        compiler_params=pltpu.CompilerParams(collective_id=0, has_side_effects=True, vmem_limit_bytes=60 * 1024 * 1024),
        name="forward",
    )(init_loc[None, :], lengths_loc, emit_seq, trans_loc)


def backward_kernel(scale_ref, lens, emit_hbm, a_hbm, rows_hbm, hist_ref,
                    mat, xbuf, coef, acc, emit, len_col, emit_sem, hist_sem, load_sem, send_sem, recv_sem):
    me = lax.axis_index("states")
    partner, cross, far = me + 1 - 2 * (me % 2), 3 - me, (me + 2) % 4
    steps, seqs, block = emit_hbm.shape
    chunks = block // TILE
    owners = (me, partner, cross, far)

    def fetch(t):
        return pltpu.make_async_copy(emit_hbm.at[t], emit.at[t % 2], emit_sem.at[t % 2])

    fetch(steps - 1).start()
    fetch(steps - 2).start()
    len_col[...] = table(lens, row_of((seqs, 128)))
    loads = []
    for k, owner in enumerate(owners):
        src = a_hbm.at[pl.ds(me * block, block)] if k == 0 else rows_hbm.at[owner]
        loads.append(pltpu.make_async_copy(src, mat.at[pl.ds(owner * block, block)], load_sem.at[k]))
        loads[-1].start()
    entry_barrier([{"states": partner}, {"states": cross}, {"states": far}])

    def weigh(t):
        inv = jnp.where(t < len_col[:, :1], unpacked(1.0 / scale_ref[t]), 0.0)
        fetch(t).wait()
        coef[...] = emit[t % 2].astype(jnp.float32) * inv
        pl.when(t > 2)(lambda: fetch(t - 2).start())

    weigh(steps - 1)
    xbuf[0, me] = jnp.zeros(xbuf.shape[2:], xbuf.dtype)

    def flips():
        side = block // TILE
        for owner, load in zip(owners, loads):
            load.wait()

            def flip_row(r, carry):
                def flip(c, inner):
                    def tile(p, q):
                        return pl.ds(pl.multiple_of(owner * block + p * TILE, TILE), TILE), pl.ds(pl.multiple_of(q * TILE, TILE), TILE)

                    upper, lower = mat[tile(r, c)], mat[tile(c, r)]
                    mat[tile(r, c)] = lower.T
                    mat[tile(c, r)] = upper.T
                    return inner

                return lax.fori_loop(r, side, flip, carry)

            lax.fori_loop(0, side, flip_row, 0)

    def body():
        ex = Exchange(me, BACKWARD_COPIES, BACKWARD_ORDER, BACKWARD_PIECES, xbuf, mat, acc, send_sem, recv_sem, hist_ref, hist_sem)
        ends = {(lo + size) // TILE - 1: k for k, (lo, size) in enumerate(ex.pieces)}

        def emit_weight(t, n, weight):
            low = weight.astype(jnp.bfloat16)
            xbuf[t % SLOTS, me, :, cols(n)] = low
            if n in ends:
                ex.send(t % SLOTS, ends[n], t > 1)

        for n in range(chunks):
            emit_weight(steps - 1, n, coef[:, cols(n)])
        ex.keep((steps - 1) % SLOTS, steps - 1).start()
        ex.keep(0, 0).start()
        flips()
        ex.keep(0, 0).wait()

        def step(k, carry):
            t = steps - 1 - k
            weigh(t - 1)

            ex.run(t % SLOTS, lambda: None)
            dead = jnp.where(t < jnp.broadcast_to(len_col[:, :1], (seqs, TILE)), 0.0, 1.0)
            for n in range(chunks):
                emit_weight(t - 1, n, coef[:, cols(n)] * (acc[:seqs, cols(n)] + dead))
            ex.keep((t - 1) % SLOTS, t - 1).start()

            @pl.when(k > 0)
            def _():
                ex.wait_sends((t + 1) % SLOTS)

            return carry

        lax.fori_loop(0, steps - 2, step, 0)
        ex.wait_sends(2 % SLOTS)
        ex.keep(1 % SLOTS, 1).wait()

    body()


def backward(emit_seq, scales, lengths_loc, trans_loc, rows_loc):
    steps, seqs, block = emit_seq.shape
    full = trans_loc.shape[0]
    vmem, hbm = pl.BlockSpec(memory_space=pltpu.VMEM), pl.BlockSpec(memory_space=pltpu.HBM)
    dma = pltpu.SemaphoreType.DMA
    return pl.pallas_call(
        backward_kernel,
        out_shape=jax.ShapeDtypeStruct((steps, seqs, block), jnp.bfloat16),
        in_specs=[vmem, pl.BlockSpec(memory_space=pltpu.SMEM)] + [hbm] * 3,
        out_specs=hbm,
        scratch_shapes=[
            pltpu.VMEM((full, block), jnp.bfloat16),
            pltpu.VMEM((SLOTS, 4, seqs, block), jnp.bfloat16),
            pltpu.VMEM((seqs, block), jnp.float32),
            pltpu.VMEM((BACKWARD_COPIES * seqs, block), jnp.float32),
            pltpu.VMEM((2, seqs, block), jnp.bfloat16),
            pltpu.VMEM((seqs, 128), jnp.int32),
            dma((2,)), dma((SLOTS,)), dma((4,)), dma((SLOTS, 3, 5)), dma((SLOTS, 3, 5)),
        ],
        compiler_params=pltpu.CompilerParams(collective_id=1, has_side_effects=True, vmem_limit_bytes=60 * 1024 * 1024),
        name="backward",
    )(scales, lengths_loc, emit_seq, trans_loc, rows_loc)


GROUP = 4
ROWS = 8


def gather_kernel(tok_smem, tok_ref, emit_hbm, out_ref, buf, sem):
    g = pl.program_id(0)
    seqs, steps = tok_ref.shape

    def fetch(group):
        for s in range(GROUP):
            for b in range(seqs):
                lo = pl.multiple_of(tok_smem[b, group * GROUP + s] // ROWS * ROWS, ROWS)
                pltpu.make_async_copy(emit_hbm.at[pl.ds(lo, ROWS)], buf.at[group % 2, s, pl.ds(b * ROWS, ROWS)], sem.at[group % 2]).start()

    pl.when(g == 0)(lambda: fetch(0))
    pl.when(g + 1 < steps // GROUP)(lambda: fetch(g + 1))
    landed = buf.at[g % 2]
    pltpu.make_async_copy(landed, landed, sem.at[g % 2]).wait()
    lane = lax.broadcasted_iota(jnp.int32, tok_ref.shape, 1)
    wide = (seqs, seqs * ROWS)
    row, column = (lax.broadcasted_iota(jnp.int32, wide, d) for d in range(2))
    for s in range(GROUP):
        token = jnp.sum(jnp.where(lane == g * GROUP + s, tok_ref[...], 0).astype(jnp.float32), axis=1, keepdims=True).astype(jnp.int32)
        chosen = jnp.where(column == row * ROWS + jnp.broadcast_to(token % ROWS, wide), 1.0, 0.0).astype(jnp.bfloat16)
        out_ref[s] = jnp.dot(chosen, buf[g % 2, s], preferred_element_type=jnp.float32).astype(jnp.bfloat16)


def gather(emit_loc, tokens_loc):
    seqs, steps = tokens_loc.shape
    block = emit_loc.shape[0]
    return pl.pallas_call(
        gather_kernel,
        grid=(steps // GROUP,),
        out_shape=jax.ShapeDtypeStruct((steps, seqs, block), jnp.bfloat16),
        in_specs=[pl.BlockSpec(memory_space=pltpu.SMEM), pl.BlockSpec(memory_space=pltpu.VMEM), pl.BlockSpec(memory_space=pltpu.HBM)],
        out_specs=pl.BlockSpec((GROUP, seqs, block), lambda g: (g, 0, 0)),
        scratch_shapes=[pltpu.VMEM((2, GROUP, seqs * ROWS, block), jnp.bfloat16), pltpu.SemaphoreType.DMA((2,))],
        compiler_params=pltpu.CompilerParams(dimension_semantics=("arbitrary",), vmem_limit_bytes=60 * 1024 * 1024),
        name="gather",
    )(tokens_loc, tokens_loc, emit_loc.T)


def solution(mesh):
    def local_run(trans_loc, emit_loc, init_loc, tokens_loc, lengths_loc):
        seqs, steps = tokens_loc.shape
        block = trans_loc.shape[1]
        emit_seq = gather(emit_loc, tokens_loc)
        alphas, scales, log_sum, last, rows_loc = forward(emit_seq, init_loc, lengths_loc, trans_loc)
        weights = backward(emit_seq, scales, lengths_loc, trans_loc, rows_loc)
        pair_sum = lax.dot_general(alphas.reshape(steps * seqs, block), weights.reshape(steps * seqs, block), (((0,), (0,)), ((), ())), preferred_element_type=jnp.float32)
        diag_block = lax.dynamic_slice_in_dim(trans_loc, lax.axis_index('states') * block, block, axis=0)
        counts = diag_block.astype(jnp.float32) * pair_sum
        return log_sum[0, :seqs], last, counts

    return jax.shard_map(local_run, mesh=mesh, in_specs=(P(None, 'states'), P('states', None), P('states'), P('seqs', None), P('seqs')), out_specs=(P('seqs'), P('seqs', 'states'), P(('seqs', 'states'), None)), check_vma=False)
```

```python
import jax
import jax.numpy as jnp
from jax import lax
from jax.experimental import pallas as pl
from jax.experimental.pallas import tpu as pltpu
from jax.sharding import PartitionSpec as P

MESH = pl.DeviceIdType.MESH
TILE = 256
SLOTS = 4
FORWARD_COPIES = 4
BACKWARD_COPIES = 4
FORWARD_PIECES = (3, 2, 2, 1)
FORWARD_ORDER = (
    "WP0", "E0", "P0", "P1", "P2", "P3", "R1", "G0", "C0", "F0", "R2", "WF1", "R3", "F1", "C3", "C2", "C1", "WF2", "WF3", "F2", "F3")
BACKWARD_PIECES = (2, 2, 2, 1, 1)
BACKWARD_ORDER = (
    "WP0", "P0", "P1", "P2", "R0", "P3", "C0", "R1", "C1", "WF0", "F0", "R2", "C2", "WF1", "R3", "C3", "R4", "F1", "C4", "WF2", "F2",
    "WF3", "WF4", "F3", "F4")


def entry_barrier(others):
    barrier = pltpu.get_barrier_semaphore()
    for other in others:
        pl.semaphore_signal(barrier, inc=1, device_id=other, device_id_type=MESH)
    pl.semaphore_wait(barrier, len(others))


def cols(c):
    return pl.ds(c * TILE, TILE)


class Exchange:
    def __init__(self, me, copies, order, eighths, xbuf, mat, acc, send_sem, recv_sem, hist, hist_sem):
        self.hist, self.hist_sem = hist, hist_sem
        self.copies, self.order = copies, order
        self.first = int("R0" not in order)
        self.me, self.xbuf, self.mat, self.acc = me, xbuf, mat, acc
        self.send_sem, self.recv_sem = send_sem, recv_sem
        self.block = xbuf.shape[3]
        self.partner = me + 1 - 2 * (me % 2)
        self.cross = 3 - me
        self.far = (me + 2) % 4
        unit = self.block // 8
        self.pieces = [(sum(eighths[:k]) * unit, e * unit) for k, e in enumerate(eighths)]

    def copy(self, slot, owner, k, kind, device):
        lo, size = self.pieces[k]
        ref = self.xbuf.at[slot, owner, :, pl.ds(lo, size)]
        return pltpu.make_async_remote_copy(
            src_ref=ref, dst_ref=ref, send_sem=self.send_sem.at[slot, kind, k], recv_sem=self.recv_sem.at[slot, kind, k],
            device_id={"states": device}, device_id_type=MESH)

    def send(self, slot, k, more):
        @pl.when(more)
        def _():
            if k >= self.first:
                self.copy(slot, self.me, k, 1, self.cross).start()
            self.copy(slot, self.me, k, 0, self.partner).start()

    def keep(self, slot, t):
        return pltpu.make_async_copy(self.xbuf.at[slot, self.me], self.hist.at[t], self.hist_sem.at[slot])

    def wait_sends(self, slot):
        self.keep(slot, 0).wait()
        for k in range(len(self.pieces)):
            self.copy(slot, self.me, k, 0, self.partner).wait_send()
            if k >= self.first:
                self.copy(slot, self.me, k, 1, self.cross).wait_send()
                self.copy(slot, self.cross, k, 2, self.partner).wait_send()

    def product(self, slot, owner, lo, size, first=False, copies=1):
        lhs = self.xbuf[slot, owner, :, pl.ds(lo, size)]
        rows = pl.ds(pl.multiple_of(owner * self.block + lo, 128), size)
        prod = jnp.dot(jnp.concatenate([lhs] * copies, axis=0), self.mat[rows, :], preferred_element_type=jnp.float32)
        out = self.acc.at[:copies * lhs.shape[0]]
        out[...] = prod if first else out[...] + prod

    def run(self, slot, meanwhile, ready=lambda k: None, early=None):
        meanwhile()
        ready(0)
        self.product(slot, self.me, 0, self.block, True, self.copies)
        for i, token in enumerate(self.order):
            what, k = token[:-1], int(token[-1])
            for part in {"WP0": (1,), "R0": (2,), "WF0": (3,), "G0": (2, 3)}.get(token, ()):
                ready(part)
            if what in "EG":
                early("EG".index(what))
            elif what == "WP":
                for j in range(len(self.pieces)):
                    self.copy(slot, self.partner, j, 0, self.partner).wait_recv()
            elif what == "P":
                self.product(slot, self.partner, k * (self.block // 4), self.block // 4, copies=self.copies)
            elif what == "R":
                self.copy(slot, self.cross, k, 1, self.cross).wait_recv()
                self.copy(slot, self.cross, k, 2, self.partner).start()
            elif what == "WF":
                self.copy(slot, self.far, k, 2, self.partner).wait_recv()
            else:
                lo, size = self.pieces[k]
                long = size >= self.block // 4 and i < len(self.order) - (1 if self.first else 2)
                self.product(slot, self.cross if what == "C" else self.far, lo, size, copies=self.copies if long else 1)


def packed(col):
    group = lax.broadcasted_iota(jnp.int32, (8, 128), 1) // 32
    out = jnp.broadcast_to(col[24:32], (8, 128))
    for k in range(3):
        out = jnp.where(group == k, jnp.broadcast_to(col[8 * k:8 * k + 8], (8, 128)), out)
    return out


def table(lens, where):
    out = jnp.zeros(where.shape, jnp.int32)
    for i in range(lens.shape[0]):
        out = jnp.where(where == i, lens[i], out)
    return out


def row_of(shape):
    return lax.broadcasted_iota(jnp.int32, shape, 0)


def unpacked(tile):
    return jnp.concatenate([tile[:, 32 * k:32 * k + 1] for k in range(4)], axis=0)


def forward_kernel(init_ref, lens, emit_hbm, a_hbm, hist_ref, scale_ref, log_ref, post_ref, rows_hbm,
                   mat, xbuf, acc, cbuf, emit, raw, raw_in, inv_ref, len_col, len_pack, log_acc, raw_send, raw_recv, emit_sem, hist_sem, load_sem, send_sem, recv_sem, csend_sem, crecv_sem,
                   over_send, over_recv, turn_send, turn_recv, near_send, near_recv):
    me, seq = lax.axis_index("states"), lax.axis_index("seqs")
    partner, cross, far = me + 1 - 2 * (me % 2), 3 - me, (me + 2) % 4
    steps, seqs, block = emit_hbm.shape
    chunks = block // TILE

    def fetch(t):
        return pltpu.make_async_copy(emit_hbm.at[t], emit.at[t % 2], emit_sem.at[t % 2])

    fetch(0).start()
    len_col[...] = table(lens, row_of((seqs, 128)))
    len_pack[...] = table(lens, lax.broadcasted_iota(jnp.int32, (8, 128), 1) // 32 * 8 + row_of((8, 128)))
    loads = []
    for k, owner in enumerate((me, partner, cross, far)):
        rows = pl.ds(owner * block, block)
        loads.append(pltpu.make_async_copy(a_hbm.at[rows], mat.at[rows], load_sem.at[k]))
        loads[-1].start()
    entry_barrier([{"states": partner}, {"states": cross}, {"states": far}, {"seqs": 1 - seq}])

    half = block // 2
    piece = half // steps
    others = ((0, cross), (1, far))

    def over(b, kind, owner, other):
        lo = seq * half + b * piece
        return pltpu.make_async_remote_copy(
            src_ref=a_hbm.at[pl.ds(other * block + lo, piece)], dst_ref=rows_hbm.at[owner, pl.ds(lo, piece)],
            send_sem=over_send.at[b % 3, kind], recv_sem=over_recv.at[b % 3, kind], device_id={"states": other}, device_id_type=MESH)

    def turn(b, kind, owner):
        ref = rows_hbm.at[owner, pl.ds(seq * half + b * piece, piece)]
        return pltpu.make_async_remote_copy(
            src_ref=ref, dst_ref=ref, send_sem=turn_send.at[b % 2, kind], recv_sem=turn_recv.at[kind],
            device_id={"seqs": 1 - seq}, device_id_type=MESH)

    def near(b):
        return pltpu.make_async_remote_copy(
            src_ref=a_hbm.at[pl.ds(partner * block + b * 2 * piece, 2 * piece)], dst_ref=rows_hbm.at[me, pl.ds(b * 2 * piece, 2 * piece)],
            send_sem=near_send.at[b % 2], recv_sem=near_recv, device_id={"states": partner}, device_id_type=MESH)

    def rows_start(b):
        for kind, other in others:
            over(b, kind, me, other).start()
        near(b).start()

    def rows_turn(b):
        near(b).wait_send()
        for kind, other in others:
            over(b, kind, me, other).wait_send()
            over(b, kind, other, other).wait_recv()
            turn(b, kind, other).start()

    def rows_end(b):
        for kind, other in others:
            turn(b, kind, other).wait_send()

    def norm_copy(owner, kind, device):
        return pltpu.make_async_remote_copy(
            src_ref=cbuf.at[owner], dst_ref=cbuf.at[owner], send_sem=csend_sem.at[kind], recv_sem=crecv_sem.at[kind],
            device_id={"states": device}, device_id_type=MESH)

    everyone = tuple(enumerate((far, cross, partner)))

    def norm_start(sums):
        cbuf[me] = packed(jnp.sum(sums, axis=1, keepdims=True))
        for kind, other in everyone:
            norm_copy(me, kind, other).start()

    def norm_end():
        for kind, other in everyone:
            norm_copy(other, kind, other).wait_recv()
        for kind, other in everyone:
            norm_copy(me, kind, other).wait_send()
        return cbuf[0] + cbuf[1] + cbuf[2] + cbuf[3]

    width = block // 8 * FORWARD_PIECES[0]

    def raw_copy(t, hop):
        slot = t % 2
        return pltpu.make_async_remote_copy(
            src_ref=raw_in.at[slot, 0] if hop else raw.at[slot], dst_ref=raw_in.at[slot, hop],
            send_sem=raw_send.at[slot, hop], recv_sem=raw_recv.at[slot, hop],
            device_id={"states": partner if hop else cross}, device_id_type=MESH)

    def raw_finish(t, hop):
        raw_copy(t, hop).wait_recv()
        if hop == 0:
            raw_copy(t, 1).start()
        owner = far if hop else cross
        live = t < len_col[...]
        for k in range(width // 128):
            part = pl.ds(k * 128, 128)
            before = xbuf[(t + SLOTS - 1) % SLOTS, owner, :, part].astype(jnp.float32)
            xbuf[t % SLOTS, owner, :, part] = jnp.where(live, raw_in[t % 2, hop, :, part] * inv_ref[...], before).astype(jnp.bfloat16)

    def raw_end(t):
        raw_copy(t, 0).wait_send()
        raw_copy(t, 1).wait_send()

    def body():
        ex = Exchange(me, FORWARD_COPIES, FORWARD_ORDER, FORWARD_PIECES, xbuf, mat, acc, send_sem, recv_sem, hist_ref, hist_sem)
        ends = {(lo + size) // TILE - 1: k for k, (lo, size) in enumerate(ex.pieces)}

        def finish_step(t, total):
            inv = jnp.broadcast_to(unpacked(1.0 / total), (seqs, TILE))
            inv_ref[...] = inv[:, :128]
            live = t < jnp.broadcast_to(len_col[:, :1], (seqs, TILE))
            for n in range(chunks):
                alpha = jnp.where(live, acc[:seqs, cols(n)] * inv, post_ref[:, cols(n)])
                post_ref[:, cols(n)] = alpha
                low = alpha.astype(jnp.bfloat16)
                xbuf[t % SLOTS, me, :, cols(n)] = low
                if n in ends:
                    ex.send(t % SLOTS, ends[n], t < steps - 1)
            ex.keep(t % SLOTS, (t + 1) % steps).start()

        def fold(t, n, mass, sums):
            acc[:seqs, cols(n)] = mass
            if (n + 1) * TILE <= width:
                raw[t % 2, :, cols(n)] = mass
            return sums + mass[:, :128] + mass[:, 128:]

        fetch(0).wait()
        sums = jnp.zeros((seqs, 128), jnp.float32)
        for n in range(chunks):
            sums = fold(0, n, init_ref[:, cols(n)] * emit[0, :, cols(n)].astype(jnp.float32), sums)
        fetch(1).start()
        norm_start(sums)
        raw_copy(0, 0).start()
        xbuf[SLOTS - 1] = jnp.zeros(xbuf.shape[1:], xbuf.dtype)
        rows_start(0)
        post_ref[...] = jnp.zeros_like(post_ref)
        total = norm_end()
        scale_ref[0] = total
        log_acc[...] = jnp.log(total)
        finish_step(0, total)

        def step(t, carry):
            slot = (t - 1) % SLOTS

            def begin():
                rows_start(t)
                fetch(t).wait()
                pl.when(t + 1 < steps)(lambda: fetch(t + 1).start())

            ex.run(slot, begin, lambda k: pl.when(t == 1)(lambda: loads[k].wait()), lambda hop: raw_finish(t - 1, hop))
            sums = jnp.zeros((seqs, 128), jnp.float32)
            for n in range(chunks):
                sums = fold(t, n, acc[:seqs, cols(n)] * emit[t % 2, :, cols(n)].astype(jnp.float32), sums)
            norm_start(sums)
            pl.when(t + 1 < steps)(lambda: raw_copy(t, 0).start())
            raw_end(t - 1)
            rows_turn(t - 1)

            @pl.when(t > 1)
            def _():
                rows_end(t - 2)
                ex.wait_sends((t - 2) % SLOTS)

            total = norm_end()
            finish_step(t, total)
            scale = jnp.where(t < len_pack[...], total, 1.0)
            scale_ref[t] = scale
            log_acc[...] += jnp.log(scale)
            return carry

        lax.fori_loop(1, steps, step, 0)
        ex.wait_sends((steps - 2) % SLOTS)
        ex.keep((steps - 1) % SLOTS, 0).wait()
        square = (seqs, 128)
        logs = jnp.broadcast_to(unpacked(log_acc[...]), square)
        diag = row_of(square) == lax.broadcasted_iota(jnp.int32, square, 1)
        log_ref[...] = jnp.sum(jnp.where(diag, logs, 0.0), axis=0, keepdims=True)[:, :seqs]

    body()
    rows_turn(steps - 1)
    rows_end(steps - 2)
    rows_end(steps - 1)

    def landed(ref, sem):
        pltpu.make_async_copy(ref, ref, sem).wait()

    for kind, other in others:
        landed(rows_hbm.at[other, pl.ds((1 - seq) * half, half)], turn_recv.at[kind])
    landed(rows_hbm.at[partner], near_recv)


def forward(emit_seq, init_loc, lengths_loc, trans_loc):
    steps, seqs, block = emit_seq.shape
    full = trans_loc.shape[0]
    vmem, hbm = pl.BlockSpec(memory_space=pltpu.VMEM), pl.BlockSpec(memory_space=pltpu.HBM)
    dma = pltpu.SemaphoreType.DMA
    return pl.pallas_call(
        forward_kernel,
        out_shape=[
            jax.ShapeDtypeStruct((steps, seqs, block), jnp.bfloat16),
            jax.ShapeDtypeStruct((steps, 8, 128), jnp.float32),
            jax.ShapeDtypeStruct((1, seqs), jnp.float32),
            jax.ShapeDtypeStruct((seqs, block), jnp.float32),
            jax.ShapeDtypeStruct((full // block, block, block), jnp.bfloat16),
        ],
        in_specs=[vmem, pl.BlockSpec(memory_space=pltpu.SMEM)] + [hbm] * 2,
        out_specs=[hbm] + [vmem] * 3 + [hbm],
        scratch_shapes=[
            pltpu.VMEM((full, block), jnp.bfloat16),
            pltpu.VMEM((SLOTS, 4, seqs, block), jnp.bfloat16),
            pltpu.VMEM((FORWARD_COPIES * seqs, block), jnp.float32),
            pltpu.VMEM((4, 8, 128), jnp.float32),
            pltpu.VMEM((2, seqs, block), jnp.bfloat16),
            pltpu.VMEM((2, seqs, block // 8 * FORWARD_PIECES[0]), jnp.float32),
            pltpu.VMEM((2, 2, seqs, block // 8 * FORWARD_PIECES[0]), jnp.float32),
            pltpu.VMEM((seqs, 128), jnp.float32),
            pltpu.VMEM((seqs, 128), jnp.int32),
            pltpu.VMEM((8, 128), jnp.int32),
            pltpu.VMEM((8, 128), jnp.float32),
            dma((2, 2)), dma((2, 2)),
            dma((2,)), dma((SLOTS,)), dma((4,)), dma((SLOTS, 3, 5)), dma((SLOTS, 3, 5)), dma((3,)), dma((3,)),
            dma((3, 2)), dma((3, 2)), dma((2, 2)), dma((2,)), dma((2,)), dma,
        ],
        compiler_params=pltpu.CompilerParams(collective_id=0, has_side_effects=True, vmem_limit_bytes=60 * 1024 * 1024),
        name="forward",
    )(init_loc[None, :], lengths_loc, emit_seq, trans_loc)


def backward_kernel(scale_ref, lens, emit_hbm, a_hbm, rows_hbm, hist_ref,
                    mat, xbuf, coef, acc, emit, len_col, emit_sem, hist_sem, load_sem, send_sem, recv_sem):
    me = lax.axis_index("states")
    partner, cross, far = me + 1 - 2 * (me % 2), 3 - me, (me + 2) % 4
    steps, seqs, block = emit_hbm.shape
    chunks = block // TILE
    owners = (me, partner, cross, far)

    def fetch(t):
        return pltpu.make_async_copy(emit_hbm.at[t], emit.at[t % 2], emit_sem.at[t % 2])

    fetch(steps - 1).start()
    fetch(steps - 2).start()
    len_col[...] = table(lens, row_of((seqs, 128)))
    loads = []
    for k, owner in enumerate(owners):
        src = a_hbm.at[pl.ds(me * block, block)] if k == 0 else rows_hbm.at[owner]
        loads.append(pltpu.make_async_copy(src, mat.at[pl.ds(owner * block, block)], load_sem.at[k]))
        loads[-1].start()
    entry_barrier([{"states": partner}, {"states": cross}, {"states": far}])

    def weigh(t):
        inv = jnp.where(t < len_col[:, :1], unpacked(1.0 / scale_ref[t]), 0.0)
        fetch(t).wait()
        coef[...] = emit[t % 2].astype(jnp.float32) * inv
        pl.when(t > 2)(lambda: fetch(t - 2).start())

    weigh(steps - 1)
    xbuf[0, me] = jnp.zeros(xbuf.shape[2:], xbuf.dtype)

    def flips():
        side = block // TILE
        for owner, load in zip(owners, loads):
            load.wait()

            def tile(p, q):
                return pl.ds(pl.multiple_of(owner * block + p * TILE, TILE), TILE), pl.ds(pl.multiple_of(q * TILE, TILE), TILE)

            def swap(p, q):
                upper, lower = mat[tile(p, q)], mat[tile(q, p)]
                mat[tile(p, q)] = lower.T
                mat[tile(q, p)] = upper.T

            def band(d, carry):
                for r in range(side):
                    swap(r, (r + d) % side)
                return carry

            for r in range(side):
                mat[tile(r, r)] = mat[tile(r, r)].T
            lax.fori_loop(1, side // 2, band, 0)
            for r in range(side // 2):
                swap(r, r + side // 2)

    def body():
        ex = Exchange(me, BACKWARD_COPIES, BACKWARD_ORDER, BACKWARD_PIECES, xbuf, mat, acc, send_sem, recv_sem, hist_ref, hist_sem)
        ends = {(lo + size) // TILE - 1: k for k, (lo, size) in enumerate(ex.pieces)}

        def emit_weight(t, n, weight):
            low = weight.astype(jnp.bfloat16)
            xbuf[t % SLOTS, me, :, cols(n)] = low
            if n in ends:
                ex.send(t % SLOTS, ends[n], t > 1)

        for n in range(chunks):
            emit_weight(steps - 1, n, coef[:, cols(n)])
        ex.keep((steps - 1) % SLOTS, steps - 1).start()
        ex.keep(0, 0).start()
        flips()
        ex.keep(0, 0).wait()

        def step(k, carry):
            t = steps - 1 - k
            weigh(t - 1)

            ex.run(t % SLOTS, lambda: None)
            dead = jnp.where(t < jnp.broadcast_to(len_col[:, :1], (seqs, TILE)), 0.0, 1.0)
            for n in range(chunks):
                emit_weight(t - 1, n, coef[:, cols(n)] * (acc[:seqs, cols(n)] + dead))
            ex.keep((t - 1) % SLOTS, t - 1).start()

            @pl.when(k > 0)
            def _():
                ex.wait_sends((t + 1) % SLOTS)

            return carry

        lax.fori_loop(0, steps - 2, step, 0)
        ex.wait_sends(2 % SLOTS)
        ex.keep(1 % SLOTS, 1).wait()

    body()


def backward(emit_seq, scales, lengths_loc, trans_loc, rows_loc):
    steps, seqs, block = emit_seq.shape
    full = trans_loc.shape[0]
    vmem, hbm = pl.BlockSpec(memory_space=pltpu.VMEM), pl.BlockSpec(memory_space=pltpu.HBM)
    dma = pltpu.SemaphoreType.DMA
    return pl.pallas_call(
        backward_kernel,
        out_shape=jax.ShapeDtypeStruct((steps, seqs, block), jnp.bfloat16),
        in_specs=[vmem, pl.BlockSpec(memory_space=pltpu.SMEM)] + [hbm] * 3,
        out_specs=hbm,
        scratch_shapes=[
            pltpu.VMEM((full, block), jnp.bfloat16),
            pltpu.VMEM((SLOTS, 4, seqs, block), jnp.bfloat16),
            pltpu.VMEM((seqs, block), jnp.float32),
            pltpu.VMEM((BACKWARD_COPIES * seqs, block), jnp.float32),
            pltpu.VMEM((2, seqs, block), jnp.bfloat16),
            pltpu.VMEM((seqs, 128), jnp.int32),
            dma((2,)), dma((SLOTS,)), dma((4,)), dma((SLOTS, 3, 5)), dma((SLOTS, 3, 5)),
        ],
        compiler_params=pltpu.CompilerParams(collective_id=1, has_side_effects=True, vmem_limit_bytes=60 * 1024 * 1024),
        name="backward",
    )(scales, lengths_loc, emit_seq, trans_loc, rows_loc)


GROUP = 4
ROWS = 8


def gather_kernel(tok_smem, tok_ref, emit_hbm, out_ref, buf, sem):
    g = pl.program_id(0)
    seqs, steps = tok_ref.shape

    def fetch(group):
        for s in range(GROUP):
            for b in range(seqs):
                rows = emit_hbm.at[lax.shift_right_logical(tok_smem[b, group * GROUP + s], ROWS.bit_length() - 1)]
                pltpu.make_async_copy(rows, buf.at[group % 2, s, pl.ds(b * ROWS, ROWS)], sem.at[group % 2]).start()

    pl.when(g == 0)(lambda: fetch(0))
    pl.when(g + 1 < steps // GROUP)(lambda: fetch(g + 1))
    landed = buf.at[g % 2]
    pltpu.make_async_copy(landed, landed, sem.at[g % 2]).wait()
    lane = lax.broadcasted_iota(jnp.int32, tok_ref.shape, 1)
    wide = (seqs, seqs * ROWS)
    row, column = (lax.broadcasted_iota(jnp.int32, wide, d) for d in range(2))
    for s in range(GROUP):
        token = jnp.sum(jnp.where(lane == g * GROUP + s, tok_ref[...], 0).astype(jnp.float32), axis=1, keepdims=True).astype(jnp.int32)
        chosen = jnp.where(column == row * ROWS + jnp.broadcast_to(token % ROWS, wide), 1.0, 0.0).astype(jnp.bfloat16)
        out_ref[s] = jnp.dot(chosen, buf[g % 2, s], preferred_element_type=jnp.float32).astype(jnp.bfloat16)


def gather(emit_loc, tokens_loc):
    seqs, steps = tokens_loc.shape
    block = emit_loc.shape[0]
    return pl.pallas_call(
        gather_kernel,
        grid=(steps // GROUP,),
        out_shape=jax.ShapeDtypeStruct((steps, seqs, block), jnp.bfloat16),
        in_specs=[pl.BlockSpec(memory_space=pltpu.SMEM), pl.BlockSpec(memory_space=pltpu.VMEM), pl.BlockSpec(memory_space=pltpu.HBM)],
        out_specs=pl.BlockSpec((GROUP, seqs, block), lambda g: (g, 0, 0)),
        scratch_shapes=[pltpu.VMEM((2, GROUP, seqs * ROWS, block), jnp.bfloat16), pltpu.SemaphoreType.DMA((2,))],
        compiler_params=pltpu.CompilerParams(dimension_semantics=("arbitrary",), vmem_limit_bytes=60 * 1024 * 1024),
        name="gather",
    )(tokens_loc, tokens_loc, emit_loc.T.reshape(-1, ROWS, block))


def solution(mesh):
    def local_run(trans_loc, emit_loc, init_loc, tokens_loc, lengths_loc):
        seqs, steps = tokens_loc.shape
        block = trans_loc.shape[1]
        emit_seq = gather(emit_loc, tokens_loc)
        alphas, scales, log_sum, last, rows_loc = forward(emit_seq, init_loc, lengths_loc, trans_loc)
        weights = backward(emit_seq, scales, lengths_loc, trans_loc, rows_loc)
        pair_sum = lax.dot_general(alphas.reshape(steps * seqs, block), weights.reshape(steps * seqs, block), (((0,), (0,)), ((), ())), preferred_element_type=jnp.float32)
        diag_block = lax.dynamic_slice_in_dim(trans_loc, lax.axis_index('states') * block, block, axis=0)
        counts = diag_block.astype(jnp.float32) * pair_sum
        return log_sum.reshape(seqs), last, counts

    return jax.shard_map(local_run, mesh=mesh, in_specs=(P(None, 'states'), P('states', None), P('states'), P('seqs', None), P('seqs')), out_specs=(P('seqs'), P('seqs', 'states'), P(('seqs', 'states'), None)), check_vma=False)
```

```python
import jax
import jax.numpy as jnp
from jax import lax
from jax.experimental import pallas as pl
from jax.experimental.pallas import tpu as pltpu
from jax.sharding import PartitionSpec as P

MESH = pl.DeviceIdType.MESH
TILE = 256
SLOTS = 4
FORWARD_COPIES = 4
BACKWARD_COPIES = 4
FORWARD_PIECES = (3, 2, 2, 1)
FORWARD_ORDER = (
    "WP0", "E0", "P0", "P1", "P2", "P3", "R1", "G0", "C0", "F0", "R2", "WF1", "R3", "F1", "C3", "C2", "C1", "WF2", "WF3", "F2", "F3")
BACKWARD_PIECES = (2, 2, 2, 1, 1)
BACKWARD_ORDER = (
    "WP0", "P0", "P1", "P2", "R0", "P3", "C0", "R1", "C1", "WF0", "F0", "R2", "C2", "WF1", "R3", "C3", "R4", "F1", "C4", "WF2", "F2",
    "WF3", "WF4", "F3", "F4")


def entry_barrier(others):
    barrier = pltpu.get_barrier_semaphore()
    for other in others:
        pl.semaphore_signal(barrier, inc=1, device_id=other, device_id_type=MESH)
    pl.semaphore_wait(barrier, len(others))


def cols(c):
    return pl.ds(c * TILE, TILE)


class Exchange:
    def __init__(self, me, copies, order, eighths, xbuf, mat, acc, send_sem, recv_sem, hist, hist_sem):
        self.hist, self.hist_sem = hist, hist_sem
        self.copies, self.order = copies, order
        self.first = int("R0" not in order)
        self.me, self.xbuf, self.mat, self.acc = me, xbuf, mat, acc
        self.send_sem, self.recv_sem = send_sem, recv_sem
        self.block = xbuf.shape[3]
        self.partner = me + 1 - 2 * (me % 2)
        self.cross = 3 - me
        self.far = (me + 2) % 4
        unit = self.block // 8
        self.pieces = [(sum(eighths[:k]) * unit, e * unit) for k, e in enumerate(eighths)]

    def copy(self, slot, owner, k, kind, device):
        lo, size = self.pieces[k]
        ref = self.xbuf.at[slot, owner, :, pl.ds(lo, size)]
        return pltpu.make_async_remote_copy(
            src_ref=ref, dst_ref=ref, send_sem=self.send_sem.at[slot, kind, k], recv_sem=self.recv_sem.at[slot, kind, k],
            device_id={"states": device}, device_id_type=MESH)

    def send(self, slot, k, more):
        @pl.when(more)
        def _():
            if k >= self.first:
                self.copy(slot, self.me, k, 1, self.cross).start()
            self.copy(slot, self.me, k, 0, self.partner).start()

    def keep(self, slot, t):
        return pltpu.make_async_copy(self.xbuf.at[slot, self.me], self.hist.at[t], self.hist_sem.at[slot])

    def wait_sends(self, slot):
        self.keep(slot, 0).wait()
        for k in range(len(self.pieces)):
            self.copy(slot, self.me, k, 0, self.partner).wait_send()
            if k >= self.first:
                self.copy(slot, self.me, k, 1, self.cross).wait_send()
                self.copy(slot, self.cross, k, 2, self.partner).wait_send()

    def product(self, slot, owner, lo, size, first=False, copies=1):
        lhs = self.xbuf[slot, owner, :, pl.ds(lo, size)]
        rows = pl.ds(pl.multiple_of(owner * self.block + lo, 128), size)
        prod = jnp.dot(jnp.concatenate([lhs] * copies, axis=0), self.mat[rows, :], preferred_element_type=jnp.float32)
        out = self.acc.at[:copies * lhs.shape[0]]
        out[...] = prod if first else out[...] + prod

    def run(self, slot, meanwhile, ready=lambda k: None, early=None):
        meanwhile()
        ready(0)
        self.product(slot, self.me, 0, self.block, True, self.copies)
        for i, token in enumerate(self.order):
            what, k = token[:-1], int(token[-1])
            for part in {"WP0": (1,), "R0": (2,), "WF0": (3,), "G0": (2, 3)}.get(token, ()):
                ready(part)
            if what in "EG":
                early("EG".index(what))
            elif what == "WP":
                for j in range(len(self.pieces)):
                    self.copy(slot, self.partner, j, 0, self.partner).wait_recv()
            elif what == "P":
                self.product(slot, self.partner, k * (self.block // 4), self.block // 4, copies=self.copies)
            elif what == "R":
                self.copy(slot, self.cross, k, 1, self.cross).wait_recv()
                self.copy(slot, self.cross, k, 2, self.partner).start()
            elif what == "WF":
                self.copy(slot, self.far, k, 2, self.partner).wait_recv()
            else:
                lo, size = self.pieces[k]
                long = size >= self.block // 4 and i < len(self.order) - (1 if self.first else 2)
                self.product(slot, self.cross if what == "C" else self.far, lo, size, copies=self.copies if long else 1)


def packed(col):
    group = lax.broadcasted_iota(jnp.int32, (8, 128), 1) // 32
    out = jnp.broadcast_to(col[24:32], (8, 128))
    for k in range(3):
        out = jnp.where(group == k, jnp.broadcast_to(col[8 * k:8 * k + 8], (8, 128)), out)
    return out


def table(lens, where):
    out = jnp.zeros(where.shape, jnp.int32)
    for i in range(lens.shape[0]):
        out = jnp.where(where == i, lens[i], out)
    return out


def row_of(shape):
    return lax.broadcasted_iota(jnp.int32, shape, 0)


def unpacked(tile):
    return jnp.concatenate([tile[:, 32 * k:32 * k + 1] for k in range(4)], axis=0)


def forward_kernel(init_ref, lens, emit_hbm, a_hbm, hist_ref, scale_ref, log_ref, post_ref, rows_hbm,
                   mat, xbuf, acc, cbuf, emit, raw, raw_in, inv_ref, len_col, len_pack, log_acc, raw_send, raw_recv, emit_sem, hist_sem, load_sem, send_sem, recv_sem, csend_sem, crecv_sem,
                   over_send, over_recv, turn_send, turn_recv, near_send, near_recv):
    me, seq = lax.axis_index("states"), lax.axis_index("seqs")
    partner, cross, far = me + 1 - 2 * (me % 2), 3 - me, (me + 2) % 4
    steps, seqs, block = emit_hbm.shape
    chunks = block // TILE

    def fetch(t):
        return pltpu.make_async_copy(emit_hbm.at[t], emit.at[t % 2], emit_sem.at[t % 2])

    fetch(0).start()
    len_col[...] = table(lens, row_of((seqs, 128)))
    len_pack[...] = table(lens, lax.broadcasted_iota(jnp.int32, (8, 128), 1) // 32 * 8 + row_of((8, 128)))
    loads = []
    for k, owner in enumerate((me, partner, cross, far)):
        rows = pl.ds(owner * block, block)
        loads.append(pltpu.make_async_copy(a_hbm.at[rows], mat.at[rows], load_sem.at[k]))
        loads[-1].start()
    entry_barrier([{"states": partner}, {"states": cross}, {"states": far}, {"seqs": 1 - seq}])

    half = block // 2
    piece = half // steps
    others = ((0, cross), (1, far))

    def over(b, kind, owner, other):
        lo = seq * half + b * piece
        return pltpu.make_async_remote_copy(
            src_ref=a_hbm.at[pl.ds(other * block + lo, piece)], dst_ref=rows_hbm.at[owner, pl.ds(lo, piece)],
            send_sem=over_send.at[b % 3, kind], recv_sem=over_recv.at[b % 3, kind], device_id={"states": other}, device_id_type=MESH)

    def turn(b, kind, owner):
        ref = rows_hbm.at[owner, pl.ds(seq * half + b * piece, piece)]
        return pltpu.make_async_remote_copy(
            src_ref=ref, dst_ref=ref, send_sem=turn_send.at[b % 2, kind], recv_sem=turn_recv.at[kind],
            device_id={"seqs": 1 - seq}, device_id_type=MESH)

    def near(b):
        return pltpu.make_async_remote_copy(
            src_ref=a_hbm.at[pl.ds(partner * block + b * 2 * piece, 2 * piece)], dst_ref=rows_hbm.at[me, pl.ds(b * 2 * piece, 2 * piece)],
            send_sem=near_send.at[b % 2], recv_sem=near_recv, device_id={"states": partner}, device_id_type=MESH)

    def rows_start(b):
        for kind, other in others:
            over(b, kind, me, other).start()
        near(b).start()

    def rows_turn(b):
        near(b).wait_send()
        for kind, other in others:
            over(b, kind, me, other).wait_send()
            over(b, kind, other, other).wait_recv()
            turn(b, kind, other).start()

    def rows_end(b):
        for kind, other in others:
            turn(b, kind, other).wait_send()

    def norm_copy(owner, kind, device):
        return pltpu.make_async_remote_copy(
            src_ref=cbuf.at[owner], dst_ref=cbuf.at[owner], send_sem=csend_sem.at[kind], recv_sem=crecv_sem.at[kind],
            device_id={"states": device}, device_id_type=MESH)

    everyone = tuple(enumerate((far, cross, partner)))

    def norm_start(sums):
        cbuf[me] = packed(jnp.sum(sums, axis=1, keepdims=True))
        for kind, other in everyone:
            norm_copy(me, kind, other).start()

    def norm_end():
        for kind, other in everyone:
            norm_copy(other, kind, other).wait_recv()
        for kind, other in everyone:
            norm_copy(me, kind, other).wait_send()
        return cbuf[0] + cbuf[1] + cbuf[2] + cbuf[3]

    width = block // 8 * FORWARD_PIECES[0]

    def raw_copy(t, hop):
        slot = t % 2
        return pltpu.make_async_remote_copy(
            src_ref=raw_in.at[slot, 0] if hop else raw.at[slot], dst_ref=raw_in.at[slot, hop],
            send_sem=raw_send.at[slot, hop], recv_sem=raw_recv.at[slot, hop],
            device_id={"states": partner if hop else cross}, device_id_type=MESH)

    def raw_finish(t, hop):
        raw_copy(t, hop).wait_recv()
        if hop == 0:
            raw_copy(t, 1).start()
        owner = far if hop else cross
        live = t < len_col[...]
        for k in range(width // 128):
            part = pl.ds(k * 128, 128)
            before = xbuf[(t + SLOTS - 1) % SLOTS, owner, :, part].astype(jnp.float32)
            xbuf[t % SLOTS, owner, :, part] = jnp.where(live, raw_in[t % 2, hop, :, part] * inv_ref[...], before).astype(jnp.bfloat16)

    def raw_end(t):
        raw_copy(t, 0).wait_send()
        raw_copy(t, 1).wait_send()

    def body():
        ex = Exchange(me, FORWARD_COPIES, FORWARD_ORDER, FORWARD_PIECES, xbuf, mat, acc, send_sem, recv_sem, hist_ref, hist_sem)
        ends = {(lo + size) // TILE - 1: k for k, (lo, size) in enumerate(ex.pieces)}

        def finish_step(t, total):
            inv = jnp.broadcast_to(unpacked(1.0 / total), (seqs, TILE))
            inv_ref[...] = inv[:, :128]
            live = t < jnp.broadcast_to(len_col[:, :1], (seqs, TILE))
            for n in range(chunks):
                alpha = jnp.where(live, acc[:seqs, cols(n)] * inv, post_ref[:, cols(n)])
                post_ref[:, cols(n)] = alpha
                low = alpha.astype(jnp.bfloat16)
                xbuf[t % SLOTS, me, :, cols(n)] = low
                if n in ends:
                    ex.send(t % SLOTS, ends[n], t < steps - 1)
            ex.keep(t % SLOTS, (t + 1) % steps).start()

        def fold(t, n, mass, sums):
            acc[:seqs, cols(n)] = mass
            if (n + 1) * TILE <= width:
                raw[t % 2, :, cols(n)] = mass
            return sums + mass[:, :128] + mass[:, 128:]

        fetch(0).wait()
        sums = jnp.zeros((seqs, 128), jnp.float32)
        for n in range(chunks):
            sums = fold(0, n, init_ref[:, cols(n)] * emit[0, :, cols(n)].astype(jnp.float32), sums)
        fetch(1).start()
        norm_start(sums)
        raw_copy(0, 0).start()
        xbuf[SLOTS - 1] = jnp.zeros(xbuf.shape[1:], xbuf.dtype)
        rows_start(0)
        post_ref[...] = jnp.zeros_like(post_ref)
        total = norm_end()
        scale_ref[0] = total
        log_acc[...] = jnp.log(total)
        finish_step(0, total)

        def step(t, carry):
            slot = (t - 1) % SLOTS

            def begin():
                rows_start(t)
                fetch(t).wait()
                pl.when(t + 1 < steps)(lambda: fetch(t + 1).start())

            ex.run(slot, begin, lambda k: pl.when(t == 1)(lambda: loads[k].wait()), lambda hop: raw_finish(t - 1, hop))
            sums = jnp.zeros((seqs, 128), jnp.float32)
            for n in range(chunks):
                sums = fold(t, n, acc[:seqs, cols(n)] * emit[t % 2, :, cols(n)].astype(jnp.float32), sums)
            norm_start(sums)
            pl.when(t + 1 < steps)(lambda: raw_copy(t, 0).start())
            raw_end(t - 1)
            rows_turn(t - 1)

            @pl.when(t > 1)
            def _():
                rows_end(t - 2)
                ex.wait_sends((t - 2) % SLOTS)

            total = norm_end()
            finish_step(t, total)
            scale = jnp.where(t < len_pack[...], total, 1.0)
            scale_ref[t] = scale
            log_acc[...] += jnp.log(scale)
            return carry

        lax.fori_loop(1, steps, step, 0)
        ex.wait_sends((steps - 2) % SLOTS)
        ex.keep((steps - 1) % SLOTS, 0).wait()
        square = (seqs, 128)
        logs = jnp.broadcast_to(unpacked(log_acc[...]), square)
        diag = row_of(square) == lax.broadcasted_iota(jnp.int32, square, 1)
        log_ref[...] = jnp.sum(jnp.where(diag, logs, 0.0), axis=0, keepdims=True)[:, :seqs]

    body()
    rows_turn(steps - 1)
    rows_end(steps - 2)
    rows_end(steps - 1)

    def landed(ref, sem):
        pltpu.make_async_copy(ref, ref, sem).wait()

    for kind, other in others:
        landed(rows_hbm.at[other, pl.ds((1 - seq) * half, half)], turn_recv.at[kind])
    landed(rows_hbm.at[partner], near_recv)


def forward(emit_seq, init_loc, lengths_loc, trans_loc):
    steps, seqs, block = emit_seq.shape
    full = trans_loc.shape[0]
    vmem, hbm = pl.BlockSpec(memory_space=pltpu.VMEM), pl.BlockSpec(memory_space=pltpu.HBM)
    dma = pltpu.SemaphoreType.DMA
    return pl.pallas_call(
        forward_kernel,
        out_shape=[
            jax.ShapeDtypeStruct((steps, seqs, block), jnp.bfloat16),
            jax.ShapeDtypeStruct((steps, 8, 128), jnp.float32),
            jax.ShapeDtypeStruct((1, seqs), jnp.float32),
            jax.ShapeDtypeStruct((seqs, block), jnp.float32),
            jax.ShapeDtypeStruct((full // block, block, block), jnp.bfloat16),
        ],
        in_specs=[vmem, pl.BlockSpec(memory_space=pltpu.SMEM)] + [hbm] * 2,
        out_specs=[hbm] + [vmem] * 3 + [hbm],
        scratch_shapes=[
            pltpu.VMEM((full, block), jnp.bfloat16),
            pltpu.VMEM((SLOTS, 4, seqs, block), jnp.bfloat16),
            pltpu.VMEM((FORWARD_COPIES * seqs, block), jnp.float32),
            pltpu.VMEM((4, 8, 128), jnp.float32),
            pltpu.VMEM((2, seqs, block), jnp.bfloat16),
            pltpu.VMEM((2, seqs, block // 8 * FORWARD_PIECES[0]), jnp.float32),
            pltpu.VMEM((2, 2, seqs, block // 8 * FORWARD_PIECES[0]), jnp.float32),
            pltpu.VMEM((seqs, 128), jnp.float32),
            pltpu.VMEM((seqs, 128), jnp.int32),
            pltpu.VMEM((8, 128), jnp.int32),
            pltpu.VMEM((8, 128), jnp.float32),
            dma((2, 2)), dma((2, 2)),
            dma((2,)), dma((SLOTS,)), dma((4,)), dma((SLOTS, 3, 5)), dma((SLOTS, 3, 5)), dma((3,)), dma((3,)),
            dma((3, 2)), dma((3, 2)), dma((2, 2)), dma((2,)), dma((2,)), dma,
        ],
        compiler_params=pltpu.CompilerParams(collective_id=0, has_side_effects=True, vmem_limit_bytes=60 * 1024 * 1024),
        name="forward",
    )(init_loc[None, :], lengths_loc, emit_seq, trans_loc)


def backward_kernel(scale_ref, lens, emit_hbm, a_hbm, rows_hbm, hist_ref,
                    mat, xbuf, coef, acc, emit, len_col, emit_sem, hist_sem, load_sem, send_sem, recv_sem):
    me = lax.axis_index("states")
    partner, cross, far = me + 1 - 2 * (me % 2), 3 - me, (me + 2) % 4
    steps, seqs, block = emit_hbm.shape
    chunks = block // TILE
    owners = (me, partner, cross, far)

    def fetch(t):
        return pltpu.make_async_copy(emit_hbm.at[t], emit.at[t % 2], emit_sem.at[t % 2])

    fetch(steps - 1).start()
    fetch(steps - 2).start()
    len_col[...] = table(lens, row_of((seqs, 128)))
    loads = []
    for k, owner in enumerate(owners):
        src = a_hbm.at[pl.ds(me * block, block)] if k == 0 else rows_hbm.at[owner]
        loads.append(pltpu.make_async_copy(src, mat.at[pl.ds(owner * block, block)], load_sem.at[k]))
        loads[-1].start()
    entry_barrier([{"states": partner}, {"states": cross}, {"states": far}])

    def weigh(t):
        inv = jnp.where(t < len_col[:, :1], unpacked(1.0 / scale_ref[t]), 0.0)
        fetch(t).wait()
        coef[...] = emit[t % 2].astype(jnp.float32) * inv
        pl.when(t > 2)(lambda: fetch(t - 2).start())

    weigh(steps - 1)
    xbuf[0, me] = jnp.zeros(xbuf.shape[2:], xbuf.dtype)

    def flips():
        side = block // TILE
        for owner, load in zip(owners, loads):
            load.wait()

            def tile(p, q):
                return pl.ds(pl.multiple_of(owner * block + p * TILE, TILE), TILE), pl.ds(pl.multiple_of(q * TILE, TILE), TILE)

            def swap(p, q):
                upper, lower = mat[tile(p, q)], mat[tile(q, p)]
                mat[tile(p, q)] = lower.T
                mat[tile(q, p)] = upper.T

            def band(d, carry):
                for r in range(side):
                    swap(r, (r + d) % side)
                return carry

            for r in range(side):
                mat[tile(r, r)] = mat[tile(r, r)].T
            lax.fori_loop(1, side // 2, band, 0)
            for r in range(side // 2):
                swap(r, r + side // 2)

    def body():
        ex = Exchange(me, BACKWARD_COPIES, BACKWARD_ORDER, BACKWARD_PIECES, xbuf, mat, acc, send_sem, recv_sem, hist_ref, hist_sem)
        ends = {(lo + size) // TILE - 1: k for k, (lo, size) in enumerate(ex.pieces)}

        def emit_weight(t, n, weight):
            low = weight.astype(jnp.bfloat16)
            xbuf[t % SLOTS, me, :, cols(n)] = low
            if n in ends:
                ex.send(t % SLOTS, ends[n], t > 1)

        for n in range(chunks):
            emit_weight(steps - 1, n, coef[:, cols(n)])
        ex.keep((steps - 1) % SLOTS, steps - 1).start()
        ex.keep(0, 0).start()
        flips()
        ex.keep(0, 0).wait()

        def step(k, carry):
            t = steps - 1 - k
            weigh(t - 1)

            ex.run(t % SLOTS, lambda: None)
            dead = jnp.where(t < jnp.broadcast_to(len_col[:, :1], (seqs, TILE)), 0.0, 1.0)
            for n in range(chunks):
                emit_weight(t - 1, n, coef[:, cols(n)] * (acc[:seqs, cols(n)] + dead))
            ex.keep((t - 1) % SLOTS, t - 1).start()

            @pl.when(k > 0)
            def _():
                ex.wait_sends((t + 1) % SLOTS)

            return carry

        lax.fori_loop(0, steps - 2, step, 0)
        ex.wait_sends(2 % SLOTS)
        ex.keep(1 % SLOTS, 1).wait()

    body()


def backward(emit_seq, scales, lengths_loc, trans_loc, rows_loc):
    steps, seqs, block = emit_seq.shape
    full = trans_loc.shape[0]
    vmem, hbm = pl.BlockSpec(memory_space=pltpu.VMEM), pl.BlockSpec(memory_space=pltpu.HBM)
    dma = pltpu.SemaphoreType.DMA
    return pl.pallas_call(
        backward_kernel,
        out_shape=jax.ShapeDtypeStruct((steps, seqs, block), jnp.bfloat16),
        in_specs=[vmem, pl.BlockSpec(memory_space=pltpu.SMEM)] + [hbm] * 3,
        out_specs=hbm,
        scratch_shapes=[
            pltpu.VMEM((full, block), jnp.bfloat16),
            pltpu.VMEM((SLOTS, 4, seqs, block), jnp.bfloat16),
            pltpu.VMEM((seqs, block), jnp.float32),
            pltpu.VMEM((BACKWARD_COPIES * seqs, block), jnp.float32),
            pltpu.VMEM((2, seqs, block), jnp.bfloat16),
            pltpu.VMEM((seqs, 128), jnp.int32),
            dma((2,)), dma((SLOTS,)), dma((4,)), dma((SLOTS, 3, 5)), dma((SLOTS, 3, 5)),
        ],
        compiler_params=pltpu.CompilerParams(collective_id=1, has_side_effects=True, vmem_limit_bytes=60 * 1024 * 1024),
        name="backward",
    )(scales, lengths_loc, emit_seq, trans_loc, rows_loc)


GROUP = 4
DEPTH = 3
ROWS = 8


def gather_kernel(tok_smem, tok_ref, emit_hbm, out_ref, buf, sem):
    g = pl.program_id(0)
    seqs, steps = tok_ref.shape

    def fetch(group):
        for s in range(GROUP):
            for b in range(seqs):
                rows = emit_hbm.at[lax.shift_right_logical(tok_smem[b, group * GROUP + s], ROWS.bit_length() - 1)]
                pltpu.make_async_copy(rows, buf.at[group % DEPTH, s, pl.ds(b * ROWS, ROWS)], sem.at[group % DEPTH]).start()

    @pl.when(g == 0)
    def _():
        for group in range(min(DEPTH - 1, steps // GROUP)):
            fetch(group)

    pl.when(g + DEPTH - 1 < steps // GROUP)(lambda: fetch(g + DEPTH - 1))
    landed = buf.at[g % DEPTH]
    pltpu.make_async_copy(landed, landed, sem.at[g % DEPTH]).wait()
    lane = lax.broadcasted_iota(jnp.int32, tok_ref.shape, 1)
    wide = (seqs, seqs * ROWS)
    row, column = (lax.broadcasted_iota(jnp.int32, wide, d) for d in range(2))
    for s in range(GROUP):
        token = jnp.sum(jnp.where(lane == g * GROUP + s, tok_ref[...], 0).astype(jnp.float32), axis=1, keepdims=True).astype(jnp.int32)
        chosen = jnp.where(column == row * ROWS + jnp.broadcast_to(token % ROWS, wide), 1.0, 0.0).astype(jnp.bfloat16)
        out_ref[s] = jnp.dot(chosen, buf[g % DEPTH, s], preferred_element_type=jnp.float32).astype(jnp.bfloat16)


def gather(emit_loc, tokens_loc):
    seqs, steps = tokens_loc.shape
    block = emit_loc.shape[0]
    return pl.pallas_call(
        gather_kernel,
        grid=(steps // GROUP,),
        out_shape=jax.ShapeDtypeStruct((steps, seqs, block), jnp.bfloat16),
        in_specs=[pl.BlockSpec(memory_space=pltpu.SMEM), pl.BlockSpec(memory_space=pltpu.VMEM), pl.BlockSpec(memory_space=pltpu.HBM)],
        out_specs=pl.BlockSpec((GROUP, seqs, block), lambda g: (g, 0, 0)),
        scratch_shapes=[pltpu.VMEM((DEPTH, GROUP, seqs * ROWS, block), jnp.bfloat16), pltpu.SemaphoreType.DMA((DEPTH,))],
        compiler_params=pltpu.CompilerParams(dimension_semantics=("arbitrary",), vmem_limit_bytes=60 * 1024 * 1024),
        name="gather",
    )(tokens_loc, tokens_loc, emit_loc.T.reshape(-1, ROWS, block))


def solution(mesh):
    def local_run(trans_loc, emit_loc, init_loc, tokens_loc, lengths_loc):
        seqs, steps = tokens_loc.shape
        block = trans_loc.shape[1]
        emit_seq = gather(emit_loc, tokens_loc)
        alphas, scales, log_sum, last, rows_loc = forward(emit_seq, init_loc, lengths_loc, trans_loc)
        weights = backward(emit_seq, scales, lengths_loc, trans_loc, rows_loc)
        pair_sum = lax.dot_general(alphas.reshape(steps * seqs, block), weights.reshape(steps * seqs, block), (((0,), (0,)), ((), ())), preferred_element_type=jnp.float32)
        diag_block = lax.dynamic_slice_in_dim(trans_loc, lax.axis_index('states') * block, block, axis=0)
        counts = diag_block.astype(jnp.float32) * pair_sum
        return log_sum.reshape(seqs), last, counts

    return jax.shard_map(local_run, mesh=mesh, in_specs=(P(None, 'states'), P('states', None), P('states'), P('seqs', None), P('seqs')), out_specs=(P('seqs'), P('seqs', 'states'), P(('seqs', 'states'), None)), check_vma=False)
```
